32 devices in a mesh: slab: 2 (over core), py: 4 (over z), pz: 4 (over y, x).
Axes of the slice: x: 2, y: 2, z: 4, core: 2. Of those that a mesh axis runs over, the one named last changes fastest.
Arguments:
- start_vector: float32 [32, 128, 256], P('pz', 'py', 'slab'), may hold values from -6 to 6
- potential: float32 [32, 128, 256], P('pz', 'py', 'slab'), may hold values from 0.5 to 4
Outputs:
- krylov_basis: float32 [6, 32, 128, 256], P(None, 'pz', 'py', 'slab')
- tridiagonal: float32 [2, 5], replicated
The draws below stay inside these ranges and needn't reach their ends.
All inputs are finite; a program needn't handle non-finite values.
Results may differ from the reference program's by a relative error of at most 0.00012.
Values sent between devices are 32-bit elements; how exact they have to be, the bound alone decides.
A program may use at most 64 MiB of HBM per device.

```python
import jax
import jax.numpy as jnp
from jax import lax

ITERS = 5
NX = 256
NY = 128
NZ = 32


def level_of(key, dims, shards, smallest, top_value):
    loudness = 1.0
    for position, parts in shards:
        steps = jax.random.uniform(jax.random.fold_in(jax.random.fold_in(key, 6), position), (parts,), jnp.float32, smallest / len(shards), top_value / len(shards))
        loudness = loudness * jnp.repeat(jnp.exp(steps), dims[position] // parts).reshape((-1,) + (1,) * (len(dims) - 1 - position))
    return loudness


def normal_values(key, shape, deviation, limit, split=(), dtype=jnp.bfloat16):
    values = jax.random.normal(key, shape, jnp.float32) * deviation
    if len(split) > 0:
        values = level_of(key, shape, split, -0.22, 0.18) * values
    return jnp.clip(values, min=-limit, max=limit).astype(dtype)


def setup_inputs(seed: int = 0) -> dict:
    key_of = jax.random.split(jax.random.key(seed), 3)
    return {
        "start_vector": normal_values(key_of[0], (NZ, NY, NX), 1.0, 6.0, ((0, 4), (1, 4), (2, 2)), jnp.float32),
        "potential": jnp.clip(0.5 + 3.5 * jax.random.uniform(key_of[1], (NZ, NY, NX), jnp.float32) ** level_of(key_of[1], (NZ, NY, NX), ((0, 4), (1, 4), (2, 2)), -0.2, 0.2), 0.5, 4.0),
    }


EPSILON = 1e-06

def apply_hamiltonian(field, potential):
    padded = jnp.pad(field, 1)
    beside = padded[2:, 1:-1, 1:-1] + padded[:-2, 1:-1, 1:-1]
    beside = beside + padded[1:-1, 2:, 1:-1] + padded[1:-1, :-2, 1:-1]
    beside = beside + padded[1:-1, 1:-1, 2:] + padded[1:-1, 1:-1, :-2]
    return (6.0 + potential) * field - beside

def reference(start_vector, potential):
    per_cell = jnp.float32(1.0 / (NX * NY * NZ))
    start_norm = jnp.sum(start_vector * start_vector) * per_cell
    vectors = [start_vector / jnp.sqrt(start_norm + EPSILON)]
    alphas = []
    beta_list = []
    for iteration in range(ITERS):
        image = apply_hamiltonian(vectors[-1], potential)
        active = jnp.stack(vectors)
        first_coeff = jnp.einsum('kzyx,zyx->k', active, image, precision=lax.Precision.HIGHEST) * per_cell
        image = image - jnp.einsum('k,kzyx->zyx', first_coeff, active, precision=lax.Precision.HIGHEST)
        second_coeff = jnp.einsum('kzyx,zyx->k', active, image, precision=lax.Precision.HIGHEST) * per_cell
        image = image - jnp.einsum('k,kzyx->zyx', second_coeff, active, precision=lax.Precision.HIGHEST)
        square_mean = jnp.sum(image * image) * per_cell
        beta_value = jnp.sqrt(square_mean + EPSILON)
        alphas.append(first_coeff[iteration] + second_coeff[iteration])
        beta_list.append(beta_value)
        vectors.append(image / beta_value)
    return (jnp.stack(vectors), jnp.stack([jnp.stack(alphas), jnp.stack(beta_list)]))
```

```python
import functools

import jax
import jax.numpy as jnp
from jax import lax
from jax.experimental import pallas as pl
from jax.experimental.pallas import tpu as pltpu
from jax.sharding import PartitionSpec as P

ITERS = 5
EPSILON = 1e-06
DIAGONAL = 6.0
SUBLANES = 8
MESH = pl.DeviceIdType.MESH
AXES = ("slab", "py", "pz")
UNROLLED = 64
CENTER = 8.25
LEAST_SQUARE, MOST_SQUARE = 0.25, 40.0
LEAST_SHIFT, MOST_SHIFT = 0.5, 16.5
VECTOR, POTENTIAL = 0, 1


def times(coeff, columns):
    total = {}
    for k, c in coeff.items():
        for q, value in columns[k].items():
            term = c * value
            total[q] = total[q] + term if q in total else term
    return total


def dot(left, right):
    total = None
    for q, value in left.items():
        if q in right:
            term = value * right[q]
            total = term if total is None else total + term
    return 0.0 if total is None else total


def advance(steps, inner, shifts, taus, removed, betas):
    vectors = [{0: 1.0}]
    image_of = []
    for i in range(steps):
        column = {i + 1: 1.0, i: shifts[i]}
        if taus[i] is not None:
            column[i - 1] = taus[i]
        image_of.append(column)
    gram, lowered = {}, []
    for n in range(steps):
        for k in range(len(lowered), n + 1):
            lowered.append({
                q: dot(vectors[k], {b: inner[q, b] for b in vectors[k]})
                for q in range(n + 1)})
            for l in range(k + 1):
                gram[k, l] = gram[l, k] = dot(vectors[l], lowered[k])
        known = {n: shifts[n]}
        if n > 0:
            known[n - 1] = betas[n - 1]
            rest = times(vectors[n], image_of)
            for k, y in known.items():
                for q, value in vectors[k].items():
                    rest[q] = rest[q] - y * value if q in rest else -y * value
        else:
            rest = {n + 1: 1.0}
        rest_lowered = {
            q: dot(rest, {b: inner[q, b] for b in rest}) for q in range(n + 2)}
        along = {k: dot(vectors[k], rest_lowered) for k in range(n + 1)}
        first = {
            k: along[k] + dot(known, {l: gram[k, l] for l in known}) for k in range(n + 1)}
        excess = {k: first[k] - known[k] if k in known else first[k] for k in range(n + 1)}
        coeffs = {
            k: along[k] - dot(excess, {
                l: gram[k, l] - 1.0 if k == l else gram[k, l] for l in range(n + 1)})
            for k in range(n + 1)}
        square = dot(rest, rest_lowered)
        for k in range(n + 1):
            back = dot(coeffs, {l: gram[k, l] for l in range(n + 1)})
            square = square + coeffs[k] * (back - 2.0 * along[k])
        beta = jnp.sqrt(jnp.maximum(square, 0.0) + EPSILON)
        inverse = 1.0 / beta
        image = dict(rest)
        for k in range(n + 1):
            for q, value in vectors[k].items():
                term = coeffs[k] * value
                image[q] = image[q] - term if q in image else -term
        vectors.append({q: value * inverse for q, value in image.items()})
        removed.append({k: coeffs[k] + known[k] if k in known else coeffs[k] for k in coeffs})
        betas.append(beta)
    return vectors[1:]


def kernel(sizes, per_cell, x_hbm, pot_hbm, out_ref, tri_ref, cells, ext, swapped, slots,
           send_sem, recv_sem, side_send, side_recv, near_send, near_recv, swap_send, swap_recv,
           stat_send, stat_recv, load_sem):
    Z, Y, X = x_hbm.shape
    S, A, B = sizes
    n = S * A * B
    H = Z // 2
    D = ITERS
    T = SUBLANES
    ZE, YE = H + 2 * D, Y + 2 * T
    slab, py, pz = (lax.axis_index(name) for name in AXES)
    me = (slab * A + py) * B + pz
    partner = (1 - slab, py, pz)
    first_plane = D - slab * H
    inside = pl.ds(T, Y)

    def to_others(act):
        if n <= UNROLLED:
            slabs = [lax.rem(slab + i, S) for i in range(S)]
            pys = [lax.rem(py + i, A) for i in range(A)]
            pzs = [lax.rem(pz + i, B) for i in range(B)]
            far = sorted(
                ((i, j, k) for i in range(S) for j in range(A) for k in range(B)),
                key=lambda t: -(min(t[1], A - t[1]) + min(t[2], B - t[2])),
            )
            for i, j, k in far:
                if i or j or k:
                    act((slabs[i], pys[j], pzs[k]))
        else:
            def step(d, carry):
                t = lax.rem(me + d, n)
                act((t // (A * B), lax.rem(t // B, A), lax.rem(t, B)))
                return carry
            lax.fori_loop(1, n, step, 0)

    def source(array):
        return cells.at[0] if array == VECTOR else ext

    def remote(src, dst, sent, received, target):
        return pltpu.make_async_remote_copy(
            src_ref=src, dst_ref=dst, send_sem=sent, recv_sem=received,
            device_id=target, device_id_type=MESH)

    def reach(array):
        return D if array == VECTOR else D - 1

    def within(step, position, size):
        if step == 0:
            return None
        return position + step >= 0 if step < 0 else position + step < size

    def guarded(conditions, act):
        conditions = [c for c in conditions if c is not None]
        if not conditions:
            act()
        else:
            pl.when(functools.reduce(jnp.logical_and, conditions))(act)

    def plane_of(t, side, d):
        z = t * H - d if side == 0 else t * H + H - 1 + d
        return z // Z, z % Z

    def lands(side, d):
        return D - d if side == 0 else D + H - 1 + d

    def rows(step, count, sending):
        if step == 0:
            return inside
        if step < 0:
            return pl.ds(T + Y - count, count) if sending else pl.ds(T - count, count)
        return pl.ds(T, count) if sending else pl.ds(T + Y, count)

    def index(array, side, d, step):
        return ((array * 2 + side) * D + d - 1) * 3 + step + 1

    def plane_copy(array, t, side, d, step, core):
        q, z = plane_of(t, side, d)
        count = reach(array) - d
        ref = source(array)
        i = index(array, side, d, step)
        return remote(
            ref.at[core, z + first_plane, rows(step, count, True)],
            ref.at[core, lands(side, d), rows(step, count, False)],
            send_sem.at[i, t], recv_sem.at[i, core], (t, py - step, pz - q))

    def planes(w, sending, act):
        for t in range(2):
            for side in range(2):
                wanted = [(array, d) for array, d in ((VECTOR, w), (POTENTIAL, w - 1))
                          if 1 <= d <= reach(array) and plane_of(t, side, d)[0] != 0]
                for q in sorted({plane_of(t, side, d)[0] for _, d in wanted}, key=abs):
                    mine = [(a, d) for a, d in wanted if plane_of(t, side, d)[0] == q]
                    sign = -1 if sending else 1
                    own = None if sending else slab == t

                    def straight(t=t, side=side, mine=mine):
                        for array, d in mine:
                            act(array, t, side, d, 0)

                    guarded([own, within(sign * q, pz, B)], straight)
                    for step in (-1, 1):
                        beside = [(a, d) for a, d in mine if reach(a) > d]
                        if beside:
                            def corner(t=t, side=side, beside=beside, step=step):
                                for array, d in beside:
                                    act(array, t, side, d, step)

                            guarded([own, within(sign * q, pz, B), within(sign * step, py, A)], corner)

    def start_plane(*key):
        plane_copy(*key, slab).start()

    def finish_plane(*key):
        plane_copy(*key, slab).wait_send()

    def take_plane(*key):
        for core in range(2):
            plane_copy(*key, core).wait_recv()

    def side_copy(array, t, step, core):
        ref = source(array)
        count = reach(array)
        return remote(
            ref.at[core, pl.ds(first_plane, Z), rows(step, count, True)],
            ref.at[core, pl.ds(D - t * H, Z), rows(step, count, False)],
            side_send.at[array, step > 0 and 1 or 0, t], side_recv.at[array, step > 0 and 1 or 0, core],
            (t, py - step, pz))

    def sides(sending, act):
        for step in (-1, 1):
            def both(step=step):
                for array in (VECTOR, POTENTIAL):
                    for other in range(2):
                        act(array, other, step)
            guarded([within(-step if sending else step, py, A)], both)

    def near_copy(array):
        ref = source(array)
        return remote(
            ref.at[slab, pl.ds(first_plane, Z), inside],
            ref.at[slab, pl.ds(D - (1 - slab) * H, Z), inside],
            near_send.at[array], near_recv.at[array], partner)

    def near_arrival(array):
        ref = source(array)
        span = ref.at[1 - slab, pl.ds(first_plane, Z), inside]
        return remote(span, span, near_send.at[array], near_recv.at[array], partner)

    def side_arrival(array, core, step):
        ref = source(array)
        span = ref.at[core, pl.ds(first_plane, Z), rows(step, reach(array), False)]
        k = step > 0 and 1 or 0
        return remote(span, span, side_send.at[array, k, 0], side_recv.at[array, k, core], partner)

    def swap_copy(level):
        return remote(
            cells.at[level, 1 - slab, pl.ds(D, H), inside], swapped.at[level - 1],
            swap_send.at[level - 1], swap_recv.at[level - 1], partner)

    def stat_copy(p, target):
        return remote(slots.at[p, me], slots.at[p, me], stat_send.at[p], stat_recv.at[p], target)

    def wait_all(p, sem):
        span = slots.at[p, pl.ds(0, n - 1)]
        pltpu.make_async_copy(span, span, sem).wait()

    def fold(value):
        return jnp.sum(value.reshape(value.shape[0] // T, T, X), axis=0)

    def share(p, sums):
        lines = [jnp.sum(v, axis=0, keepdims=True) for v in sums]
        height = -(-len(lines) // T) * T
        lines = lines + [jnp.zeros((1, X), jnp.float32)] * (height - len(lines))
        totals = jnp.sum(jnp.concatenate(lines, axis=0), axis=1, keepdims=True)
        at = lax.broadcasted_iota(jnp.int32, (height, X), 0)
        lanes = lax.broadcasted_iota(jnp.int32, (height, X), 1)
        slots[p, me] = jnp.sum(jnp.where(at == lanes, totals, 0.0), axis=0, keepdims=True)

    def gathered(p, count):
        wait_all(p, stat_recv.at[p])
        total = jnp.sum(slots[p], axis=0) * per_cell
        return [jnp.broadcast_to(total[:, s:s + 1], (1, X)) for s in range(count)]

    barrier = pltpu.get_barrier_semaphore()
    to_others(lambda t: pl.semaphore_signal(barrier, inc=1, device_id=t, device_id_type=MESH))
    loads = [pltpu.make_async_copy(
        hbm, source(array).at[slab, pl.ds(first_plane, Z), inside], load_sem.at[array])
        for array, hbm in ((VECTOR, x_hbm), (POTENTIAL, pot_hbm))]
    for load in loads:
        load.start()

    plane = pz * Z + slab * H - D
    present = [jnp.logical_and(plane + e >= 0, plane + e < B * Z) for e in range(ZE)]
    for e in range(ZE):
        if D <= e < D + H:
            continue
        @pl.when(jnp.logical_not(present[e]))
        def _(e=e):
            for ref in (cells.at[0], ext):
                for core in range(2):
                    ref[core, e] = jnp.zeros((YE, X), jnp.float32)
    for missing, at in ((py == 0, 0), (py == A - 1, T + Y)):
        @pl.when(missing)
        def _(at=at):
            for ref in (cells.at[0], ext):
                for core in range(2):
                    for e in range(ZE):
                        ref[core, e, at:at + T] = jnp.zeros((T, X), jnp.float32)
    for load in loads:
        load.wait()

    def rough():
        lane = lax.broadcasted_iota(jnp.int32, (Y, X), 1)
        row = lax.broadcasted_iota(jnp.int32, (Y, X), 0)

        def apply(own, z):
            here = own(z)
            total = (jnp.where(row == 0, 0.0, pltpu.roll(here, 1, 0))
                     + jnp.where(row == Y - 1, 0.0, pltpu.roll(here, Y - 1, 0))
                     + jnp.where(lane == 0, 0.0, pltpu.roll(here, 1, 1))
                     + jnp.where(lane == X - 1, 0.0, pltpu.roll(here, X - 1, 1)))
            for beside in (z - 1, z + 1):
                if 0 <= beside < Z:
                    total = total + own(beside)
            return ext[slab, first_plane + z, inside] * here - total

        start = lambda z: cells[0, slab, first_plane + z, inside]
        once = lambda z: out_ref[0, z]
        sums = [jnp.zeros((T, X), jnp.float32)] * 5
        for z in range(Z):
            out_ref[0, z] = apply(start, z)
        for z in range(Z):
            zero, one, two = start(z), once(z), apply(once, z)
            for i, (u, v) in enumerate(((zero, zero), (zero, one), (one, one), (one, two), (two, two))):
                sums[i] = sums[i] + fold(u * v)
        return sums

    share(0, rough())
    pl.semaphore_wait(barrier, n - 1)

    to_others(lambda target: stat_copy(0, target).start())
    for array in (VECTOR, POTENTIAL):
        near_copy(array).start()
    planes(1, True, start_plane)
    sides(True, lambda array, t, step: side_copy(array, t, step, slab).start())
    for w in range(2, D + 1):
        planes(w, True, start_plane)

    m0, m1, m2, m3, m4 = gathered(0, 5)
    some = m0 > 1e-30
    over = 1.0 / jnp.where(some, m0, 1.0)
    m1, m2, m3, m4 = m1 * over, m2 * over, m3 * over, m4 * over
    c2 = m2 - m1 * m1
    c3 = m3 - 3.0 * m1 * m2 + 2.0 * m1 * m1 * m1
    c4 = m4 - 4.0 * m1 * m3 + 6.0 * m1 * m1 * m2 - 3.0 * m1 * m1 * m1 * m1
    down = 1.0 / jnp.maximum(c2, 1e-3)
    slope = c3 * down
    bound = lambda value, low, high: jnp.minimum(jnp.maximum(value, low), high)
    alpha = [bound(jnp.where(some, DIAGONAL + a, CENTER), LEAST_SHIFT, MOST_SHIFT) for a in (m1, m1 + slope)]
    square = [bound(b, LEAST_SQUARE, MOST_SQUARE) for b in (c2, c4 * down - c2 - slope * slope)]
    shifts = [alpha[0]] + [alpha[1]] * (D - 1)
    taus = [None, square[0]] + [square[1]] * (D - 2)

    lane = lax.broadcasted_iota(jnp.int32, (YE, X), 1)
    low_rows, high_rows = (py > 0).astype(jnp.float32), (py < A - 1).astype(jnp.float32)

    def level(l, e):
        left, right = cells[l - 1, 0, e], cells[l - 1, 1, e]
        up = [pltpu.roll(v, 1, 1) for v in (left, right)]
        down = [pltpu.roll(v, X - 1, 1) for v in (left, right)]
        along = (jnp.where(lane == 0, 0.0, up[0]) + jnp.where(lane == X - 1, down[1], down[0]),
                 jnp.where(lane == 0, up[0], up[1]) + jnp.where(lane == X - 1, 0.0, down[1]))
        for core, here in enumerate((left, right)):
            around = (cells[l - 1, core, e - 1] + cells[l - 1, core, e + 1]
                      + (pltpu.roll(here, 1, 0) + pltpu.roll(here, YE - 1, 0)) + along[core])
            image = ((DIAGONAL - shifts[l - 1]) + ext[core, e]) * here - around
            if taus[l - 1] is not None:
                image = image - taus[l - 1] * cells[l - 2, core, e]
            if not D <= e < D + H:
                image = image * present[e].astype(jnp.float32)
            cells[l, core, e, inside] = image[T:T + Y]
            if l < D:
                cells[l, core, e, 0:T] = image[0:T] * low_rows
                cells[l, core, e, T + Y:YE] = image[T + Y:YE] * high_rows

    def measure(pairs):
        sums = [jnp.zeros((T, X), jnp.float32)] * len(pairs)
        for core in range(2):
            for e in range(D, D + H):
                held = {k: cells[k, core, e, inside] for k in sorted({k for pair in pairs for k in pair})}
                for i, (k, l) in enumerate(pairs):
                    sums[i] = sums[i] + fold(held[k] * held[l])
        return sums

    for array in (VECTOR, POTENTIAL):
        near_arrival(array).wait_recv()
    sides(False, lambda array, core, step: side_arrival(array, core, step).wait_recv())
    early = [(k, l) for l in range(D) for k in range(l + 1)]
    late = [(k, D) for k in range(D + 1)]
    for w in range(D + 1):
        if w:
            planes(w, False, take_plane)
        for l in range(1, D + 1):
            for e in range(l, ZE - l):
                if l + max(D - e, e - (D + H - 1)) == w:
                    level(l, e)
        if 1 <= w:
            swap_copy(w).start()
        if w == D - 1:
            sums = measure(early)
    sums = sums + measure(late)
    share(1, sums)
    to_others(lambda target: stat_copy(1, target).start())
    stats = gathered(1, len(sums))
    scale = 1.0 / jnp.sqrt(stats[0] + EPSILON)
    inner = {}
    for (k, l), value in zip(early + late, stats):
        inner[k, l] = inner[l, k] = value * scale * scale
    removed, betas = [], []
    found = advance(D, inner, shifts, taus, removed, betas)
    for v in range(D):
        tri_ref[0:1, v:v + 1] = removed[v][v][:, 0:1]
        tri_ref[1:2, v:v + 1] = betas[v][:, 0:1]
    found = [{q: t * scale for q, t in coords.items()} for coords in found]

    for l in range(1, D + 1):
        swap_copy(l).wait_recv()
    for half in range(2):
        for i in range(H):
            if half == 0:
                z = slab * H + i
                columns = [cells[q, slab, D + i, inside] for q in range(D + 1)]
            else:
                z = (1 - slab) * H + i
                columns = [cells[0, slab, first_plane + z, inside]] + [swapped[q, i] for q in range(D)]
            out_ref[0, z] = columns[0] * scale
            for k, coords in enumerate(found):
                total = None
                for q in sorted(coords, reverse=True):
                    term = coords[q] * columns[q]
                    total = term if total is None else total + term
                out_ref[k + 1, z] = total

    for array in (VECTOR, POTENTIAL):
        near_copy(array).wait_send()
    sides(True, lambda array, t, step: side_copy(array, t, step, slab).wait_send())
    for w in range(1, D + 1):
        planes(w, True, finish_plane)
    for l in range(1, D + 1):
        swap_copy(l).wait_send()
    for p in range(2):
        wait_all(p, stat_send.at[p])


def write_out(basis_ref, tri_ref, basis_out, tri_out, sems):
    copies = (pltpu.make_async_copy(basis_ref, basis_out, sems.at[0]),
              pltpu.make_async_copy(tri_ref, tri_out, sems.at[1]))
    for copy in copies:
        copy.start()
    for copy in copies:
        copy.wait()


def shards(sizes, start_vector, potential):
    Z, Y, X = start_vector.shape
    n = sizes[0] * sizes[1] * sizes[2]
    f32 = jnp.float32
    H, D, T = Z // 2, ITERS, SUBLANES
    assert sizes[0] == 2 and Z % 2 == 0 and H <= D and Y >= D and Y % T == 0
    vmem = pl.BlockSpec(memory_space=pltpu.VMEM)
    hbm = pl.BlockSpec(memory_space=pl.ANY)
    dma = pltpu.SemaphoreType.DMA
    extended = (2, H + 2 * D, Y + 2 * T, X)
    basis, tri = pl.pallas_call(
        functools.partial(kernel, sizes, 1.0 / (start_vector.size * n)),
        out_shape=(pltpu.VMEM((D + 1, Z, Y, X), f32), pltpu.VMEM((2, D), f32)),
        in_specs=[hbm, hbm],
        out_specs=(vmem, vmem),
        scratch_shapes=[
            pltpu.VMEM((D + 1,) + extended, f32),
            pltpu.VMEM(extended, f32),
            pltpu.VMEM((D, H, Y, X), f32),
            pltpu.VMEM((2, n, 1, X), f32),
            dma((2 * 2 * D * 3, 2)),
            dma((2 * 2 * D * 3, 2)),
            dma((2, 2, 2)),
            dma((2, 2, 2)),
            dma((2,)),
            dma((2,)),
            dma((D,)),
            dma((D,)),
            dma((2,)),
            dma((2,)),
            dma((2,)),
        ],
        compiler_params=pltpu.CompilerParams(collective_id=0, has_side_effects=True),
    )(start_vector, potential)
    return tuple(pl.pallas_call(
        write_out,
        out_shape=(jax.ShapeDtypeStruct(basis.shape, f32), jax.ShapeDtypeStruct(tri.shape, f32)),
        in_specs=[vmem, vmem],
        out_specs=(hbm, hbm),
        scratch_shapes=[dma((2,))],
    )(pltpu.with_memory_space_constraint(basis, pltpu.VMEM), pltpu.with_memory_space_constraint(tri, pltpu.VMEM)))


def solution(mesh):
    sizes = tuple(mesh.shape[name] for name in AXES)
    in_specs = (P("pz", "py", "slab"), P("pz", "py", "slab"))
    out_specs = (P(None, "pz", "py", "slab"), P())
    return jax.shard_map(functools.partial(shards, sizes), mesh=mesh, in_specs=in_specs,
                         out_specs=out_specs, check_vma=False)
```

```python
import functools

import jax
import jax.numpy as jnp
from jax import lax
from jax.experimental import pallas as pl
from jax.experimental.pallas import tpu as pltpu
from jax.sharding import PartitionSpec as P

ITERS = 5
EPSILON = 1e-06
DIAGONAL = 6.0
SUBLANES = 8
MESH = pl.DeviceIdType.MESH
AXES = ("slab", "py", "pz")
UNROLLED = 64
CENTER = 8.25
LEAST_SQUARE, MOST_SQUARE = 0.25, 40.0
LEAST_SHIFT, MOST_SHIFT = 0.5, 16.5
VECTOR, POTENTIAL = 0, 1
RELAY_RING, RELAY_WAVE = 4, 4


def times(coeff, columns):
    total = {}
    for k, c in coeff.items():
        for q, value in columns[k].items():
            term = c * value
            total[q] = total[q] + term if q in total else term
    return total


def dot(left, right):
    total = None
    for q, value in left.items():
        if q in right:
            term = value * right[q]
            total = term if total is None else total + term
    return 0.0 if total is None else total


def advance(steps, inner, shifts, taus, removed, betas):
    vectors = [{0: 1.0}]
    image_of = []
    for i in range(steps):
        column = {i + 1: 1.0, i: shifts[i]}
        if taus[i] is not None:
            column[i - 1] = taus[i]
        image_of.append(column)
    gram, lowered = {}, []
    for n in range(steps):
        for k in range(len(lowered), n + 1):
            lowered.append({
                q: dot(vectors[k], {b: inner[q, b] for b in vectors[k]})
                for q in range(n + 1)})
            for l in range(k + 1):
                gram[k, l] = gram[l, k] = dot(vectors[l], lowered[k])
        known = {n: shifts[n]}
        if n > 0:
            known[n - 1] = betas[n - 1]
            rest = times(vectors[n], image_of)
            for k, y in known.items():
                for q, value in vectors[k].items():
                    rest[q] = rest[q] - y * value if q in rest else -y * value
        else:
            rest = {n + 1: 1.0}
        rest_lowered = {
            q: dot(rest, {b: inner[q, b] for b in rest}) for q in range(n + 2)}
        along = {k: dot(vectors[k], rest_lowered) for k in range(n + 1)}
        first = {
            k: along[k] + dot(known, {l: gram[k, l] for l in known}) for k in range(n + 1)}
        excess = {k: first[k] - known[k] if k in known else first[k] for k in range(n + 1)}
        coeffs = {
            k: along[k] - dot(excess, {
                l: gram[k, l] - 1.0 if k == l else gram[k, l] for l in range(n + 1)})
            for k in range(n + 1)}
        square = dot(rest, rest_lowered)
        for k in range(n + 1):
            back = dot(coeffs, {l: gram[k, l] for l in range(n + 1)})
            square = square + coeffs[k] * (back - 2.0 * along[k])
        beta = jnp.sqrt(jnp.maximum(square, 0.0) + EPSILON)
        inverse = 1.0 / beta
        image = dict(rest)
        for k in range(n + 1):
            for q, value in vectors[k].items():
                term = coeffs[k] * value
                image[q] = image[q] - term if q in image else -term
        vectors.append({q: value * inverse for q, value in image.items()})
        removed.append({k: coeffs[k] + known[k] if k in known else coeffs[k] for k in coeffs})
        betas.append(beta)
    return vectors[1:]


def kernel(sizes, per_cell, x_hbm, pot_hbm, out_ref, tri_ref, cells, ext, swapped, relayed, slots,
           send_sem, recv_sem, relay_send, relay_recv, onward_send, side_send, side_recv, near_send, near_recv, swap_send, swap_recv,
           stat_send, stat_recv, load_sem):
    Z, Y, X = x_hbm.shape
    S, A, B = sizes
    n = S * A * B
    H = Z // 2
    D = ITERS
    T = SUBLANES
    ZE, YE = H + 2 * D, Y + 2 * T
    slab, py, pz = (lax.axis_index(name) for name in AXES)
    me = (slab * A + py) * B + pz
    partner = (1 - slab, py, pz)
    first_plane = D - slab * H
    inside = pl.ds(T, Y)

    def to_others(act):
        if n <= UNROLLED:
            slabs = [lax.rem(slab + i, S) for i in range(S)]
            pys = [lax.rem(py + i, A) for i in range(A)]
            pzs = [lax.rem(pz + i, B) for i in range(B)]
            far = sorted(
                ((i, j, k) for i in range(S) for j in range(A) for k in range(B)),
                key=lambda t: -(min(t[1], A - t[1]) + min(t[2], B - t[2])),
            )
            for i, j, k in far:
                if i or j or k:
                    act((slabs[i], pys[j], pzs[k]))
        else:
            def step(d, carry):
                t = lax.rem(me + d, n)
                act((t // (A * B), lax.rem(t // B, A), lax.rem(t, B)))
                return carry
            lax.fori_loop(1, n, step, 0)

    def source(array):
        return cells.at[0] if array == VECTOR else ext

    def remote(src, dst, sent, received, target):
        return pltpu.make_async_remote_copy(
            src_ref=src, dst_ref=dst, send_sem=sent, recv_sem=received,
            device_id=target, device_id_type=MESH)

    def reach(array):
        return D if array == VECTOR else D - 1

    def within(step, position, size):
        if step == 0:
            return None
        return position + step >= 0 if step < 0 else position + step < size

    def guarded(conditions, act):
        conditions = [c for c in conditions if c is not None]
        if not conditions:
            act()
        else:
            pl.when(functools.reduce(jnp.logical_and, conditions))(act)

    def plane_of(t, side, d):
        z = t * H - d if side == 0 else t * H + H - 1 + d
        return z // Z, z % Z

    def lands(side, d):
        return D - d if side == 0 else D + H - 1 + d

    def rows(step, count, sending):
        if step == 0:
            return inside
        if step < 0:
            return pl.ds(T + Y - count, count) if sending else pl.ds(T - count, count)
        return pl.ds(T, count) if sending else pl.ds(T + Y, count)

    def index(array, side, d, step):
        return ((array * 2 + side) * D + d - 1) * 3 + step + 1

    def plane_copy(array, t, side, d, step, core):
        q, z = plane_of(t, side, d)
        count = reach(array) - d
        ref = source(array)
        i = index(array, side, d, step)
        return remote(
            ref.at[core, z + first_plane, rows(step, count, True)],
            ref.at[core, lands(side, d), rows(step, count, False)],
            send_sem.at[i, t], recv_sem.at[i, core], (t, py - step, pz - q))

    relays = [(a, d) for w in range(RELAY_WAVE, D + 1) for a, d in ((VECTOR, w), (POTENTIAL, w - 1))] if (
        B == RELAY_RING and plane_of(0, 0, D)[0] == -1) else []

    def relay_copy(k, t):
        array, d = relays[k]
        z = plane_of(t, t, d)[1]
        return remote(source(array).at[slab, z + first_plane, inside], relayed.at[k],
                      relay_send.at[k], relay_recv.at[k], (slab, py, B - 1 if t == 0 else 0))

    def onward_copy(k, t):
        array, d = relays[k]
        return remote(relayed.at[k], source(array).at[slab, lands(t, d), inside], onward_send.at[k],
                      recv_sem.at[index(array, t, d, 0), slab], (t, py, B - 2 if t == 0 else 1))

    def each_relay(at, act):
        for t in range(2):
            if relays:
                @pl.when(pz == at[t])
                def _(t=t):
                    for k in range(len(relays)):
                        act(k, t)

    def planes(w, sending, act):
        for t in range(2):
            for side in range(2):
                wanted = [(array, d) for array, d in ((VECTOR, w), (POTENTIAL, w - 1))
                          if 1 <= d <= reach(array) and plane_of(t, side, d)[0] != 0]
                for q in sorted({plane_of(t, side, d)[0] for _, d in wanted}, key=abs):
                    mine = [(a, d) for a, d in wanted if plane_of(t, side, d)[0] == q]
                    sign = -1 if sending else 1
                    own = None if sending else slab == t

                    def straight(t=t, side=side, mine=mine):
                        for array, d in mine:
                            act(array, t, side, d, 0)

                    direct = None
                    if sending and t == side and set(mine) & set(relays):
                        direct = pz != 1 + t
                    guarded([own, within(sign * q, pz, B), direct], straight)
                    for step in (-1, 1):
                        beside = [(a, d) for a, d in mine if reach(a) > d]
                        if beside:
                            def corner(t=t, side=side, beside=beside, step=step):
                                for array, d in beside:
                                    act(array, t, side, d, step)

                            guarded([own, within(sign * q, pz, B), within(sign * step, py, A)], corner)

    def start_plane(*key):
        plane_copy(*key, slab).start()

    def finish_plane(*key):
        plane_copy(*key, slab).wait_send()

    def take_plane(*key):
        for core in range(2):
            plane_copy(*key, core).wait_recv()

    def side_copy(array, t, step, core):
        ref = source(array)
        count = reach(array)
        return remote(
            ref.at[core, pl.ds(first_plane, Z), rows(step, count, True)],
            ref.at[core, pl.ds(D - t * H, Z), rows(step, count, False)],
            side_send.at[array, step > 0 and 1 or 0, t], side_recv.at[array, step > 0 and 1 or 0, core],
            (t, py - step, pz))

    def sides(sending, act):
        for step in (-1, 1):
            def both(step=step):
                for array in (VECTOR, POTENTIAL):
                    for other in range(2):
                        act(array, other, step)
            guarded([within(-step if sending else step, py, A)], both)

    def near_copy(array):
        ref = source(array)
        return remote(
            ref.at[slab, pl.ds(first_plane, Z), inside],
            ref.at[slab, pl.ds(D - (1 - slab) * H, Z), inside],
            near_send.at[array], near_recv.at[array], partner)

    def near_arrival(array):
        ref = source(array)
        span = ref.at[1 - slab, pl.ds(first_plane, Z), inside]
        return remote(span, span, near_send.at[array], near_recv.at[array], partner)

    def side_arrival(array, core, step):
        ref = source(array)
        span = ref.at[core, pl.ds(first_plane, Z), rows(step, reach(array), False)]
        k = step > 0 and 1 or 0
        return remote(span, span, side_send.at[array, k, 0], side_recv.at[array, k, core], partner)

    def swap_copy(level):
        return remote(
            cells.at[level, 1 - slab, pl.ds(D, H), inside], swapped.at[level - 1],
            swap_send.at[level - 1], swap_recv.at[level - 1], partner)

    def stat_copy(p, target):
        return remote(slots.at[p, me], slots.at[p, me], stat_send.at[p], stat_recv.at[p], target)

    def wait_all(p, sem):
        span = slots.at[p, pl.ds(0, n - 1)]
        pltpu.make_async_copy(span, span, sem).wait()

    def fold(value):
        return jnp.sum(value.reshape(value.shape[0] // T, T, X), axis=0)

    def share(p, sums):
        lines = [jnp.sum(v, axis=0, keepdims=True) for v in sums]
        height = -(-len(lines) // T) * T
        lines = lines + [jnp.zeros((1, X), jnp.float32)] * (height - len(lines))
        totals = jnp.sum(jnp.concatenate(lines, axis=0), axis=1, keepdims=True)
        at = lax.broadcasted_iota(jnp.int32, (height, X), 0)
        lanes = lax.broadcasted_iota(jnp.int32, (height, X), 1)
        slots[p, me] = jnp.sum(jnp.where(at == lanes, totals, 0.0), axis=0, keepdims=True)

    def gathered(p, count):
        wait_all(p, stat_recv.at[p])
        total = jnp.sum(slots[p], axis=0) * per_cell
        return [jnp.broadcast_to(total[:, s:s + 1], (1, X)) for s in range(count)]

    barrier = pltpu.get_barrier_semaphore()
    to_others(lambda t: pl.semaphore_signal(barrier, inc=1, device_id=t, device_id_type=MESH))
    loads = [pltpu.make_async_copy(
        hbm, source(array).at[slab, pl.ds(first_plane, Z), inside], load_sem.at[array])
        for array, hbm in ((VECTOR, x_hbm), (POTENTIAL, pot_hbm))]
    for load in loads:
        load.start()

    plane = pz * Z + slab * H - D
    present = [jnp.logical_and(plane + e >= 0, plane + e < B * Z) for e in range(ZE)]
    for e in range(ZE):
        if D <= e < D + H:
            continue
        @pl.when(jnp.logical_not(present[e]))
        def _(e=e):
            for ref in (cells.at[0], ext):
                for core in range(2):
                    ref[core, e] = jnp.zeros((YE, X), jnp.float32)
    for missing, at in ((py == 0, 0), (py == A - 1, T + Y)):
        @pl.when(missing)
        def _(at=at):
            for ref in (cells.at[0], ext):
                for core in range(2):
                    for e in range(ZE):
                        ref[core, e, at:at + T] = jnp.zeros((T, X), jnp.float32)
    for load in loads:
        load.wait()

    def rough():
        lane = lax.broadcasted_iota(jnp.int32, (Y, X), 1)
        row = lax.broadcasted_iota(jnp.int32, (Y, X), 0)

        def apply(own, z):
            here = own(z)
            total = (jnp.where(row == 0, 0.0, pltpu.roll(here, 1, 0))
                     + jnp.where(row == Y - 1, 0.0, pltpu.roll(here, Y - 1, 0))
                     + jnp.where(lane == 0, 0.0, pltpu.roll(here, 1, 1))
                     + jnp.where(lane == X - 1, 0.0, pltpu.roll(here, X - 1, 1)))
            for beside in (z - 1, z + 1):
                if 0 <= beside < Z:
                    total = total + own(beside)
            return ext[slab, first_plane + z, inside] * here - total

        start = lambda z: cells[0, slab, first_plane + z, inside]
        once = lambda z: out_ref[0, z]
        sums = [jnp.zeros((T, X), jnp.float32)] * 5
        for z in range(Z):
            out_ref[0, z] = apply(start, z)
        for z in range(Z):
            zero, one, two = start(z), once(z), apply(once, z)
            for i, (u, v) in enumerate(((zero, zero), (zero, one), (one, one), (one, two), (two, two))):
                sums[i] = sums[i] + fold(u * v)
        return sums

    share(0, rough())
    pl.semaphore_wait(barrier, n - 1)

    to_others(lambda target: stat_copy(0, target).start())
    each_relay((1, 2), lambda k, t: relay_copy(k, t).start())
    for array in (VECTOR, POTENTIAL):
        near_copy(array).start()
    planes(1, True, start_plane)
    sides(True, lambda array, t, step: side_copy(array, t, step, slab).start())
    for w in range(2, D + 1):
        planes(w, True, start_plane)

    def forward(k, t):
        relay_copy(k, t).wait_recv()
        onward_copy(k, t).start()

    each_relay((B - 1, 0), forward)

    m0, m1, m2, m3, m4 = gathered(0, 5)
    some = m0 > 1e-30
    over = 1.0 / jnp.where(some, m0, 1.0)
    m1, m2, m3, m4 = m1 * over, m2 * over, m3 * over, m4 * over
    c2 = m2 - m1 * m1
    c3 = m3 - 3.0 * m1 * m2 + 2.0 * m1 * m1 * m1
    c4 = m4 - 4.0 * m1 * m3 + 6.0 * m1 * m1 * m2 - 3.0 * m1 * m1 * m1 * m1
    down = 1.0 / jnp.maximum(c2, 1e-3)
    slope = c3 * down
    bound = lambda value, low, high: jnp.minimum(jnp.maximum(value, low), high)
    alpha = [bound(jnp.where(some, DIAGONAL + a, CENTER), LEAST_SHIFT, MOST_SHIFT) for a in (m1, m1 + slope)]
    square = [bound(b, LEAST_SQUARE, MOST_SQUARE) for b in (c2, c4 * down - c2 - slope * slope)]
    shifts = [alpha[0]] + [alpha[1]] * (D - 1)
    taus = [None, square[0]] + [square[1]] * (D - 2)

    lane = lax.broadcasted_iota(jnp.int32, (YE, X), 1)
    low_rows, high_rows = (py > 0).astype(jnp.float32), (py < A - 1).astype(jnp.float32)

    def level(l, e):
        left, right = cells[l - 1, 0, e], cells[l - 1, 1, e]
        up = [pltpu.roll(v, 1, 1) for v in (left, right)]
        down = [pltpu.roll(v, X - 1, 1) for v in (left, right)]
        along = (jnp.where(lane == 0, 0.0, up[0]) + jnp.where(lane == X - 1, down[1], down[0]),
                 jnp.where(lane == 0, up[0], up[1]) + jnp.where(lane == X - 1, 0.0, down[1]))
        for core, here in enumerate((left, right)):
            around = (cells[l - 1, core, e - 1] + cells[l - 1, core, e + 1]
                      + (pltpu.roll(here, 1, 0) + pltpu.roll(here, YE - 1, 0)) + along[core])
            image = ((DIAGONAL - shifts[l - 1]) + ext[core, e]) * here - around
            if taus[l - 1] is not None:
                image = image - taus[l - 1] * cells[l - 2, core, e]
            if not D <= e < D + H:
                image = image * present[e].astype(jnp.float32)
            cells[l, core, e, inside] = image[T:T + Y]
            if l < D:
                cells[l, core, e, 0:T] = image[0:T] * low_rows
                cells[l, core, e, T + Y:YE] = image[T + Y:YE] * high_rows

    def measure(pairs):
        sums = [jnp.zeros((T, X), jnp.float32)] * len(pairs)
        for core in range(2):
            for e in range(D, D + H):
                held = {k: cells[k, core, e, inside] for k in sorted({k for pair in pairs for k in pair})}
                for i, (k, l) in enumerate(pairs):
                    sums[i] = sums[i] + fold(held[k] * held[l])
        return sums

    for array in (VECTOR, POTENTIAL):
        near_arrival(array).wait_recv()
    sides(False, lambda array, core, step: side_arrival(array, core, step).wait_recv())
    early = [(k, l) for l in range(D) for k in range(l + 1)]
    late = [(k, D) for k in range(D + 1)]
    for w in range(D + 1):
        if w:
            planes(w, False, take_plane)
        for l in range(1, D + 1):
            for e in range(l, ZE - l):
                if l + max(D - e, e - (D + H - 1)) == w:
                    level(l, e)
        if 1 <= w:
            swap_copy(w).start()
        if w == D - 1:
            sums = measure(early)
    sums = sums + measure(late)
    share(1, sums)
    to_others(lambda target: stat_copy(1, target).start())
    stats = gathered(1, len(sums))
    scale = 1.0 / jnp.sqrt(stats[0] + EPSILON)
    inner = {}
    for (k, l), value in zip(early + late, stats):
        inner[k, l] = inner[l, k] = value * scale * scale
    removed, betas = [], []
    found = advance(D, inner, shifts, taus, removed, betas)
    for v in range(D):
        tri_ref[0:1, v:v + 1] = removed[v][v][:, 0:1]
        tri_ref[1:2, v:v + 1] = betas[v][:, 0:1]
    found = [{q: t * scale for q, t in coords.items()} for coords in found]

    for l in range(1, D + 1):
        swap_copy(l).wait_recv()
    for half in range(2):
        for i in range(H):
            if half == 0:
                z = slab * H + i
                columns = [cells[q, slab, D + i, inside] for q in range(D + 1)]
            else:
                z = (1 - slab) * H + i
                columns = [cells[0, slab, first_plane + z, inside]] + [swapped[q, i] for q in range(D)]
            out_ref[0, z] = columns[0] * scale
            for k, coords in enumerate(found):
                total = None
                for q in sorted(coords, reverse=True):
                    term = coords[q] * columns[q]
                    total = term if total is None else total + term
                out_ref[k + 1, z] = total

    for array in (VECTOR, POTENTIAL):
        near_copy(array).wait_send()
    sides(True, lambda array, t, step: side_copy(array, t, step, slab).wait_send())
    each_relay((1, 2), lambda k, t: relay_copy(k, t).wait_send())
    each_relay((B - 1, 0), lambda k, t: onward_copy(k, t).wait_send())
    for w in range(1, D + 1):
        planes(w, True, finish_plane)
    for l in range(1, D + 1):
        swap_copy(l).wait_send()
    for p in range(2):
        wait_all(p, stat_send.at[p])


def write_out(basis_ref, tri_ref, basis_out, tri_out, sems):
    copies = (pltpu.make_async_copy(basis_ref, basis_out, sems.at[0]),
              pltpu.make_async_copy(tri_ref, tri_out, sems.at[1]))
    for copy in copies:
        copy.start()
    for copy in copies:
        copy.wait()


def shards(sizes, start_vector, potential):
    Z, Y, X = start_vector.shape
    n = sizes[0] * sizes[1] * sizes[2]
    f32 = jnp.float32
    H, D, T = Z // 2, ITERS, SUBLANES
    assert sizes[0] == 2 and Z % 2 == 0 and H <= D and Y >= D and Y % T == 0
    vmem = pl.BlockSpec(memory_space=pltpu.VMEM)
    hbm = pl.BlockSpec(memory_space=pl.ANY)
    dma = pltpu.SemaphoreType.DMA
    extended = (2, H + 2 * D, Y + 2 * T, X)
    basis, tri = pl.pallas_call(
        functools.partial(kernel, sizes, 1.0 / (start_vector.size * n)),
        out_shape=(pltpu.VMEM((D + 1, Z, Y, X), f32), pltpu.VMEM((2, D), f32)),
        in_specs=[hbm, hbm],
        out_specs=(vmem, vmem),
        scratch_shapes=[
            pltpu.VMEM((D + 1,) + extended, f32),
            pltpu.VMEM(extended, f32),
            pltpu.VMEM((D, H, Y, X), f32),
            pltpu.VMEM((2 * (D + 1 - RELAY_WAVE), Y, X), f32),
            pltpu.VMEM((2, n, 1, X), f32),
            dma((2 * 2 * D * 3, 2)),
            dma((2 * 2 * D * 3, 2)),
            dma((2 * (D + 1 - RELAY_WAVE),)),
            dma((2 * (D + 1 - RELAY_WAVE),)),
            dma((2 * (D + 1 - RELAY_WAVE),)),
            dma((2, 2, 2)),
            dma((2, 2, 2)),
            dma((2,)),
            dma((2,)),
            dma((D,)),
            dma((D,)),
            dma((2,)),
            dma((2,)),
            dma((2,)),
        ],
        compiler_params=pltpu.CompilerParams(collective_id=0, has_side_effects=True),
    )(start_vector, potential)
    return tuple(pl.pallas_call(
        write_out,
        out_shape=(jax.ShapeDtypeStruct(basis.shape, f32), jax.ShapeDtypeStruct(tri.shape, f32)),
        in_specs=[vmem, vmem],
        out_specs=(hbm, hbm),
        scratch_shapes=[dma((2,))],
    )(pltpu.with_memory_space_constraint(basis, pltpu.VMEM), pltpu.with_memory_space_constraint(tri, pltpu.VMEM)))


def solution(mesh):
    sizes = tuple(mesh.shape[name] for name in AXES)
    in_specs = (P("pz", "py", "slab"), P("pz", "py", "slab"))
    out_specs = (P(None, "pz", "py", "slab"), P())
    return jax.shard_map(functools.partial(shards, sizes), mesh=mesh, in_specs=in_specs,
                         out_specs=out_specs, check_vma=False)
```

```python
import functools

import jax
import jax.numpy as jnp
from jax import lax
from jax.experimental import pallas as pl
from jax.experimental.pallas import tpu as pltpu
from jax.sharding import PartitionSpec as P

ITERS = 5
EPSILON = 1e-06
DIAGONAL = 6.0
SUBLANES = 8
MESH = pl.DeviceIdType.MESH
AXES = ("slab", "py", "pz")
UNROLLED = 64
CENTER = 8.25
LEAST_SQUARE, MOST_SQUARE = 0.25, 40.0
LEAST_SHIFT, MOST_SHIFT = 0.5, 16.5
VECTOR, POTENTIAL = 0, 1
RELAY_RING, RELAYED = 4, 5


def times(coeff, columns):
    total = {}
    for k, c in coeff.items():
        for q, value in columns[k].items():
            term = c * value
            total[q] = total[q] + term if q in total else term
    return total


def dot(left, right):
    total = None
    for q, value in left.items():
        if q in right:
            term = value * right[q]
            total = term if total is None else total + term
    return 0.0 if total is None else total


def advance(steps, inner, shifts, taus, removed, betas):
    vectors = [{0: 1.0}]
    image_of = []
    for i in range(steps):
        column = {i + 1: 1.0, i: shifts[i]}
        if taus[i] is not None:
            column[i - 1] = taus[i]
        image_of.append(column)
    gram, lowered = {}, []
    for n in range(steps):
        for k in range(len(lowered), n + 1):
            lowered.append({
                q: dot(vectors[k], {b: inner[q, b] for b in vectors[k]})
                for q in range(n + 1)})
            for l in range(k + 1):
                gram[k, l] = gram[l, k] = dot(vectors[l], lowered[k])
        known = {n: shifts[n]}
        if n > 0:
            known[n - 1] = betas[n - 1]
            rest = times(vectors[n], image_of)
            for k, y in known.items():
                for q, value in vectors[k].items():
                    rest[q] = rest[q] - y * value if q in rest else -y * value
        else:
            rest = {n + 1: 1.0}
        rest_lowered = {
            q: dot(rest, {b: inner[q, b] for b in rest}) for q in range(n + 2)}
        along = {k: dot(vectors[k], rest_lowered) for k in range(n + 1)}
        first = {
            k: along[k] + dot(known, {l: gram[k, l] for l in known}) for k in range(n + 1)}
        excess = {k: first[k] - known[k] if k in known else first[k] for k in range(n + 1)}
        coeffs = {
            k: along[k] - dot(excess, {
                l: gram[k, l] - 1.0 if k == l else gram[k, l] for l in range(n + 1)})
            for k in range(n + 1)}
        square = dot(rest, rest_lowered)
        for k in range(n + 1):
            back = dot(coeffs, {l: gram[k, l] for l in range(n + 1)})
            square = square + coeffs[k] * (back - 2.0 * along[k])
        beta = jnp.sqrt(jnp.maximum(square, 0.0) + EPSILON)
        inverse = 1.0 / beta
        image = dict(rest)
        for k in range(n + 1):
            for q, value in vectors[k].items():
                term = coeffs[k] * value
                image[q] = image[q] - term if q in image else -term
        vectors.append({q: value * inverse for q, value in image.items()})
        removed.append({k: coeffs[k] + known[k] if k in known else coeffs[k] for k in coeffs})
        betas.append(beta)
    return vectors[1:]


def kernel(sizes, per_cell, x_hbm, pot_hbm, out_ref, tri_ref, cells, ext, swapped, relayed, slots,
           send_sem, recv_sem, relay_send, relay_recv, onward_send, side_send, side_recv, near_send, near_recv, swap_send, swap_recv,
           stat_send, stat_recv, load_sem):
    Z, Y, X = x_hbm.shape
    S, A, B = sizes
    n = S * A * B
    H = Z // 2
    D = ITERS
    T = SUBLANES
    ZE, YE = H + 2 * D, Y + 2 * T
    slab, py, pz = (lax.axis_index(name) for name in AXES)
    me = (slab * A + py) * B + pz
    partner = (1 - slab, py, pz)
    first_plane = D - slab * H
    inside = pl.ds(T, Y)

    def to_others(act):
        if n <= UNROLLED:
            slabs = [lax.rem(slab + i, S) for i in range(S)]
            pys = [lax.rem(py + i, A) for i in range(A)]
            pzs = [lax.rem(pz + i, B) for i in range(B)]
            far = sorted(
                ((i, j, k) for i in range(S) for j in range(A) for k in range(B)),
                key=lambda t: -(min(t[1], A - t[1]) + min(t[2], B - t[2])),
            )
            for i, j, k in far:
                if i or j or k:
                    act((slabs[i], pys[j], pzs[k]))
        else:
            def step(d, carry):
                t = lax.rem(me + d, n)
                act((t // (A * B), lax.rem(t // B, A), lax.rem(t, B)))
                return carry
            lax.fori_loop(1, n, step, 0)

    def source(array):
        return cells.at[0] if array == VECTOR else ext

    def remote(src, dst, sent, received, target):
        return pltpu.make_async_remote_copy(
            src_ref=src, dst_ref=dst, send_sem=sent, recv_sem=received,
            device_id=target, device_id_type=MESH)

    def reach(array):
        return D if array == VECTOR else D - 1

    def within(step, position, size):
        if step == 0:
            return None
        return position + step >= 0 if step < 0 else position + step < size

    def guarded(conditions, act):
        conditions = [c for c in conditions if c is not None]
        if not conditions:
            act()
        else:
            pl.when(functools.reduce(jnp.logical_and, conditions))(act)

    def plane_of(t, side, d):
        z = t * H - d if side == 0 else t * H + H - 1 + d
        return z // Z, z % Z

    def lands(side, d):
        return D - d if side == 0 else D + H - 1 + d

    def rows(step, count, sending):
        if step == 0:
            return inside
        if step < 0:
            return pl.ds(T + Y - count, count) if sending else pl.ds(T - count, count)
        return pl.ds(T, count) if sending else pl.ds(T + Y, count)

    def index(array, side, d, step):
        return ((array * 2 + side) * D + d - 1) * 3 + step + 1

    def plane_copy(array, t, side, d, step, core):
        q, z = plane_of(t, side, d)
        count = reach(array) - d
        ref = source(array)
        i = index(array, side, d, step)
        return remote(
            ref.at[core, z + first_plane, rows(step, count, True)],
            ref.at[core, lands(side, d), rows(step, count, False)],
            send_sem.at[i, t], recv_sem.at[i, core], (t, py - step, pz - q))

    order = [(a, d) for w in range(1, D + 1) for a, d in ((VECTOR, w), (POTENTIAL, w - 1)) if d]
    relays = order[-RELAYED:] if B == RELAY_RING and plane_of(0, 0, D)[0] == -1 else []

    def relay_copy(k, t):
        array, d = relays[k]
        z = plane_of(t, t, d)[1]
        return remote(source(array).at[slab, z + first_plane, inside], relayed.at[k],
                      relay_send.at[k], relay_recv.at[k], (slab, py, B - 1 if t == 0 else 0))

    def onward_copy(k, t):
        array, d = relays[k]
        return remote(relayed.at[k], source(array).at[slab, lands(t, d), inside], onward_send.at[k],
                      recv_sem.at[index(array, t, d, 0), slab], (t, py, B - 2 if t == 0 else 1))

    def each_relay(at, act):
        for t in range(2):
            if relays:
                @pl.when(pz == at[t])
                def _(t=t):
                    for k in range(len(relays)):
                        act(k, t)

    def planes(w, sending, act):
        for t in range(2):
            for side in range(2):
                wanted = [(array, d) for array, d in ((VECTOR, w), (POTENTIAL, w - 1))
                          if 1 <= d <= reach(array) and plane_of(t, side, d)[0] != 0]
                for q in sorted({plane_of(t, side, d)[0] for _, d in wanted}, key=abs):
                    mine = [(a, d) for a, d in wanted if plane_of(t, side, d)[0] == q]
                    sign = -1 if sending else 1
                    own = None if sending else slab == t

                    for turned in (False, True):
                        some = [key for key in mine
                                if (sending and t == side and key in relays) == turned]
                        if some:
                            def straight(t=t, side=side, some=some):
                                for array, d in some:
                                    act(array, t, side, d, 0)

                            guarded([own, within(sign * q, pz, B), pz != 1 + t if turned else None], straight)
                    for step in (-1, 1):
                        beside = [(a, d) for a, d in mine if reach(a) > d]
                        if beside:
                            def corner(t=t, side=side, beside=beside, step=step):
                                for array, d in beside:
                                    act(array, t, side, d, step)

                            guarded([own, within(sign * q, pz, B), within(sign * step, py, A)], corner)

    def start_plane(*key):
        plane_copy(*key, slab).start()

    def finish_plane(*key):
        plane_copy(*key, slab).wait_send()

    def take_plane(*key):
        for core in range(2):
            plane_copy(*key, core).wait_recv()

    def side_copy(array, t, step, core):
        ref = source(array)
        count = reach(array)
        return remote(
            ref.at[core, pl.ds(first_plane, Z), rows(step, count, True)],
            ref.at[core, pl.ds(D - t * H, Z), rows(step, count, False)],
            side_send.at[array, step > 0 and 1 or 0, t], side_recv.at[array, step > 0 and 1 or 0, core],
            (t, py - step, pz))

    def sides(sending, act):
        for step in (-1, 1):
            def both(step=step):
                for array in (VECTOR, POTENTIAL):
                    for other in range(2):
                        act(array, other, step)
            guarded([within(-step if sending else step, py, A)], both)

    def near_copy(array):
        ref = source(array)
        return remote(
            ref.at[slab, pl.ds(first_plane, Z), inside],
            ref.at[slab, pl.ds(D - (1 - slab) * H, Z), inside],
            near_send.at[array], near_recv.at[array], partner)

    def near_arrival(array):
        ref = source(array)
        span = ref.at[1 - slab, pl.ds(first_plane, Z), inside]
        return remote(span, span, near_send.at[array], near_recv.at[array], partner)

    def side_arrival(array, core, step):
        ref = source(array)
        span = ref.at[core, pl.ds(first_plane, Z), rows(step, reach(array), False)]
        k = step > 0 and 1 or 0
        return remote(span, span, side_send.at[array, k, 0], side_recv.at[array, k, core], partner)

    def swap_copy(level):
        return remote(
            cells.at[level, 1 - slab, pl.ds(D, H), inside], swapped.at[level - 1],
            swap_send.at[level - 1], swap_recv.at[level - 1], partner)

    def stat_copy(p, target):
        return remote(slots.at[p, me], slots.at[p, me], stat_send.at[p], stat_recv.at[p], target)

    def wait_all(p, sem):
        span = slots.at[p, pl.ds(0, n - 1)]
        pltpu.make_async_copy(span, span, sem).wait()

    def fold(value):
        return jnp.sum(value.reshape(value.shape[0] // T, T, X), axis=0)

    def share(p, sums):
        lines = [jnp.sum(v, axis=0, keepdims=True) for v in sums]
        height = -(-len(lines) // T) * T
        lines = lines + [jnp.zeros((1, X), jnp.float32)] * (height - len(lines))
        totals = jnp.sum(jnp.concatenate(lines, axis=0), axis=1, keepdims=True)
        at = lax.broadcasted_iota(jnp.int32, (height, X), 0)
        lanes = lax.broadcasted_iota(jnp.int32, (height, X), 1)
        slots[p, me] = jnp.sum(jnp.where(at == lanes, totals, 0.0), axis=0, keepdims=True)

    def gathered(p, count):
        wait_all(p, stat_recv.at[p])
        total = jnp.sum(slots[p], axis=0) * per_cell
        return [jnp.broadcast_to(total[:, s:s + 1], (1, X)) for s in range(count)]

    barrier = pltpu.get_barrier_semaphore()
    to_others(lambda t: pl.semaphore_signal(barrier, inc=1, device_id=t, device_id_type=MESH))
    loads = [pltpu.make_async_copy(
        hbm, source(array).at[slab, pl.ds(first_plane, Z), inside], load_sem.at[array])
        for array, hbm in ((VECTOR, x_hbm), (POTENTIAL, pot_hbm))]
    for load in loads:
        load.start()

    plane = pz * Z + slab * H - D
    present = [jnp.logical_and(plane + e >= 0, plane + e < B * Z) for e in range(ZE)]
    for e in range(ZE):
        if D <= e < D + H:
            continue
        @pl.when(jnp.logical_not(present[e]))
        def _(e=e):
            for ref in (cells.at[0], ext):
                for core in range(2):
                    ref[core, e] = jnp.zeros((YE, X), jnp.float32)
    for missing, at in ((py == 0, 0), (py == A - 1, T + Y)):
        @pl.when(missing)
        def _(at=at):
            for ref in (cells.at[0], ext):
                for core in range(2):
                    for e in range(ZE):
                        ref[core, e, at:at + T] = jnp.zeros((T, X), jnp.float32)
    for load in loads:
        load.wait()

    def rough():
        lane = lax.broadcasted_iota(jnp.int32, (Y, X), 1)
        row = lax.broadcasted_iota(jnp.int32, (Y, X), 0)

        def apply(own, z):
            here = own(z)
            total = (jnp.where(row == 0, 0.0, pltpu.roll(here, 1, 0))
                     + jnp.where(row == Y - 1, 0.0, pltpu.roll(here, Y - 1, 0))
                     + jnp.where(lane == 0, 0.0, pltpu.roll(here, 1, 1))
                     + jnp.where(lane == X - 1, 0.0, pltpu.roll(here, X - 1, 1)))
            for beside in (z - 1, z + 1):
                if 0 <= beside < Z:
                    total = total + own(beside)
            return ext[slab, first_plane + z, inside] * here - total

        start = lambda z: cells[0, slab, first_plane + z, inside]
        once = lambda z: out_ref[0, z]
        sums = [jnp.zeros((T, X), jnp.float32)] * 5
        for z in range(Z):
            out_ref[0, z] = apply(start, z)
        for z in range(Z):
            zero, one, two = start(z), once(z), apply(once, z)
            for i, (u, v) in enumerate(((zero, zero), (zero, one), (one, one), (one, two), (two, two))):
                sums[i] = sums[i] + fold(u * v)
        return sums

    share(0, rough())
    pl.semaphore_wait(barrier, n - 1)

    to_others(lambda target: stat_copy(0, target).start())
    each_relay((1, 2), lambda k, t: relay_copy(k, t).start())
    for array in (VECTOR, POTENTIAL):
        near_copy(array).start()
    planes(1, True, start_plane)
    sides(True, lambda array, t, step: side_copy(array, t, step, slab).start())
    for w in range(2, D + 1):
        planes(w, True, start_plane)

    def forward(k, t):
        relay_copy(k, t).wait_recv()
        onward_copy(k, t).start()

    each_relay((B - 1, 0), forward)

    m0, m1, m2, m3, m4 = gathered(0, 5)
    some = m0 > 1e-30
    over = 1.0 / jnp.where(some, m0, 1.0)
    m1, m2, m3, m4 = m1 * over, m2 * over, m3 * over, m4 * over
    c2 = m2 - m1 * m1
    c3 = m3 - 3.0 * m1 * m2 + 2.0 * m1 * m1 * m1
    c4 = m4 - 4.0 * m1 * m3 + 6.0 * m1 * m1 * m2 - 3.0 * m1 * m1 * m1 * m1
    down = 1.0 / jnp.maximum(c2, 1e-3)
    slope = c3 * down
    bound = lambda value, low, high: jnp.minimum(jnp.maximum(value, low), high)
    alpha = [bound(jnp.where(some, DIAGONAL + a, CENTER), LEAST_SHIFT, MOST_SHIFT) for a in (m1, m1 + slope)]
    square = [bound(b, LEAST_SQUARE, MOST_SQUARE) for b in (c2, c4 * down - c2 - slope * slope)]
    shifts = [alpha[0]] + [alpha[1]] * (D - 1)
    taus = [None, square[0]] + [square[1]] * (D - 2)

    lane = lax.broadcasted_iota(jnp.int32, (YE, X), 1)
    low_rows, high_rows = (py > 0).astype(jnp.float32), (py < A - 1).astype(jnp.float32)

    def depth(e):
        return max(D - e, e - (D + H - 1))

    def outer(e):
        return [b for b in (e - 1, e + 1) if depth(b) > depth(e)]

    def prepare(l, e):
        left, right = cells[l - 1, 0, e], cells[l - 1, 1, e]
        up = [pltpu.roll(v, 1, 1) for v in (left, right)]
        down = [pltpu.roll(v, X - 1, 1) for v in (left, right)]
        along = (jnp.where(lane == 0, 0.0, up[0]) + jnp.where(lane == X - 1, down[1], down[0]),
                 jnp.where(lane == 0, up[0], up[1]) + jnp.where(lane == X - 1, 0.0, down[1]))
        for core, here in enumerate((left, right)):
            around = (pltpu.roll(here, 1, 0) + pltpu.roll(here, YE - 1, 0)) + along[core]
            for b in (e - 1, e + 1):
                if b not in outer(e):
                    around = around + cells[l - 1, core, b]
            if l == 1:
                image = -around
            else:
                image = ((DIAGONAL - shifts[l - 1]) + ext[core, e]) * here - around
                image = image - taus[l - 1] * cells[l - 2, core, e]
            cells[l, core, e] = image

    def finish(l, e):
        for core in range(2):
            image = cells[l, core, e]
            for b in outer(e):
                image = image - cells[l - 1, core, b]
            if l == 1:
                image = ((DIAGONAL - shifts[0]) + ext[core, e]) * cells[0, core, e] + image
            if not D <= e < D + H:
                image = image * present[e].astype(jnp.float32)
            cells[l, core, e, inside] = image[T:T + Y]
            if l < D:
                cells[l, core, e, 0:T] = image[0:T] * low_rows
                cells[l, core, e, T + Y:YE] = image[T + Y:YE] * high_rows

    def wave(w):
        return [(l, e) for l in range(1, D + 1) for e in range(l, ZE - l) if max(l + depth(e), 0) == w]

    def measure(pairs, at, sums=None):
        sums = sums or [jnp.zeros((T, X), jnp.float32)] * len(pairs)
        for core in range(2):
            for e in at:
                held = {k: cells[k, core, e, inside] for k in sorted({k for pair in pairs for k in pair})}
                for i, (k, l) in enumerate(pairs):
                    sums[i] = sums[i] + fold(held[k] * held[l])
        return sums

    for array in (VECTOR, POTENTIAL):
        near_arrival(array).wait_recv()
    sides(False, lambda array, core, step: side_arrival(array, core, step).wait_recv())
    early = [(k, l) for l in range(D) for k in range(l + 1)]
    late = [(k, D) for k in range(D + 1)]
    held = range(D, D + H)
    done = [e for e in held if depth(e) < 0]
    for l, e in wave(0):
        prepare(l, e)
        finish(l, e)
    for l, e in wave(1):
        prepare(l, e)
    for w in range(1, D + 1):
        planes(w, False, take_plane)
        for l, e in wave(w):
            finish(l, e)
        swap_copy(w).start()
        if w == D - 1:
            sums = measure(early, held)
            last = measure(late, done)
        if w < D:
            for l, e in wave(w + 1):
                prepare(l, e)
    sums = sums + measure(late, [e for e in held if e not in done], last)
    share(1, sums)
    to_others(lambda target: stat_copy(1, target).start())
    stats = gathered(1, len(sums))
    scale = 1.0 / jnp.sqrt(stats[0] + EPSILON)
    inner = {}
    for (k, l), value in zip(early + late, stats):
        inner[k, l] = inner[l, k] = value * scale * scale
    removed, betas = [], []
    found = advance(D, inner, shifts, taus, removed, betas)
    for v in range(D):
        tri_ref[0:1, v:v + 1] = removed[v][v][:, 0:1]
        tri_ref[1:2, v:v + 1] = betas[v][:, 0:1]
    found = [{q: t * scale for q, t in coords.items()} for coords in found]

    for l in range(1, D + 1):
        swap_copy(l).wait_recv()
    for half in range(2):
        for i in range(H):
            if half == 0:
                z = slab * H + i
                columns = [cells[q, slab, D + i, inside] for q in range(D + 1)]
            else:
                z = (1 - slab) * H + i
                columns = [cells[0, slab, first_plane + z, inside]] + [swapped[q, i] for q in range(D)]
            out_ref[0, z] = columns[0] * scale
            for k, coords in enumerate(found):
                total = None
                for q in sorted(coords, reverse=True):
                    term = coords[q] * columns[q]
                    total = term if total is None else total + term
                out_ref[k + 1, z] = total

    for array in (VECTOR, POTENTIAL):
        near_copy(array).wait_send()
    sides(True, lambda array, t, step: side_copy(array, t, step, slab).wait_send())
    each_relay((1, 2), lambda k, t: relay_copy(k, t).wait_send())
    each_relay((B - 1, 0), lambda k, t: onward_copy(k, t).wait_send())
    for w in range(1, D + 1):
        planes(w, True, finish_plane)
    for l in range(1, D + 1):
        swap_copy(l).wait_send()
    for p in range(2):
        wait_all(p, stat_send.at[p])


def write_out(basis_ref, tri_ref, basis_out, tri_out, sems):
    copies = (pltpu.make_async_copy(basis_ref, basis_out, sems.at[0]),
              pltpu.make_async_copy(tri_ref, tri_out, sems.at[1]))
    for copy in copies:
        copy.start()
    for copy in copies:
        copy.wait()


def shards(sizes, start_vector, potential):
    Z, Y, X = start_vector.shape
    n = sizes[0] * sizes[1] * sizes[2]
    f32 = jnp.float32
    H, D, T = Z // 2, ITERS, SUBLANES
    assert sizes[0] == 2 and Z % 2 == 0 and H <= D and Y >= D and Y % T == 0
    vmem = pl.BlockSpec(memory_space=pltpu.VMEM)
    hbm = pl.BlockSpec(memory_space=pl.ANY)
    dma = pltpu.SemaphoreType.DMA
    extended = (2, H + 2 * D, Y + 2 * T, X)
    basis, tri = pl.pallas_call(
        functools.partial(kernel, sizes, 1.0 / (start_vector.size * n)),
        out_shape=(pltpu.VMEM((D + 1, Z, Y, X), f32), pltpu.VMEM((2, D), f32)),
        in_specs=[hbm, hbm],
        out_specs=(vmem, vmem),
        scratch_shapes=[
            pltpu.VMEM((D + 1,) + extended, f32),
            pltpu.VMEM(extended, f32),
            pltpu.VMEM((D, H, Y, X), f32),
            pltpu.VMEM((RELAYED, Y, X), f32),
            pltpu.VMEM((2, n, 1, X), f32),
            dma((2 * 2 * D * 3, 2)),
            dma((2 * 2 * D * 3, 2)),
            dma((RELAYED,)),
            dma((RELAYED,)),
            dma((RELAYED,)),
            dma((2, 2, 2)),
            dma((2, 2, 2)),
            dma((2,)),
            dma((2,)),
            dma((D,)),
            dma((D,)),
            dma((2,)),
            dma((2,)),
            dma((2,)),
        ],
        compiler_params=pltpu.CompilerParams(collective_id=0, has_side_effects=True),
    )(start_vector, potential)
    return tuple(pl.pallas_call(
        write_out,
        out_shape=(jax.ShapeDtypeStruct(basis.shape, f32), jax.ShapeDtypeStruct(tri.shape, f32)),
        in_specs=[vmem, vmem],
        out_specs=(hbm, hbm),
        scratch_shapes=[dma((2,))],
    )(pltpu.with_memory_space_constraint(basis, pltpu.VMEM), pltpu.with_memory_space_constraint(tri, pltpu.VMEM)))


def solution(mesh):
    sizes = tuple(mesh.shape[name] for name in AXES)
    in_specs = (P("pz", "py", "slab"), P("pz", "py", "slab"))
    out_specs = (P(None, "pz", "py", "slab"), P())
    return jax.shard_map(functools.partial(shards, sizes), mesh=mesh, in_specs=in_specs,
                         out_specs=out_specs, check_vma=False)
```

```python
import functools

import jax
import jax.numpy as jnp
from jax import lax
from jax.experimental import pallas as pl
from jax.experimental.pallas import tpu as pltpu
from jax.sharding import PartitionSpec as P

ITERS = 5
EPSILON = 1e-06
DIAGONAL = 6.0
SUBLANES = 8
MESH = pl.DeviceIdType.MESH
AXES = ("slab", "py", "pz")
UNROLLED = 64
CENTER = 8.25
LEAST_SQUARE, MOST_SQUARE = 0.25, 40.0
LEAST_SHIFT, MOST_SHIFT = 0.5, 16.5
VECTOR, POTENTIAL = 0, 1
RELAY_RING, RELAYED = 4, 5
CHUNK = 3


def times(coeff, columns):
    total = {}
    for k, c in coeff.items():
        for q, value in columns[k].items():
            term = c * value
            total[q] = total[q] + term if q in total else term
    return total


def dot(left, right):
    total = None
    for q, value in left.items():
        if q in right:
            term = value * right[q]
            total = term if total is None else total + term
    return 0.0 if total is None else total


def advance(steps, inner, shifts, taus, removed, betas):
    vectors = [{0: 1.0}]
    image_of = []
    for i in range(steps):
        column = {i + 1: 1.0, i: shifts[i]}
        if taus[i] is not None:
            column[i - 1] = taus[i]
        image_of.append(column)
    gram, lowered = {}, []
    for n in range(steps):
        for k in range(len(lowered), n + 1):
            lowered.append({
                q: dot(vectors[k], {b: inner[q, b] for b in vectors[k]})
                for q in range(n + 1)})
            for l in range(k + 1):
                gram[k, l] = gram[l, k] = dot(vectors[l], lowered[k])
        known = {n: shifts[n]}
        if n > 0:
            known[n - 1] = betas[n - 1]
            rest = times(vectors[n], image_of)
            for k, y in known.items():
                for q, value in vectors[k].items():
                    rest[q] = rest[q] - y * value if q in rest else -y * value
        else:
            rest = {n + 1: 1.0}
        rest_lowered = {
            q: dot(rest, {b: inner[q, b] for b in rest}) for q in range(n + 2)}
        along = {k: dot(vectors[k], rest_lowered) for k in range(n + 1)}
        first = {
            k: along[k] + dot(known, {l: gram[k, l] for l in known}) for k in range(n + 1)}
        excess = {k: first[k] - known[k] if k in known else first[k] for k in range(n + 1)}
        coeffs = {
            k: along[k] - dot(excess, {
                l: gram[k, l] - 1.0 if k == l else gram[k, l] for l in range(n + 1)})
            for k in range(n + 1)}
        square = dot(rest, rest_lowered)
        for k in range(n + 1):
            back = dot(coeffs, {l: gram[k, l] for l in range(n + 1)})
            square = square + coeffs[k] * (back - 2.0 * along[k])
        beta = jnp.sqrt(jnp.maximum(square, 0.0) + EPSILON)
        inverse = 1.0 / beta
        image = dict(rest)
        for k in range(n + 1):
            for q, value in vectors[k].items():
                term = coeffs[k] * value
                image[q] = image[q] - term if q in image else -term
        vectors.append({q: value * inverse for q, value in image.items()})
        removed.append({k: coeffs[k] + known[k] if k in known else coeffs[k] for k in coeffs})
        betas.append(beta)
    return vectors[1:]


def kernel(sizes, per_cell, x_hbm, pot_hbm, out_ref, tri_ref, cells, ext, swapped, relayed, slots,
           group_send, plane_recv, corner_recv, relay_recv, relay_send, side_send, side_recv,
           pair_send, pair_recv, stat_send, stat_recv, load_sem):
    Z, Y, X = x_hbm.shape
    S, A, B = sizes
    n = S * A * B
    H = Z // 2
    D = ITERS
    T = SUBLANES
    ZE, YE = H + 2 * D, Y + 2 * T
    slab, py, pz = (lax.axis_index(name) for name in AXES)
    me = (slab * A + py) * B + pz
    partner = (1 - slab, py, pz)
    first_plane = D - slab * H
    inside = pl.ds(T, Y)

    def to_others(act):
        if n <= UNROLLED:
            slabs = [lax.rem(slab + i, S) for i in range(S)]
            pys = [lax.rem(py + i, A) for i in range(A)]
            pzs = [lax.rem(pz + i, B) for i in range(B)]
            far = sorted(
                ((i, j, k) for i in range(S) for j in range(A) for k in range(B)),
                key=lambda t: -(min(t[1], A - t[1]) + min(t[2], B - t[2])),
            )
            for i, j, k in far:
                if i or j or k:
                    act((slabs[i], pys[j], pzs[k]))
        else:
            def step(d, carry):
                t = lax.rem(me + d, n)
                act((t // (A * B), lax.rem(t // B, A), lax.rem(t, B)))
                return carry
            lax.fori_loop(1, n, step, 0)

    def source(array):
        return cells.at[0] if array == VECTOR else ext

    def remote(src, dst, sent, received, target):
        return pltpu.make_async_remote_copy(
            src_ref=src, dst_ref=dst, send_sem=sent, recv_sem=received,
            device_id=target, device_id_type=MESH)

    def reach(array):
        return D if array == VECTOR else D - 1

    def within(step, position, size):
        if step == 0:
            return None
        return position + step >= 0 if step < 0 else position + step < size

    def guarded(conditions, act):
        conditions = [c for c in conditions if c is not None]
        if not conditions:
            act()
        else:
            pl.when(functools.reduce(jnp.logical_and, conditions))(act)

    def plane_of(t, side, d):
        return block_of(t, side, d, Z)

    def lands(side, d):
        return D - d if side == 0 else D + H - 1 + d

    def rows(step, count, sending):
        if step == 0:
            return inside
        if step < 0:
            return pl.ds(T + Y - count, count) if sending else pl.ds(T - count, count)
        return pl.ds(T, count) if sending else pl.ds(T + Y, count)

    def arrival(array, side, d, step):
        w = d if array == VECTOR else d + 1
        return plane_recv.at[side, w - 1] if step == 0 else corner_recv.at[side, w - 1, step > 0 and 1 or 0]

    def plane_copy(array, t, side, d, step, sent):
        q, z = plane_of(t, side, d)
        count = reach(array) - d
        ref = source(array)
        return remote(
            ref.at[slab, z + first_plane, rows(step, count, True)],
            ref.at[slab, lands(side, d), rows(step, count, False)],
            sent, arrival(array, side, d, step), (t, py - step, pz - q))

    def wait_for(span, sem):
        pltpu.make_async_copy(span, span, sem).wait()

    def lines(count):
        if count % Y == 0:
            return cells.at[0, 0, pl.ds(0, count // Y), pl.ds(0, Y)]
        return cells.at[0, 0, 0, pl.ds(0, count)]

    order = [(a, d) for w in range(1, D + 1) for a, d in ((VECTOR, w), (POTENTIAL, w - 1)) if d]
    relays = order[-RELAYED:] if relaying(Z, B) else []

    def relay_copy(k, t):
        array, d = relays[k]
        z = plane_of(t, t, d)[1]
        return remote(source(array).at[slab, z + first_plane, inside], relayed.at[k],
                      relay_send.at[0], relay_recv.at[k], (slab, py, B - 1 if t == 0 else 0))

    def onward_copy(k, t):
        array, d = relays[k]
        return remote(relayed.at[k], source(array).at[slab, lands(t, d), inside], relay_send.at[1],
                      arrival(array, t, d, 0), (t, py, B - 2 if t == 0 else 1))

    def each_relay(at, act):
        for t in range(2):
            if relays:
                @pl.when(pz == at[t])
                def _(t=t):
                    for k in range(len(relays)):
                        act(k, t)

    def batches(w, sending):
        found = []
        for t in range(2):
            for side in range(2):
                wanted = [(array, d) for array, d in ((VECTOR, w), (POTENTIAL, w - 1))
                          if 1 <= d <= reach(array) and plane_of(t, side, d)[0] != 0]
                for q in sorted({plane_of(t, side, d)[0] for _, d in wanted}, key=abs):
                    mine = [(a, d) for a, d in wanted if plane_of(t, side, d)[0] == q]
                    sign = -1 if sending else 1
                    there = [None if sending else slab == t, within(sign * q, pz, B)]
                    for turned in (False, True):
                        keys = [(a, t, side, d, 0) for a, d in mine
                                if (sending and t == side and (a, d) in relays) == turned]
                        found.append(((t, side, q, 0, turned), there + [pz != 1 + t if turned else None], keys))
                    for step in (-1, 1):
                        keys = [(a, t, side, d, step) for a, d in mine if reach(a) > d]
                        found.append(((t, side, q, step, False), there + [within(sign * step, py, A)], keys))
        return [batch for batch in found if batch[2]]

    def volume(keys):
        return sum(Y if step == 0 else reach(array) - d for array, _, _, d, step in keys)

    groups = {}
    for w in range(1, D + 1):
        for tag, conditions, keys in batches(w, True):
            _, _, size = groups.get(tag, (0, 0, 0))
            groups[tag] = (conditions, list(groups).index(tag) if tag in groups else len(groups), size + volume(keys))

    assert len(groups) == group_count(Z, B)

    def send_planes(w):
        for tag, conditions, keys in batches(w, True):
            def start(tag=tag, keys=keys):
                for key in keys:
                    plane_copy(*key, group_send.at[groups[tag][1]]).start()
            guarded(conditions, start)

    def finish_planes():
        for conditions, g, size in groups.values():
            guarded(conditions, lambda g=g, size=size: wait_for(lines(size), group_send.at[g]))

    def take_planes(w):
        for tag, conditions, keys in batches(w, False):
            array, _, side, d, step = keys[0]
            guarded(conditions, lambda keys=keys, sem=arrival(array, side, d, step): wait_for(
                lines(2 * volume(keys)), sem))

    def side_copy(array, t, step):
        ref = source(array)
        count = reach(array)
        k = step > 0 and 1 or 0
        return remote(
            ref.at[slab, pl.ds(first_plane, Z), rows(step, count, True)],
            ref.at[slab, pl.ds(D - t * H, Z), rows(step, count, False)],
            side_send.at[k], side_recv.at[k], (t, py - step, pz))

    def send_sides():
        for step in (-1, 1):
            def both(step=step):
                for array in (VECTOR, POTENTIAL):
                    for other in range(2):
                        side_copy(array, other, step).start()
            guarded([within(-step, py, A)], both)

    def wait_sides(sign, sems):
        span = cells.at[0, 0, pl.ds(0, Z), pl.ds(0, 2 * (reach(VECTOR) + reach(POTENTIAL)))]
        for k, step in enumerate((-1, 1)):
            guarded([within(sign * step, py, A)], lambda k=k: wait_for(span, sems.at[k]))

    def near_copy(array):
        ref = source(array)
        return remote(
            ref.at[slab, pl.ds(first_plane, Z), inside],
            ref.at[slab, pl.ds(D - (1 - slab) * H, Z), inside],
            pair_send.at[0], pair_recv.at[0], partner)

    def wait_near(sem):
        wait_for(cells.at[0, pl.ds(0, 2), pl.ds(0, Z), pl.ds(0, Y)], sem)

    def swap_copy(level):
        return remote(
            cells.at[level, 1 - slab, pl.ds(D, H), inside], swapped.at[level - 1],
            pair_send.at[1], pair_recv.at[1], partner)

    def stat_copy(p, target):
        return remote(slots.at[p, me], slots.at[p, me], stat_send.at[p], stat_recv.at[p], target)

    def wait_all(p, sem):
        span = slots.at[p, pl.ds(0, n - 1)]
        pltpu.make_async_copy(span, span, sem).wait()

    def fold(value):
        return jnp.sum(value.reshape(value.shape[0] // T, T, X), axis=0)

    def share(p, sums):
        lines = [jnp.sum(v, axis=0, keepdims=True) for v in sums]
        height = -(-len(lines) // T) * T
        lines = lines + [jnp.zeros((1, X), jnp.float32)] * (height - len(lines))
        totals = jnp.sum(jnp.concatenate(lines, axis=0), axis=1, keepdims=True)
        at = lax.broadcasted_iota(jnp.int32, (height, X), 0)
        lanes = lax.broadcasted_iota(jnp.int32, (height, X), 1)
        slots[p, me] = jnp.sum(jnp.where(at == lanes, totals, 0.0), axis=0, keepdims=True)

    def gathered(p, count):
        wait_all(p, stat_recv.at[p])
        total = jnp.sum(slots[p], axis=0) * per_cell
        return [jnp.broadcast_to(total[:, s:s + 1], (1, X)) for s in range(count)]

    barrier = pltpu.get_barrier_semaphore()
    to_others(lambda t: pl.semaphore_signal(barrier, inc=1, device_id=t, device_id_type=MESH))
    loads = [pltpu.make_async_copy(
        hbm, source(array).at[slab, pl.ds(first_plane, Z), inside], load_sem.at[array])
        for array, hbm in ((VECTOR, x_hbm), (POTENTIAL, pot_hbm))]
    for load in loads:
        load.start()

    plane = pz * Z + slab * H - D
    present = [jnp.logical_and(plane + e >= 0, plane + e < B * Z) for e in range(ZE)]
    for e in range(ZE):
        if D <= e < D + H:
            continue
        @pl.when(jnp.logical_not(present[e]))
        def _(e=e):
            for ref in (cells.at[0], ext):
                for core in range(2):
                    ref[core, e] = jnp.zeros((YE, X), jnp.float32)
    for missing, at in ((py == 0, 0), (py == A - 1, T + Y)):
        @pl.when(missing)
        def _(at=at):
            for ref in (cells.at[0], ext):
                for core in range(2):
                    for e in range(ZE):
                        ref[core, e, at:at + T] = jnp.zeros((T, X), jnp.float32)
    for load in loads:
        load.wait()

    def rough():
        lane = lax.broadcasted_iota(jnp.int32, (Y, X), 1)
        row = lax.broadcasted_iota(jnp.int32, (Y, X), 0)

        def apply(own, z):
            here = own(z)
            total = (jnp.where(row == 0, 0.0, pltpu.roll(here, 1, 0))
                     + jnp.where(row == Y - 1, 0.0, pltpu.roll(here, Y - 1, 0))
                     + jnp.where(lane == 0, 0.0, pltpu.roll(here, 1, 1))
                     + jnp.where(lane == X - 1, 0.0, pltpu.roll(here, X - 1, 1)))
            for beside in (z - 1, z + 1):
                if 0 <= beside < Z:
                    total = total + own(beside)
            return ext[slab, first_plane + z, inside] * here - total

        start = lambda z: cells[0, slab, first_plane + z, inside]
        once = lambda z: out_ref[0, z]
        sums = [jnp.zeros((T, X), jnp.float32)] * 5
        for z in range(Z):
            out_ref[0, z] = apply(start, z)
        for z in range(Z):
            zero, one, two = start(z), once(z), apply(once, z)
            for i, (u, v) in enumerate(((zero, zero), (zero, one), (one, one), (one, two), (two, two))):
                sums[i] = sums[i] + fold(u * v)
        return sums

    share(0, rough())
    pl.semaphore_wait(barrier, n - 1)

    to_others(lambda target: stat_copy(0, target).start())
    each_relay((1, 2), lambda k, t: relay_copy(k, t).start())
    for array in (VECTOR, POTENTIAL):
        near_copy(array).start()
    send_planes(1)
    send_sides()
    for w in range(2, D + 1):
        send_planes(w)

    def forward(k, t):
        relay_copy(k, t).wait_recv()
        onward_copy(k, t).start()

    each_relay((B - 1, 0), forward)

    m0, m1, m2, m3, m4 = gathered(0, 5)
    some = m0 > 1e-30
    over = 1.0 / jnp.where(some, m0, 1.0)
    m1, m2, m3, m4 = m1 * over, m2 * over, m3 * over, m4 * over
    c2 = m2 - m1 * m1
    c3 = m3 - 3.0 * m1 * m2 + 2.0 * m1 * m1 * m1
    c4 = m4 - 4.0 * m1 * m3 + 6.0 * m1 * m1 * m2 - 3.0 * m1 * m1 * m1 * m1
    down = 1.0 / jnp.maximum(c2, 1e-3)
    slope = c3 * down
    bound = lambda value, low, high: jnp.minimum(jnp.maximum(value, low), high)
    alpha = [bound(jnp.where(some, DIAGONAL + a, CENTER), LEAST_SHIFT, MOST_SHIFT) for a in (m1, m1 + slope)]
    square = [bound(b, LEAST_SQUARE, MOST_SQUARE) for b in (c2, c4 * down - c2 - slope * slope)]
    shifts = [alpha[0]] + [alpha[1]] * (D - 1)
    taus = [None, square[0]] + [square[1]] * (D - 2)

    first_lane = lax.broadcasted_iota(jnp.int32, (T, X), 1) == 0
    last_lane = lax.broadcasted_iota(jnp.int32, (T, X), 1) == X - 1
    line = lax.broadcasted_iota(jnp.int32, (T, X), 0)
    low_rows = jnp.where(jnp.logical_and(line < D - 1, py == 0), 0.0, 1.0)
    high_rows = jnp.where(jnp.logical_and(line > T - D, py == A - 1), 0.0, 1.0)

    def windows(l):
        reach = D - 1 if l < D else 0
        count = (Y + 2 * reach) // T
        starts = [T - reach + T * i for i in range(count)]
        return [(starts[i], min(CHUNK, count - i), i) for i in range(0, count, CHUNK)], count

    def depth(e):
        return max(D - e, e - (D + H - 1))

    def outer(e):
        return [b for b in (e - 1, e + 1) if depth(b) > depth(e)]

    def tiled(mask, tiles):
        return jnp.concatenate([mask] * tiles, axis=0) if tiles > 1 else mask

    def prepare(l, e):
        for start, tiles, _ in windows(l)[0]:
            at = lambda shift=0: pl.ds(start + shift, tiles * T)
            left, right = cells[l - 1, 0, e, at()], cells[l - 1, 1, e, at()]
            up = [pltpu.roll(v, 1, 1) for v in (left, right)]
            down = [pltpu.roll(v, X - 1, 1) for v in (left, right)]
            head, tail = tiled(first_lane, tiles), tiled(last_lane, tiles)
            along = (jnp.where(head, 0.0, up[0]) + jnp.where(tail, down[1], down[0]),
                     jnp.where(head, up[0], up[1]) + jnp.where(tail, 0.0, down[1]))
            for core, here in enumerate((left, right)):
                around = (cells[l - 1, core, e, at(-1)] + cells[l - 1, core, e, at(1)]) + along[core]
                for b in (e - 1, e + 1):
                    if b not in outer(e):
                        around = around + cells[l - 1, core, b, at()]
                if l == 1:
                    image = -around
                else:
                    image = ((DIAGONAL - shifts[l - 1]) + ext[core, e, at()]) * here - around
                    image = image - taus[l - 1] * cells[l - 2, core, e, at()]
                cells[l, core, e, at()] = image

    def finish(l, e):
        chunks, count = windows(l)
        for core in range(2):
            for start, tiles, first in chunks:
                at = pl.ds(start, tiles * T)
                image = cells[l, core, e, at]
                for b in outer(e):
                    image = image - cells[l - 1, core, b, at]
                if l == 1:
                    image = ((DIAGONAL - shifts[0]) + ext[core, e, at]) * cells[0, core, e, at] + image
                if not D <= e < D + H:
                    image = image * present[e].astype(jnp.float32)
                for i in range(tiles):
                    part = image[i * T:(i + 1) * T]
                    if l < D and first + i == 0:
                        part = part * low_rows
                    if l < D and first + i == count - 1:
                        part = part * high_rows
                    cells[l, core, e, pl.ds(start + i * T, T)] = part

    def wave(w):
        return [(l, e) for l in range(1, D + 1) for e in range(l, ZE - l) if max(l + depth(e), 0) == w]

    def measure(pairs, at, sums=None):
        sums = sums or [jnp.zeros((T, X), jnp.float32)] * len(pairs)
        for core in range(2):
            for e in at:
                held = {k: cells[k, core, e, inside] for k in sorted({k for pair in pairs for k in pair})}
                for i, (k, l) in enumerate(pairs):
                    sums[i] = sums[i] + fold(held[k] * held[l])
        return sums

    wait_near(pair_recv.at[0])
    wait_sides(1, side_recv)
    early = [(k, l) for l in range(D) for k in range(l + 1)]
    late = [(k, D) for k in range(D + 1)]
    held = range(D, D + H)
    done = [e for e in held if depth(e) < 0]
    for l, e in wave(0):
        prepare(l, e)
        finish(l, e)
    for l, e in wave(1):
        prepare(l, e)
    for w in range(1, D + 1):
        take_planes(w)
        for l, e in wave(w):
            finish(l, e)
        swap_copy(w).start()
        if w == D - 1:
            sums = measure(early, held)
            last = measure(late, done)
        if w < D:
            for l, e in wave(w + 1):
                prepare(l, e)
    sums = sums + measure(late, [e for e in held if e not in done], last)
    share(1, sums)
    to_others(lambda target: stat_copy(1, target).start())
    wait_near(pair_send.at[0])
    wait_sides(-1, side_send)
    if relays:
        for at, k in (((1, 2), 0), ((B - 1, 0), 1)):
            @pl.when(jnp.logical_or(pz == at[0], pz == at[1]))
            def _(k=k):
                wait_for(relayed, relay_send.at[k])
    finish_planes()
    wait_for(swapped, pair_send.at[1])
    wait_all(0, stat_send.at[0])
    wait_for(swapped, pair_recv.at[1])
    stats = gathered(1, len(sums))
    scale = 1.0 / jnp.sqrt(stats[0] + EPSILON)
    inner = {}
    for (k, l), value in zip(early + late, stats):
        inner[k, l] = inner[l, k] = value * scale * scale
    removed, betas = [], []
    found = advance(D, inner, shifts, taus, removed, betas)
    for v in range(D):
        tri_ref[0:1, v:v + 1] = removed[v][v][:, 0:1]
        tri_ref[1:2, v:v + 1] = betas[v][:, 0:1]
    found = [{q: t * scale for q, t in coords.items()} for coords in found]

    for half in range(2):
        for i in range(H):
            if half == 0:
                z = slab * H + i
                columns = [cells[q, slab, D + i, inside] for q in range(D + 1)]
            else:
                z = (1 - slab) * H + i
                columns = [cells[0, slab, first_plane + z, inside]] + [swapped[q, i] for q in range(D)]
            out_ref[0, z] = columns[0] * scale
            for k, coords in enumerate(found):
                total = None
                for q in sorted(coords, reverse=True):
                    term = coords[q] * columns[q]
                    total = term if total is None else total + term
                out_ref[k + 1, z] = total

    wait_all(1, stat_send.at[1])


def block_of(t, side, d, Z):
    z = t * (Z // 2) - d if side == 0 else (t + 1) * (Z // 2) - 1 + d
    return z // Z, z % Z


def relaying(Z, B):
    return B == RELAY_RING and block_of(0, 0, ITERS, Z)[0] == -1


def group_count(Z, B):
    count = 2 if relaying(Z, B) else 0
    for t in range(2):
        for side in range(2):
            blocks = [block_of(t, side, d, Z)[0] for d in range(1, ITERS + 1)]
            count += len(set(blocks) - {0}) + 2 * len(set(blocks[:-1]) - {0})
    return count


def write_out(basis_ref, tri_ref, basis_out, tri_out, sems):
    copies = (pltpu.make_async_copy(basis_ref, basis_out, sems.at[0]),
              pltpu.make_async_copy(tri_ref, tri_out, sems.at[1]))
    for copy in copies:
        copy.start()
    for copy in copies:
        copy.wait()


def shards(sizes, start_vector, potential):
    Z, Y, X = start_vector.shape
    n = sizes[0] * sizes[1] * sizes[2]
    f32 = jnp.float32
    H, D, T = Z // 2, ITERS, SUBLANES
    assert sizes[0] == 2 and Z % 2 == 0 and H <= D and Y >= D and Y % T == 0
    vmem = pl.BlockSpec(memory_space=pltpu.VMEM)
    hbm = pl.BlockSpec(memory_space=pl.ANY)
    dma = pltpu.SemaphoreType.DMA
    extended = (2, H + 2 * D, Y + 2 * T, X)
    basis, tri = pl.pallas_call(
        functools.partial(kernel, sizes, 1.0 / (start_vector.size * n)),
        out_shape=(pltpu.VMEM((D + 1, Z, Y, X), f32), pltpu.VMEM((2, D), f32)),
        in_specs=[hbm, hbm],
        out_specs=(vmem, vmem),
        scratch_shapes=[
            pltpu.VMEM((D + 1,) + extended, f32),
            pltpu.VMEM(extended, f32),
            pltpu.VMEM((D, H, Y, X), f32),
            pltpu.VMEM((RELAYED, Y, X), f32),
            pltpu.VMEM((2, n, 1, X), f32),
            dma((group_count(Z, sizes[2]),)),
            dma((2, D)),
            dma((2, D - 1, 2)),
            dma((RELAYED,)),
            dma((2,)),
            dma((2,)),
            dma((2,)),
            dma((2,)),
            dma((2,)),
            dma((2,)),
            dma((2,)),
            dma((2,)),
        ],
        compiler_params=pltpu.CompilerParams(collective_id=0, has_side_effects=True),
    )(start_vector, potential)
    return tuple(pl.pallas_call(
        write_out,
        out_shape=(jax.ShapeDtypeStruct(basis.shape, f32), jax.ShapeDtypeStruct(tri.shape, f32)),
        in_specs=[vmem, vmem],
        out_specs=(hbm, hbm),
        scratch_shapes=[dma((2,))],
    )(pltpu.with_memory_space_constraint(basis, pltpu.VMEM), pltpu.with_memory_space_constraint(tri, pltpu.VMEM)))


def solution(mesh):
    sizes = tuple(mesh.shape[name] for name in AXES)
    in_specs = (P("pz", "py", "slab"), P("pz", "py", "slab"))
    out_specs = (P(None, "pz", "py", "slab"), P())
    return jax.shard_map(functools.partial(shards, sizes), mesh=mesh, in_specs=in_specs,
                         out_specs=out_specs, check_vma=False)
```

```python
import functools

import jax
import jax.numpy as jnp
from jax import lax
from jax.experimental import pallas as pl
from jax.experimental.pallas import tpu as pltpu
from jax.sharding import PartitionSpec as P

ITERS = 5
EPSILON = 1e-06
DIAGONAL = 6.0
SUBLANES = 8
MESH = pl.DeviceIdType.MESH
AXES = ("slab", "py", "pz")
UNROLLED = 64
CENTER = 8.25
LEAST_SQUARE, MOST_SQUARE = 0.25, 40.0
LEAST_SHIFT, MOST_SHIFT = 0.5, 16.5
VECTOR, POTENTIAL = 0, 1
RELAY_RING, RELAYED = 4, 5
CHUNK = 3


def times(coeff, columns):
    total = {}
    for k, c in coeff.items():
        for q, value in columns[k].items():
            term = c * value
            total[q] = total[q] + term if q in total else term
    return total


def dot(left, right):
    total = None
    for q, value in left.items():
        if q in right:
            term = value * right[q]
            total = term if total is None else total + term
    return 0.0 if total is None else total


def advance(steps, inner, shifts, taus, removed, betas):
    vectors = [{0: 1.0}]
    image_of = []
    for i in range(steps):
        column = {i + 1: 1.0, i: shifts[i]}
        if taus[i] is not None:
            column[i - 1] = taus[i]
        image_of.append(column)
    gram, lowered = {}, []
    for n in range(steps):
        for k in range(len(lowered), n + 1):
            lowered.append({
                q: dot(vectors[k], {b: inner[q, b] for b in vectors[k]})
                for q in range(n + 1)})
            for l in range(k + 1):
                gram[k, l] = gram[l, k] = dot(vectors[l], lowered[k])
        known = {n: shifts[n]}
        if n > 0:
            known[n - 1] = betas[n - 1]
            rest = times(vectors[n], image_of)
            for k, y in known.items():
                for q, value in vectors[k].items():
                    rest[q] = rest[q] - y * value if q in rest else -y * value
        else:
            rest = {n + 1: 1.0}
        rest_lowered = {
            q: dot(rest, {b: inner[q, b] for b in rest}) for q in range(n + 2)}
        along = {k: dot(vectors[k], rest_lowered) for k in range(n + 1)}
        first = {
            k: along[k] + dot(known, {l: gram[k, l] for l in known}) for k in range(n + 1)}
        excess = {k: first[k] - known[k] if k in known else first[k] for k in range(n + 1)}
        coeffs = {
            k: along[k] - dot(excess, {
                l: gram[k, l] - 1.0 if k == l else gram[k, l] for l in range(n + 1)})
            for k in range(n + 1)}
        square = dot(rest, rest_lowered)
        for k in range(n + 1):
            back = dot(coeffs, {l: gram[k, l] for l in range(n + 1)})
            square = square + coeffs[k] * (back - 2.0 * along[k])
        beta = jnp.sqrt(jnp.maximum(square, 0.0) + EPSILON)
        inverse = 1.0 / beta
        image = dict(rest)
        for k in range(n + 1):
            for q, value in vectors[k].items():
                term = coeffs[k] * value
                image[q] = image[q] - term if q in image else -term
        vectors.append({q: value * inverse for q, value in image.items()})
        removed.append({k: coeffs[k] + known[k] if k in known else coeffs[k] for k in coeffs})
        betas.append(beta)
    return vectors[1:]


def kernel(sizes, per_cell, x_hbm, pot_hbm, out_ref, tri_ref, cells, ext, swapped, relayed, slots,
           group_send, plane_recv, corner_recv, relay_recv, relay_send, side_sems, pair_sems, stat_sems, load_sem):
    Z, Y, X = x_hbm.shape
    S, A, B = sizes
    n = S * A * B
    H = Z // 2
    D = ITERS
    T = SUBLANES
    ZE, YE = H + 2 * D, Y + 2 * T
    slab, py, pz = (lax.axis_index(name) for name in AXES)
    me = (slab * A + py) * B + pz
    partner = (1 - slab, py, pz)
    first_plane = D - slab * H
    inside = pl.ds(T, Y)

    def to_others(act):
        if n <= UNROLLED:
            slabs = [lax.rem(slab + i, S) for i in range(S)]
            pys = [lax.rem(py + i, A) for i in range(A)]
            pzs = [lax.rem(pz + i, B) for i in range(B)]
            far = sorted(
                ((i, j, k) for i in range(S) for j in range(A) for k in range(B)),
                key=lambda t: -(min(t[1], A - t[1]) + min(t[2], B - t[2])),
            )
            for i, j, k in far:
                if i or j or k:
                    act((slabs[i], pys[j], pzs[k]))
        else:
            def step(d, carry):
                t = lax.rem(me + d, n)
                act((t // (A * B), lax.rem(t // B, A), lax.rem(t, B)))
                return carry
            lax.fori_loop(1, n, step, 0)

    def source(array):
        return cells.at[0] if array == VECTOR else ext

    def remote(src, dst, sent, received, target):
        return pltpu.make_async_remote_copy(
            src_ref=src, dst_ref=dst, send_sem=sent, recv_sem=received,
            device_id=target, device_id_type=MESH)

    def reach(array):
        return D if array == VECTOR else D - 1

    def within(step, position, size):
        if step == 0:
            return None
        return position + step >= 0 if step < 0 else position + step < size

    def guarded(conditions, act):
        conditions = [c for c in conditions if c is not None]
        if not conditions:
            act()
        else:
            pl.when(functools.reduce(jnp.logical_and, conditions))(act)

    def plane_of(t, side, d):
        return block_of(t, side, d, Z)

    def lands(side, d):
        return D - d if side == 0 else D + H - 1 + d

    def rows(step, count, sending):
        if step == 0:
            return inside
        if step < 0:
            return pl.ds(T + Y - count, count) if sending else pl.ds(T - count, count)
        return pl.ds(T, count) if sending else pl.ds(T + Y, count)

    def arrival(array, t, side, d, step):
        w = d if array == VECTOR else d + 1
        if side != t:
            w = w + H - Z + (D if step == 0 else D - 1)
        return (plane_recv if step == 0 else corner_recv).at[w - 1]

    def plane_copy(array, t, side, d, step, sent):
        q, z = plane_of(t, side, d)
        count = reach(array) - d
        ref = source(array)
        return remote(
            ref.at[slab, z + first_plane, rows(step, count, True)],
            ref.at[slab, lands(side, d), rows(step, count, False)],
            sent, arrival(array, t, side, d, step), (t, py - step, pz - q))

    def wait_for(span, sem):
        pltpu.make_async_copy(span, span, sem).wait()

    def lines(count):
        if count % Y:
            return cells.at[0, 0, 0, pl.ds(0, count)]
        a, b, c = next((a, b, count // Y // (a * b)) for a in range(1, D + 2) for b in (1, 2)
                       if count // Y % (a * b) == 0 and count // Y // (a * b) <= ZE)
        return cells.at[pl.ds(0, a), pl.ds(0, b), pl.ds(0, c), pl.ds(0, Y)]

    below, above = py > 0, py < A - 1
    beside_both, beside_one = jnp.logical_and(below, above), below != above

    order = [(a, d) for w in range(1, D + 1) for a, d in ((VECTOR, w), (POTENTIAL, w - 1)) if d]
    relays = order[-RELAYED:] if relaying(Z, B) else []

    def relay_copy(k, t):
        array, d = relays[k]
        z = plane_of(t, t, d)[1]
        return remote(source(array).at[slab, z + first_plane, inside], relayed.at[k],
                      relay_send.at[0], relay_recv.at[k], (slab, py, B - 1 if t == 0 else 0))

    def onward_copy(k, t):
        array, d = relays[k]
        return remote(relayed.at[k], source(array).at[slab, lands(t, d), inside], relay_send.at[0],
                      arrival(array, t, t, d, 0), (t, py, B - 2 if t == 0 else 1))

    def each_relay(at, act):
        for t in range(2):
            if relays:
                @pl.when(pz == at[t])
                def _(t=t):
                    for k in range(len(relays)):
                        act(k, t)

    def batches(w, sending):
        found = []
        for t in range(2):
            for side in range(2):
                wanted = [(array, d) for array, d in ((VECTOR, w), (POTENTIAL, w - 1))
                          if 1 <= d <= reach(array) and plane_of(t, side, d)[0] != 0]
                for q in sorted({plane_of(t, side, d)[0] for _, d in wanted}, key=abs):
                    mine = [(a, d) for a, d in wanted if plane_of(t, side, d)[0] == q]
                    sign = -1 if sending else 1
                    there = [None if sending else slab == t, within(sign * q, pz, B)]
                    for turned in (False, True):
                        keys = [(a, t, side, d, 0) for a, d in mine
                                if (sending and t == side and (a, d) in relays) == turned]
                        found.append(((q, 0, turned), there + [pz != 1 + t if turned else None], keys))
                    low, high = ([(a, t, side, d, step) for a, d in mine if reach(a) > d] for step in (-1, 1))
                    if sending:
                        found.append(((q, -1, False), there + [above], low))
                        found.append(((q, 1, False), there + [below], high))
                    else:
                        found.append(((q, 1, False), there + [beside_both], low + high))
                        found.append(((q, 1, False), there + [beside_one], low))
        return [batch for batch in found if batch[2]]

    def volume(keys):
        return sum(Y if step == 0 else reach(array) - d for array, _, _, d, step in keys)

    totals = {}
    for w in range(1, D + 1):
        for tag, conditions, keys in batches(w, True):
            totals[tag] = (conditions, totals.get(tag, (0, 0))[1] + volume(keys))
    slot_of = {tag: i for i, tag in enumerate(dict.fromkeys((q, step and 1, turned) for q, step, turned in totals))}
    assert len(slot_of) == group_count(Z, B)

    def group(tag):
        q, step, turned = tag
        return group_send.at[slot_of[q, step and 1, turned]]

    def send_planes(w):
        for tag, conditions, keys in batches(w, True):
            def start(tag=tag, keys=keys):
                for key in keys:
                    plane_copy(*key, group(tag)).start()
            guarded(conditions, start)

    def finish_planes():
        for tag, (conditions, size) in totals.items():
            q, step, _ = tag
            if step == 0:
                guarded(conditions, lambda tag=tag, size=size: wait_for(lines(size), group(tag)))
            elif step > 0:
                for times_, beside in ((2, beside_both), (1, beside_one)):
                    guarded([within(-q, pz, B), beside], lambda tag=tag, rows_=times_ * size: wait_for(
                        lines(rows_), group(tag)))

    def take_planes(w):
        for tag, conditions, keys in batches(w, False):
            array, t, side, d, step = keys[0]
            guarded(conditions, lambda keys=keys, sem=arrival(array, t, side, d, step): wait_for(
                lines(2 * volume(keys)), sem))

    def side_copy(array, t, step):
        ref = source(array)
        count = reach(array)
        return remote(
            ref.at[slab, pl.ds(first_plane, Z), rows(step, count, True)],
            ref.at[slab, pl.ds(D - t * H, Z), rows(step, count, False)],
            side_sems.at[0], side_sems.at[1], (t, py - step, pz))

    def send_sides():
        for step in (-1, 1):
            def both(step=step):
                for array in (VECTOR, POTENTIAL):
                    for other in range(2):
                        side_copy(array, other, step).start()
            guarded([within(-step, py, A)], both)

    def wait_sides(sem):
        count = 2 * (reach(VECTOR) + reach(POTENTIAL))
        for times_, beside in ((2, beside_both), (1, beside_one)):
            guarded([beside], lambda times_=times_: wait_for(
                cells.at[0, 0, pl.ds(0, Z), pl.ds(0, times_ * count)], sem))

    def near_copy(array):
        ref = source(array)
        return remote(
            ref.at[slab, pl.ds(first_plane, Z), inside],
            ref.at[slab, pl.ds(D - (1 - slab) * H, Z), inside],
            pair_sems.at[0], pair_sems.at[1], partner)

    def swap_copy(level):
        return remote(
            cells.at[level, 1 - slab, pl.ds(D, H), inside], swapped.at[level - 1],
            pair_sems.at[0], pair_sems.at[2], partner)

    def stat_copy(p, target):
        return remote(slots.at[p, me], slots.at[p, me], stat_sems.at[2], stat_sems.at[p], target)

    def fold(value):
        return jnp.sum(value.reshape(value.shape[0] // T, T, X), axis=0)

    def share(p, sums):
        lines = [jnp.sum(v, axis=0, keepdims=True) for v in sums]
        height = -(-len(lines) // T) * T
        lines = lines + [jnp.zeros((1, X), jnp.float32)] * (height - len(lines))
        totals = jnp.sum(jnp.concatenate(lines, axis=0), axis=1, keepdims=True)
        at = lax.broadcasted_iota(jnp.int32, (height, X), 0)
        lanes = lax.broadcasted_iota(jnp.int32, (height, X), 1)
        slots[p, me] = jnp.sum(jnp.where(at == lanes, totals, 0.0), axis=0, keepdims=True)

    def gathered(p, count):
        wait_for(slots.at[p, pl.ds(0, n - 1)], stat_sems.at[p])
        total = jnp.sum(slots[p], axis=0) * per_cell
        return [jnp.broadcast_to(total[:, s:s + 1], (1, X)) for s in range(count)]

    barrier = pltpu.get_barrier_semaphore()
    to_others(lambda t: pl.semaphore_signal(barrier, inc=1, device_id=t, device_id_type=MESH))
    loads = [pltpu.make_async_copy(
        hbm, source(array).at[slab, pl.ds(first_plane, Z), inside], load_sem.at[0])
        for array, hbm in ((VECTOR, x_hbm), (POTENTIAL, pot_hbm))]
    for load in loads:
        load.start()

    plane = pz * Z + slab * H - D
    present = [jnp.logical_and(plane + e >= 0, plane + e < B * Z) for e in range(ZE)]
    for e in range(ZE):
        if D <= e < D + H:
            continue
        @pl.when(jnp.logical_not(present[e]))
        def _(e=e):
            for ref in (cells.at[0], ext):
                for core in range(2):
                    ref[core, e] = jnp.zeros((YE, X), jnp.float32)
    for missing, at in ((py == 0, 0), (py == A - 1, T + Y)):
        @pl.when(missing)
        def _(at=at):
            for ref in (cells.at[0], ext):
                for core in range(2):
                    for e in range(ZE):
                        ref[core, e, at:at + T] = jnp.zeros((T, X), jnp.float32)
    wait_for(lines(2 * Z * Y), load_sem.at[0])

    def rough():
        lane = lax.broadcasted_iota(jnp.int32, (Y, X), 1)
        row = lax.broadcasted_iota(jnp.int32, (Y, X), 0)

        def apply(own, z):
            here = own(z)
            total = (jnp.where(row == 0, 0.0, pltpu.roll(here, 1, 0))
                     + jnp.where(row == Y - 1, 0.0, pltpu.roll(here, Y - 1, 0))
                     + jnp.where(lane == 0, 0.0, pltpu.roll(here, 1, 1))
                     + jnp.where(lane == X - 1, 0.0, pltpu.roll(here, X - 1, 1)))
            for beside in (z - 1, z + 1):
                if 0 <= beside < Z:
                    total = total + own(beside)
            return ext[slab, first_plane + z, inside] * here - total

        start = lambda z: cells[0, slab, first_plane + z, inside]
        once = lambda z: out_ref[0, z]
        sums = [jnp.zeros((T, X), jnp.float32)] * 5
        for z in range(Z):
            out_ref[0, z] = apply(start, z)
        for z in range(Z):
            zero, one, two = start(z), once(z), apply(once, z)
            for i, (u, v) in enumerate(((zero, zero), (zero, one), (one, one), (one, two), (two, two))):
                sums[i] = sums[i] + fold(u * v)
        return sums

    share(0, rough())
    pl.semaphore_wait(barrier, n - 1)

    each_relay((1, 2), lambda k, t: relay_copy(k, t).start())
    send_planes(1)
    to_others(lambda target: stat_copy(0, target).start())
    for array in (VECTOR, POTENTIAL):
        near_copy(array).start()
    send_sides()
    for w in range(2, D + 1):
        send_planes(w)

    def forward(k, t):
        relay_copy(k, t).wait_recv()
        onward_copy(k, t).start()

    each_relay((B - 1, 0), forward)

    first_lane = lax.broadcasted_iota(jnp.int32, (T, X), 1) == 0
    last_lane = lax.broadcasted_iota(jnp.int32, (T, X), 1) == X - 1
    line = lax.broadcasted_iota(jnp.int32, (T, X), 0)
    low_rows = jnp.where(jnp.logical_and(line < D - 1, py == 0), 0.0, 1.0)
    high_rows = jnp.where(jnp.logical_and(line > T - D, py == A - 1), 0.0, 1.0)

    def windows(l):
        reach = D - 1 if l < D else 0
        count = (Y + 2 * reach) // T
        starts = [T - reach + T * i for i in range(count)]
        return [(starts[i], min(CHUNK, count - i), i) for i in range(0, count, CHUNK)], count

    def depth(e):
        return max(D - e, e - (D + H - 1))

    def outer(e):
        return [b for b in (e - 1, e + 1) if depth(b) > depth(e)]

    def tiled(mask, tiles):
        return jnp.concatenate([mask] * tiles, axis=0) if tiles > 1 else mask

    def prepare(l, e):
        for start, tiles, _ in windows(l)[0]:
            at = lambda shift=0: pl.ds(start + shift, tiles * T)
            left, right = cells[l - 1, 0, e, at()], cells[l - 1, 1, e, at()]
            up = [pltpu.roll(v, 1, 1) for v in (left, right)]
            down = [pltpu.roll(v, X - 1, 1) for v in (left, right)]
            head, tail = tiled(first_lane, tiles), tiled(last_lane, tiles)
            along = (jnp.where(head, 0.0, up[0]) + jnp.where(tail, down[1], down[0]),
                     jnp.where(head, up[0], up[1]) + jnp.where(tail, 0.0, down[1]))
            for core, here in enumerate((left, right)):
                around = (cells[l - 1, core, e, at(-1)] + cells[l - 1, core, e, at(1)]) + along[core]
                for b in (e - 1, e + 1):
                    if b not in outer(e):
                        around = around + cells[l - 1, core, b, at()]
                if l == 1:
                    image = -around
                else:
                    image = ((DIAGONAL - shifts[l - 1]) + ext[core, e, at()]) * here - around
                    image = image - taus[l - 1] * cells[l - 2, core, e, at()]
                cells[l, core, e, at()] = image

    def finish(l, e):
        chunks, count = windows(l)
        for core in range(2):
            for start, tiles, first in chunks:
                at = pl.ds(start, tiles * T)
                image = cells[l, core, e, at]
                for b in outer(e):
                    image = image - cells[l - 1, core, b, at]
                if l == 1:
                    image = ((DIAGONAL - shifts[0]) + ext[core, e, at]) * cells[0, core, e, at] + image
                if not D <= e < D + H:
                    image = image * present[e].astype(jnp.float32)
                for i in range(tiles):
                    part = image[i * T:(i + 1) * T]
                    if l < D and first + i == 0:
                        part = part * low_rows
                    if l < D and first + i == count - 1:
                        part = part * high_rows
                    cells[l, core, e, pl.ds(start + i * T, T)] = part

    def wave(w):
        return [(l, e) for l in range(1, D + 1) for e in range(l, ZE - l) if max(l + depth(e), 0) == w]

    def measure(pairs, at, sums=None):
        sums = sums or [jnp.zeros((T, X), jnp.float32)] * len(pairs)
        for core in range(2):
            for e in at:
                held = {k: cells[k, core, e, inside] for k in sorted({k for pair in pairs for k in pair})}
                for i, (k, l) in enumerate(pairs):
                    sums[i] = sums[i] + fold(held[k] * held[l])
        return sums

    wait_for(lines(2 * Z * Y), pair_sems.at[1])
    wait_sides(side_sems.at[1])
    ready = []
    for reached in range(2):
        if reached:
            take_planes(reached)
        for e in range(1, ZE - 1):
            if depth(e) <= reached and e not in ready:
                prepare(1, e)
                ready.append(e)

    m0, m1, m2, m3, m4 = gathered(0, 5)
    some = m0 > 1e-30
    over = 1.0 / jnp.where(some, m0, 1.0)
    m1, m2, m3, m4 = m1 * over, m2 * over, m3 * over, m4 * over
    c2 = m2 - m1 * m1
    c3 = m3 - 3.0 * m1 * m2 + 2.0 * m1 * m1 * m1
    c4 = m4 - 4.0 * m1 * m3 + 6.0 * m1 * m1 * m2 - 3.0 * m1 * m1 * m1 * m1
    down = 1.0 / jnp.maximum(c2, 1e-3)
    slope = c3 * down
    bound = lambda value, low, high: jnp.minimum(jnp.maximum(value, low), high)
    alpha = [bound(jnp.where(some, DIAGONAL + a, CENTER), LEAST_SHIFT, MOST_SHIFT) for a in (m1, m1 + slope)]
    square = [bound(b, LEAST_SQUARE, MOST_SQUARE) for b in (c2, c4 * down - c2 - slope * slope)]
    shifts = [alpha[0]] + [alpha[1]] * (D - 1)
    taus = [None, square[0]] + [square[1]] * (D - 2)

    early = [(k, l) for l in range(D) for k in range(l + 1)]
    late = [(k, D) for k in range(D + 1)]
    held = range(D, D + H)
    done = [e for e in held if depth(e) < 0]
    def prepare_all(entries):
        for l, e in entries:
            if l > 1 or e not in ready:
                prepare(l, e)

    for entry in wave(0):
        prepare_all([entry])
        finish(*entry)
    prepare_all(wave(1))
    for w in range(1, D + 1):
        if w > 1:
            take_planes(w)
        for l, e in wave(w):
            finish(l, e)
        swap_copy(w).start()
        if w == D - 1:
            sums = measure(early, held)
            last = measure(late, done)
        if w < D:
            prepare_all(wave(w + 1))
    sums = sums + measure(late, [e for e in held if e not in done], last)
    share(1, sums)
    to_others(lambda target: stat_copy(1, target).start())
    wait_for(lines((2 * Z + D * H) * Y), pair_sems.at[0])
    wait_sides(side_sems.at[0])
    if relays:
        wait_for(relayed, relay_send.at[0])
    finish_planes()
    wait_for(swapped, pair_sems.at[2])
    stats = gathered(1, len(sums))
    scale = 1.0 / jnp.sqrt(stats[0] + EPSILON)
    inner = {}
    for (k, l), value in zip(early + late, stats):
        inner[k, l] = inner[l, k] = value * scale * scale
    removed, betas = [], []
    found = advance(D, inner, shifts, taus, removed, betas)
    for v in range(D):
        tri_ref[0:1, v:v + 1] = removed[v][v][:, 0:1]
        tri_ref[1:2, v:v + 1] = betas[v][:, 0:1]
    found = [{q: t * scale for q, t in coords.items()} for coords in found]

    for half in range(2):
        for i in range(H):
            if half == 0:
                z = slab * H + i
                columns = [cells[q, slab, D + i, inside] for q in range(D + 1)]
            else:
                z = (1 - slab) * H + i
                columns = [cells[0, slab, first_plane + z, inside]] + [swapped[q, i] for q in range(D)]
            out_ref[0, z] = columns[0] * scale
            for k, coords in enumerate(found):
                total = None
                for q in sorted(coords, reverse=True):
                    term = coords[q] * columns[q]
                    total = term if total is None else total + term
                out_ref[k + 1, z] = total

    wait_for(slots.at[pl.ds(0, 2), pl.ds(0, n - 1)], stat_sems.at[2])


def block_of(t, side, d, Z):
    z = t * (Z // 2) - d if side == 0 else (t + 1) * (Z // 2) - 1 + d
    return z // Z, z % Z


def relaying(Z, B):
    return B == RELAY_RING and block_of(0, 0, ITERS, Z)[0] == -1


def group_count(Z, B):
    blocks = [[block_of(t, side, d, Z)[0] for d in range(1, ITERS + 1)] for t in range(2) for side in range(2)]
    straight = {q for row in blocks for q in row} - {0}
    beside = {q for row in blocks for q in row[:-1]} - {0}
    return len(straight) + len(beside) + (2 if relaying(Z, B) else 0)


def write_out(basis_ref, tri_ref, basis_out, tri_out, sems):
    copies = (pltpu.make_async_copy(basis_ref, basis_out, sems.at[0]),
              pltpu.make_async_copy(tri_ref, tri_out, sems.at[1]))
    for copy in copies:
        copy.start()
    for copy in copies:
        copy.wait()


def shards(sizes, start_vector, potential):
    Z, Y, X = start_vector.shape
    n = sizes[0] * sizes[1] * sizes[2]
    f32 = jnp.float32
    H, D, T = Z // 2, ITERS, SUBLANES
    assert sizes[0] == 2 and Z % 2 == 0 and H <= D and Y >= D and Y % T == 0
    vmem = pl.BlockSpec(memory_space=pltpu.VMEM)
    hbm = pl.BlockSpec(memory_space=pl.ANY)
    dma = pltpu.SemaphoreType.DMA
    extended = (2, H + 2 * D, Y + 2 * T, X)
    basis, tri = pl.pallas_call(
        functools.partial(kernel, sizes, 1.0 / (start_vector.size * n)),
        out_shape=(pltpu.VMEM((D + 1, Z, Y, X), f32), pltpu.VMEM((2, D), f32)),
        in_specs=[hbm, hbm],
        out_specs=(vmem, vmem),
        scratch_shapes=[
            pltpu.VMEM((D + 1,) + extended, f32),
            pltpu.VMEM(extended, f32),
            pltpu.VMEM((D, H, Y, X), f32),
            pltpu.VMEM((RELAYED, Y, X), f32),
            pltpu.VMEM((2, n, 1, X), f32),
            dma((group_count(Z, sizes[2]),)),
            dma((D + max(0, D - Z + H),)),
            dma((D - 1 + max(0, D - 1 - Z + H),)),
            dma((RELAYED,)),
            dma((1,)),
            dma((2,)),
            dma((3,)),
            dma((3,)),
            dma((1,)),
        ],
        compiler_params=pltpu.CompilerParams(collective_id=0, has_side_effects=True),
    )(start_vector, potential)
    return tuple(pl.pallas_call(
        write_out,
        out_shape=(jax.ShapeDtypeStruct(basis.shape, f32), jax.ShapeDtypeStruct(tri.shape, f32)),
        in_specs=[vmem, vmem],
        out_specs=(hbm, hbm),
        scratch_shapes=[dma((2,))],
    )(pltpu.with_memory_space_constraint(basis, pltpu.VMEM), pltpu.with_memory_space_constraint(tri, pltpu.VMEM)))


def solution(mesh):
    sizes = tuple(mesh.shape[name] for name in AXES)
    in_specs = (P("pz", "py", "slab"), P("pz", "py", "slab"))
    out_specs = (P(None, "pz", "py", "slab"), P())
    return jax.shard_map(functools.partial(shards, sizes), mesh=mesh, in_specs=in_specs,
                         out_specs=out_specs, check_vma=False)
```

```python
import functools

import jax
import jax.numpy as jnp
from jax import lax
from jax.experimental import pallas as pl
from jax.experimental.pallas import tpu as pltpu
from jax.sharding import PartitionSpec as P

ITERS = 5
EPSILON = 1e-06
DIAGONAL = 6.0
SUBLANES = 8
MESH = pl.DeviceIdType.MESH
AXES = ("slab", "py", "pz")
UNROLLED = 64
CENTER = 8.25
LEAST_SQUARE, MOST_SQUARE = 0.25, 40.0
LEAST_SHIFT, MOST_SHIFT = 0.5, 16.5
VECTOR, POTENTIAL = 0, 1
RELAY_RING, RELAYED = 4, 5
CHUNK = 3


def times(coeff, columns):
    total = {}
    for k, c in coeff.items():
        for q, value in columns[k].items():
            term = c * value
            total[q] = total[q] + term if q in total else term
    return total


def dot(left, right):
    total = None
    for q, value in left.items():
        if q in right:
            term = value * right[q]
            total = term if total is None else total + term
    return 0.0 if total is None else total


def advance(steps, inner, shifts, taus, removed, betas):
    vectors = [{0: 1.0}]
    image_of = []
    for i in range(steps):
        column = {i + 1: 1.0, i: shifts[i]}
        if taus[i] is not None:
            column[i - 1] = taus[i]
        image_of.append(column)
    gram, lowered = {}, []
    for n in range(steps):
        for k in range(len(lowered), n + 1):
            lowered.append({
                q: dot(vectors[k], {b: inner[q, b] for b in vectors[k]})
                for q in range(n + 1)})
            for l in range(k + 1):
                gram[k, l] = gram[l, k] = dot(vectors[l], lowered[k])
        known = {n: shifts[n]}
        if n > 0:
            known[n - 1] = betas[n - 1]
            rest = times(vectors[n], image_of)
            for k, y in known.items():
                for q, value in vectors[k].items():
                    rest[q] = rest[q] - y * value if q in rest else -y * value
        else:
            rest = {n + 1: 1.0}
        rest_lowered = {
            q: dot(rest, {b: inner[q, b] for b in rest}) for q in range(n + 2)}
        along = {k: dot(vectors[k], rest_lowered) for k in range(n + 1)}
        first = {
            k: along[k] + dot(known, {l: gram[k, l] for l in known}) for k in range(n + 1)}
        excess = {k: first[k] - known[k] if k in known else first[k] for k in range(n + 1)}
        coeffs = {
            k: along[k] - dot(excess, {
                l: gram[k, l] - 1.0 if k == l else gram[k, l] for l in range(n + 1)})
            for k in range(n + 1)}
        square = dot(rest, rest_lowered)
        for k in range(n + 1):
            back = dot(coeffs, {l: gram[k, l] for l in range(n + 1)})
            square = square + coeffs[k] * (back - 2.0 * along[k])
        beta = jnp.sqrt(jnp.maximum(square, 0.0) + EPSILON)
        inverse = 1.0 / beta
        image = dict(rest)
        for k in range(n + 1):
            for q, value in vectors[k].items():
                term = coeffs[k] * value
                image[q] = image[q] - term if q in image else -term
        vectors.append({q: value * inverse for q, value in image.items()})
        removed.append({k: coeffs[k] + known[k] if k in known else coeffs[k] for k in coeffs})
        betas.append(beta)
    return vectors[1:]


def kernel(sizes, per_cell, x_hbm, pot_hbm, out_ref, coeff_ref, tri_ref, cells, ext, swapped, relayed, slots,
           group_send, plane_recv, corner_recv, relay_recv, relay_send, side_sems, pair_sems, stat_sems, load_sem):
    Z, Y, X = x_hbm.shape
    S, A, B = sizes
    n = S * A * B
    H = Z // 2
    D = ITERS
    T = SUBLANES
    ZE, YE = H + 2 * D, Y + 2 * T
    slab, py, pz = (lax.axis_index(name) for name in AXES)
    me = (slab * A + py) * B + pz
    partner = (1 - slab, py, pz)
    first_plane = D - slab * H
    inside = pl.ds(T, Y)

    def to_others(act):
        if n <= UNROLLED:
            slabs = [lax.rem(slab + i, S) for i in range(S)]
            pys = [lax.rem(py + i, A) for i in range(A)]
            pzs = [lax.rem(pz + i, B) for i in range(B)]
            far = sorted(
                ((i, j, k) for i in range(S) for j in range(A) for k in range(B)),
                key=lambda t: -(min(t[1], A - t[1]) + min(t[2], B - t[2])),
            )
            for i, j, k in far:
                if i or j or k:
                    act((slabs[i], pys[j], pzs[k]))
        else:
            def step(d, carry):
                t = lax.rem(me + d, n)
                act((t // (A * B), lax.rem(t // B, A), lax.rem(t, B)))
                return carry
            lax.fori_loop(1, n, step, 0)

    def source(array):
        return cells.at[0] if array == VECTOR else ext

    def remote(src, dst, sent, received, target):
        return pltpu.make_async_remote_copy(
            src_ref=src, dst_ref=dst, send_sem=sent, recv_sem=received,
            device_id=target, device_id_type=MESH)

    def reach(array):
        return D if array == VECTOR else D - 1

    def within(step, position, size):
        if step == 0:
            return None
        return position + step >= 0 if step < 0 else position + step < size

    def guarded(conditions, act):
        conditions = [c for c in conditions if c is not None]
        if not conditions:
            act()
        else:
            pl.when(functools.reduce(jnp.logical_and, conditions))(act)

    def plane_of(t, side, d):
        return block_of(t, side, d, Z)

    def lands(side, d):
        return D - d if side == 0 else D + H - 1 + d

    def rows(step, count, sending):
        if step == 0:
            return inside
        if step < 0:
            return pl.ds(T + Y - count, count) if sending else pl.ds(T - count, count)
        return pl.ds(T, count) if sending else pl.ds(T + Y, count)

    def arrival(array, t, side, d, step):
        w = d if array == VECTOR else d + 1
        if side != t:
            w = w + H - Z + (D if step == 0 else D - 1)
        return (plane_recv if step == 0 else corner_recv).at[w - 1]

    def plane_copy(array, t, side, d, step, sent):
        q, z = plane_of(t, side, d)
        count = reach(array) - d
        ref = source(array)
        return remote(
            ref.at[slab, z + first_plane, rows(step, count, True)],
            ref.at[slab, lands(side, d), rows(step, count, False)],
            sent, arrival(array, t, side, d, step), (t, py - step, pz - q))

    def wait_for(span, sem):
        pltpu.make_async_copy(span, span, sem).wait()

    def lines(count):
        if count % Y:
            return cells.at[0, 0, 0, pl.ds(0, count)]
        a, b, c = next((a, b, count // Y // (a * b)) for a in range(1, D + 2) for b in (1, 2)
                       if count // Y % (a * b) == 0 and count // Y // (a * b) <= ZE)
        return cells.at[pl.ds(0, a), pl.ds(0, b), pl.ds(0, c), pl.ds(0, Y)]

    below, above = py > 0, py < A - 1
    beside_both, beside_one = jnp.logical_and(below, above), below != above

    order = [(a, d) for w in range(1, D + 1) for a, d in ((VECTOR, w), (POTENTIAL, w - 1)) if d]
    relays = order[-RELAYED:] if relaying(Z, B) else []

    def relay_copy(k, t):
        array, d = relays[k]
        z = plane_of(t, t, d)[1]
        return remote(source(array).at[slab, z + first_plane, inside], relayed.at[k],
                      relay_send.at[0], relay_recv.at[k], (slab, py, B - 1 if t == 0 else 0))

    def onward_copy(k, t):
        array, d = relays[k]
        return remote(relayed.at[k], source(array).at[slab, lands(t, d), inside], relay_send.at[0],
                      arrival(array, t, t, d, 0), (t, py, B - 2 if t == 0 else 1))

    def each_relay(at, act):
        for t in range(2):
            if relays:
                @pl.when(pz == at[t])
                def _(t=t):
                    for k in range(len(relays)):
                        act(k, t)

    def batches(w, sending):
        found = []
        for t in range(2):
            for side in range(2):
                wanted = [(array, d) for array, d in ((VECTOR, w), (POTENTIAL, w - 1))
                          if 1 <= d <= reach(array) and plane_of(t, side, d)[0] != 0]
                for q in sorted({plane_of(t, side, d)[0] for _, d in wanted}, key=abs):
                    mine = [(a, d) for a, d in wanted if plane_of(t, side, d)[0] == q]
                    sign = -1 if sending else 1
                    there = [None if sending else slab == t, within(sign * q, pz, B)]
                    for turned in (False, True):
                        keys = [(a, t, side, d, 0) for a, d in mine
                                if (sending and t == side and (a, d) in relays) == turned]
                        found.append(((q, 0, turned), there + [pz != 1 + t if turned else None], keys))
                    low, high = ([(a, t, side, d, step) for a, d in mine if reach(a) > d] for step in (-1, 1))
                    if sending:
                        found.append(((q, -1, False), there + [above], low))
                        found.append(((q, 1, False), there + [below], high))
                    else:
                        found.append(((q, 1, False), there + [beside_both], low + high))
                        found.append(((q, 1, False), there + [beside_one], low))
        return [batch for batch in found if batch[2]]

    def volume(keys):
        return sum(Y if step == 0 else reach(array) - d for array, _, _, d, step in keys)

    totals = {}
    for w in range(1, D + 1):
        for tag, conditions, keys in batches(w, True):
            totals[tag] = (conditions, totals.get(tag, (0, 0))[1] + volume(keys))
    slot_of = {tag: i for i, tag in enumerate(dict.fromkeys((q, step and 1, turned) for q, step, turned in totals))}
    assert len(slot_of) == group_count(Z, B)

    def group(tag):
        q, step, turned = tag
        return group_send.at[slot_of[q, step and 1, turned]]

    def send_planes(w):
        for tag, conditions, keys in batches(w, True):
            def start(tag=tag, keys=keys):
                for key in keys:
                    plane_copy(*key, group(tag)).start()
            guarded(conditions, start)

    def finish_planes():
        for tag, (conditions, size) in totals.items():
            q, step, _ = tag
            if step == 0:
                guarded(conditions, lambda tag=tag, size=size: wait_for(lines(size), group(tag)))
            elif step > 0:
                for times_, beside in ((2, beside_both), (1, beside_one)):
                    guarded([within(-q, pz, B), beside], lambda tag=tag, rows_=times_ * size: wait_for(
                        lines(rows_), group(tag)))

    def take_planes(w):
        for tag, conditions, keys in batches(w, False):
            array, t, side, d, step = keys[0]
            guarded(conditions, lambda keys=keys, sem=arrival(array, t, side, d, step): wait_for(
                lines(2 * volume(keys)), sem))

    def side_copy(array, t, step):
        ref = source(array)
        count = reach(array)
        return remote(
            ref.at[slab, pl.ds(first_plane, Z), rows(step, count, True)],
            ref.at[slab, pl.ds(D - t * H, Z), rows(step, count, False)],
            side_sems.at[0], side_sems.at[1], (t, py - step, pz))

    def send_sides():
        for step in (-1, 1):
            def both(step=step):
                for array in (VECTOR, POTENTIAL):
                    for other in range(2):
                        side_copy(array, other, step).start()
            guarded([within(-step, py, A)], both)

    def wait_sides(sem):
        count = 2 * (reach(VECTOR) + reach(POTENTIAL))
        for times_, beside in ((2, beside_both), (1, beside_one)):
            guarded([beside], lambda times_=times_: wait_for(
                cells.at[0, 0, pl.ds(0, Z), pl.ds(0, times_ * count)], sem))

    def near_copy(array):
        ref = source(array)
        return remote(
            ref.at[slab, pl.ds(first_plane, Z), inside],
            ref.at[slab, pl.ds(D - (1 - slab) * H, Z), inside],
            pair_sems.at[0], pair_sems.at[1], partner)

    def swap_copy(level):
        return remote(
            cells.at[level, 1 - slab, pl.ds(D, H), inside], swapped.at[level - 1],
            pair_sems.at[0], pair_sems.at[2], partner)

    def stat_copy(p, target):
        return remote(slots.at[p, me], slots.at[p, me], stat_sems.at[2], stat_sems.at[p], target)

    def fold(value):
        return jnp.sum(value.reshape(value.shape[0] // T, T, X), axis=0)

    def share(p, sums):
        lines = [jnp.sum(v, axis=0, keepdims=True) for v in sums]
        height = -(-len(lines) // T) * T
        lines = lines + [jnp.zeros((1, X), jnp.float32)] * (height - len(lines))
        totals = jnp.sum(jnp.concatenate(lines, axis=0), axis=1, keepdims=True)
        at = lax.broadcasted_iota(jnp.int32, (height, X), 0)
        lanes = lax.broadcasted_iota(jnp.int32, (height, X), 1)
        slots[p, me] = jnp.sum(jnp.where(at == lanes, totals, 0.0), axis=0, keepdims=True)

    def gathered(p, count):
        wait_for(slots.at[p, pl.ds(0, n - 1)], stat_sems.at[p])
        total = jnp.sum(slots[p], axis=0) * per_cell
        return [jnp.broadcast_to(total[:, s:s + 1], (1, X)) for s in range(count)]

    barrier = pltpu.get_barrier_semaphore()
    to_others(lambda t: pl.semaphore_signal(barrier, inc=1, device_id=t, device_id_type=MESH))
    loads = [pltpu.make_async_copy(
        hbm, source(array).at[slab, pl.ds(first_plane, Z), inside], load_sem.at[0])
        for array, hbm in ((VECTOR, x_hbm), (POTENTIAL, pot_hbm))]
    for load in loads:
        load.start()

    plane = pz * Z + slab * H - D
    present = [jnp.logical_and(plane + e >= 0, plane + e < B * Z) for e in range(ZE)]
    for e in range(ZE):
        if D <= e < D + H:
            continue
        @pl.when(jnp.logical_not(present[e]))
        def _(e=e):
            for ref in (cells.at[0], ext):
                for core in range(2):
                    ref[core, e] = jnp.zeros((YE, X), jnp.float32)
    for missing, at in ((py == 0, 0), (py == A - 1, T + Y)):
        @pl.when(missing)
        def _(at=at):
            for ref in (cells.at[0], ext):
                for core in range(2):
                    for e in range(ZE):
                        ref[core, e, at:at + T] = jnp.zeros((T, X), jnp.float32)
    wait_for(lines(2 * Z * Y), load_sem.at[0])

    def rough():
        lane = lax.broadcasted_iota(jnp.int32, (Y, X), 1)
        row = lax.broadcasted_iota(jnp.int32, (Y, X), 0)

        def apply(own, z):
            here = own(z)
            total = (jnp.where(row == 0, 0.0, pltpu.roll(here, 1, 0))
                     + jnp.where(row == Y - 1, 0.0, pltpu.roll(here, Y - 1, 0))
                     + jnp.where(lane == 0, 0.0, pltpu.roll(here, 1, 1))
                     + jnp.where(lane == X - 1, 0.0, pltpu.roll(here, X - 1, 1)))
            for beside in (z - 1, z + 1):
                if 0 <= beside < Z:
                    total = total + own(beside)
            return ext[slab, first_plane + z, inside] * here - total

        start = lambda z: cells[0, slab, first_plane + z, inside]
        once = lambda z: out_ref[0, z]
        sums = [jnp.zeros((T, X), jnp.float32)] * 5
        for z in range(Z):
            out_ref[0, z] = apply(start, z)
        for z in range(Z):
            zero, one, two = start(z), once(z), apply(once, z)
            for i, (u, v) in enumerate(((zero, zero), (zero, one), (one, one), (one, two), (two, two))):
                sums[i] = sums[i] + fold(u * v)
        return sums

    share(0, rough())
    pl.semaphore_wait(barrier, n - 1)

    each_relay((1, 2), lambda k, t: relay_copy(k, t).start())
    send_planes(1)
    to_others(lambda target: stat_copy(0, target).start())
    for array in (VECTOR, POTENTIAL):
        near_copy(array).start()
    send_sides()
    for w in range(2, D + 1):
        send_planes(w)

    def forward(k, t):
        relay_copy(k, t).wait_recv()
        onward_copy(k, t).start()

    each_relay((B - 1, 0), forward)

    first_lane = lax.broadcasted_iota(jnp.int32, (T, X), 1) == 0
    last_lane = lax.broadcasted_iota(jnp.int32, (T, X), 1) == X - 1
    line = lax.broadcasted_iota(jnp.int32, (T, X), 0)
    low_rows = jnp.where(jnp.logical_and(line < D - 1, py == 0), 0.0, 1.0)
    high_rows = jnp.where(jnp.logical_and(line > T - D, py == A - 1), 0.0, 1.0)

    def windows(l):
        reach = D - 1 if l < D else 0
        count = (Y + 2 * reach) // T
        starts = [T - reach + T * i for i in range(count)]
        return [(starts[i], min(CHUNK, count - i), i) for i in range(0, count, CHUNK)], count

    def depth(e):
        return max(D - e, e - (D + H - 1))

    def outer(e):
        return [b for b in (e - 1, e + 1) if depth(b) > depth(e)]

    def tiled(mask, tiles):
        return jnp.concatenate([mask] * tiles, axis=0) if tiles > 1 else mask

    def prepare(l, e):
        for start, tiles, _ in windows(l)[0]:
            at = lambda shift=0: pl.ds(start + shift, tiles * T)
            left, right = cells[l - 1, 0, e, at()], cells[l - 1, 1, e, at()]
            up = [pltpu.roll(v, 1, 1) for v in (left, right)]
            down = [pltpu.roll(v, X - 1, 1) for v in (left, right)]
            head, tail = tiled(first_lane, tiles), tiled(last_lane, tiles)
            along = (jnp.where(head, 0.0, up[0]) + jnp.where(tail, down[1], down[0]),
                     jnp.where(head, up[0], up[1]) + jnp.where(tail, 0.0, down[1]))
            for core, here in enumerate((left, right)):
                around = (cells[l - 1, core, e, at(-1)] + cells[l - 1, core, e, at(1)]) + along[core]
                for b in (e - 1, e + 1):
                    if b not in outer(e):
                        around = around + cells[l - 1, core, b, at()]
                if l == 1:
                    image = -around
                else:
                    image = ((DIAGONAL - shifts[l - 1]) + ext[core, e, at()]) * here - around
                    image = image - taus[l - 1] * cells[l - 2, core, e, at()]
                cells[l, core, e, at()] = image

    def finish(l, e):
        chunks, count = windows(l)
        for core in range(2):
            for start, tiles, first in chunks:
                at = pl.ds(start, tiles * T)
                image = cells[l, core, e, at]
                for b in outer(e):
                    image = image - cells[l - 1, core, b, at]
                if l == 1:
                    image = ((DIAGONAL - shifts[0]) + ext[core, e, at]) * cells[0, core, e, at] + image
                if not D <= e < D + H:
                    image = image * present[e].astype(jnp.float32)
                for i in range(tiles):
                    part = image[i * T:(i + 1) * T]
                    if l < D and first + i == 0:
                        part = part * low_rows
                    if l < D and first + i == count - 1:
                        part = part * high_rows
                    cells[l, core, e, pl.ds(start + i * T, T)] = part

    def wave(w):
        return [(l, e) for l in range(1, D + 1) for e in range(l, ZE - l) if max(l + depth(e), 0) == w]

    def measure(pairs, at, sums=None):
        sums = sums or [jnp.zeros((T, X), jnp.float32)] * len(pairs)
        for core in range(2):
            for e in at:
                held = {k: cells[k, core, e, inside] for k in sorted({k for pair in pairs for k in pair})}
                for i, (k, l) in enumerate(pairs):
                    sums[i] = sums[i] + fold(held[k] * held[l])
        return sums

    wait_for(lines(2 * Z * Y), pair_sems.at[1])
    wait_sides(side_sems.at[1])
    ready = []
    for reached in range(2):
        if reached:
            take_planes(reached)
        for e in range(1, ZE - 1):
            if depth(e) <= reached and e not in ready:
                prepare(1, e)
                ready.append(e)

    m0, m1, m2, m3, m4 = gathered(0, 5)
    some = m0 > 1e-30
    over = 1.0 / jnp.where(some, m0, 1.0)
    m1, m2, m3, m4 = m1 * over, m2 * over, m3 * over, m4 * over
    c2 = m2 - m1 * m1
    c3 = m3 - 3.0 * m1 * m2 + 2.0 * m1 * m1 * m1
    c4 = m4 - 4.0 * m1 * m3 + 6.0 * m1 * m1 * m2 - 3.0 * m1 * m1 * m1 * m1
    down = 1.0 / jnp.maximum(c2, 1e-3)
    slope = c3 * down
    bound = lambda value, low, high: jnp.minimum(jnp.maximum(value, low), high)
    alpha = [bound(jnp.where(some, DIAGONAL + a, CENTER), LEAST_SHIFT, MOST_SHIFT) for a in (m1, m1 + slope)]
    square = [bound(b, LEAST_SQUARE, MOST_SQUARE) for b in (c2, c4 * down - c2 - slope * slope)]
    shifts = [alpha[0]] + [alpha[1]] * (D - 1)
    taus = [None, square[0]] + [square[1]] * (D - 2)

    early = [(k, l) for l in range(D) for k in range(l + 1)]
    late = [(k, D) for k in range(D + 1)]
    held = range(D, D + H)
    done = [e for e in held if depth(e) < 0]
    def prepare_all(entries):
        for l, e in entries:
            if l > 1 or e not in ready:
                prepare(l, e)

    for entry in wave(0):
        prepare_all([entry])
        finish(*entry)
    prepare_all(wave(1))
    for w in range(1, D + 1):
        if w > 1:
            take_planes(w)
        for l, e in wave(w):
            finish(l, e)
        swap_copy(w).start()
        if w == D - 1:
            sums = measure(early, held)
            last = measure(late, done)
        if w < D:
            prepare_all(wave(w + 1))
    sums = sums + measure(late, [e for e in held if e not in done], last)
    share(1, sums)
    to_others(lambda target: stat_copy(1, target).start())
    wait_for(lines((2 * Z + D * H) * Y), pair_sems.at[0])
    wait_sides(side_sems.at[0])
    if relays:
        wait_for(relayed, relay_send.at[0])
    finish_planes()
    wait_for(swapped, pair_sems.at[2])
    for i in range(H):
        mine, other = slab * H + i, (1 - slab) * H + i
        out_ref[0, mine] = cells[0, slab, D + i, inside]
        out_ref[0, other] = cells[0, slab, first_plane + other, inside]
        for q in range(1, D + 1):
            out_ref[q, mine] = cells[q, slab, D + i, inside]
            out_ref[q, other] = swapped[q - 1, i]
    stats = gathered(1, len(sums))
    scale = 1.0 / jnp.sqrt(stats[0] + EPSILON)
    inner = {}
    for (k, l), value in zip(early + late, stats):
        inner[k, l] = inner[l, k] = value * scale * scale
    removed, betas = [], []
    found = advance(D, inner, shifts, taus, removed, betas)
    for v in range(D):
        tri_ref[0:1, v:v + 1] = removed[v][v][:, 0:1]
        tri_ref[1:2, v:v + 1] = betas[v][:, 0:1]
    found = [{q: t * scale for q, t in coords.items()} for coords in found]

    for r, value in enumerate([scale] + [coords[q] for coords in found for q in range(len(coords))]):
        coeff_ref[r:r + 1] = value

    wait_for(slots.at[pl.ds(0, 2), pl.ds(0, n - 1)], stat_sems.at[2])


def block_of(t, side, d, Z):
    z = t * (Z // 2) - d if side == 0 else (t + 1) * (Z // 2) - 1 + d
    return z // Z, z % Z


def relaying(Z, B):
    return B == RELAY_RING and block_of(0, 0, ITERS, Z)[0] == -1


def group_count(Z, B):
    blocks = [[block_of(t, side, d, Z)[0] for d in range(1, ITERS + 1)] for t in range(2) for side in range(2)]
    straight = {q for row in blocks for q in row} - {0}
    beside = {q for row in blocks for q in row[:-1]} - {0}
    return len(straight) + len(beside) + (2 if relaying(Z, B) else 0)


def write_out(columns, coeff_ref, tri_ref, basis_out, tri_out, basis, sems):
    count, Z = columns.shape[:2]
    small = pltpu.make_async_copy(tri_ref, tri_out, sems.at[1])
    small.start()
    for z in range(Z):
        held = [columns[q, z] for q in range(count)]
        for k in range(count):
            total = None
            for q in reversed(range(k + 1)):
                r = 0 if k == 0 else k * (k + 1) // 2 + q
                term = coeff_ref[r:r + 1] * held[q]
                total = term if total is None else total + term
            basis[k, z] = total
        pltpu.make_async_copy(basis.at[:, z], basis_out.at[:, z], sems.at[0]).start()
    pltpu.make_async_copy(basis, basis_out, sems.at[0]).wait()
    small.wait()


def shards(sizes, start_vector, potential):
    Z, Y, X = start_vector.shape
    n = sizes[0] * sizes[1] * sizes[2]
    f32 = jnp.float32
    H, D, T = Z // 2, ITERS, SUBLANES
    assert sizes[0] == 2 and Z % 2 == 0 and H <= D and Y >= D and Y % T == 0
    vmem = pl.BlockSpec(memory_space=pltpu.VMEM)
    hbm = pl.BlockSpec(memory_space=pl.ANY)
    dma = pltpu.SemaphoreType.DMA
    extended = (2, H + 2 * D, Y + 2 * T, X)
    coeffs = -(-((D + 1) * (D + 2) // 2) // T) * T
    held = pl.pallas_call(
        functools.partial(kernel, sizes, 1.0 / (start_vector.size * n)),
        out_shape=(pltpu.VMEM((D + 1, Z, Y, X), f32), pltpu.VMEM((coeffs, X), f32), pltpu.VMEM((2, D), f32)),
        in_specs=[hbm, hbm],
        out_specs=(vmem,) * 3,
        scratch_shapes=[
            pltpu.VMEM((D + 1,) + extended, f32),
            pltpu.VMEM(extended, f32),
            pltpu.VMEM((D, H, Y, X), f32),
            pltpu.VMEM((RELAYED, Y, X), f32),
            pltpu.VMEM((2, n, 1, X), f32),
            dma((group_count(Z, sizes[2]),)),
            dma((D + max(0, D - Z + H),)),
            dma((D - 1 + max(0, D - 1 - Z + H),)),
            dma((RELAYED,)),
            dma((1,)),
            dma((2,)),
            dma((3,)),
            dma((3,)),
            dma((1,)),
        ],
        compiler_params=pltpu.CompilerParams(collective_id=0, has_side_effects=True),
    )(start_vector, potential)
    return tuple(pl.pallas_call(
        write_out,
        out_shape=(jax.ShapeDtypeStruct((D + 1, Z, Y, X), f32), jax.ShapeDtypeStruct((2, D), f32)),
        in_specs=[vmem] * 3,
        out_specs=(hbm, hbm),
        scratch_shapes=[pltpu.VMEM((D + 1, Z, Y, X), f32), dma((2,))],
    )(*(pltpu.with_memory_space_constraint(ref, pltpu.VMEM) for ref in held)))


def solution(mesh):
    sizes = tuple(mesh.shape[name] for name in AXES)
    in_specs = (P("pz", "py", "slab"), P("pz", "py", "slab"))
    out_specs = (P(None, "pz", "py", "slab"), P())
    return jax.shard_map(functools.partial(shards, sizes), mesh=mesh, in_specs=in_specs,
                         out_specs=out_specs, check_vma=False)
```

```python
import functools

import jax
import jax.numpy as jnp
from jax import lax
from jax.experimental import pallas as pl
from jax.experimental.pallas import tpu as pltpu
from jax.sharding import PartitionSpec as P

ITERS = 5
EPSILON = 1e-06
DIAGONAL = 6.0
SUBLANES = 8
MESH = pl.DeviceIdType.MESH
AXES = ("slab", "py", "pz")
UNROLLED = 64
CENTER = 8.25
LEAST_SQUARE, MOST_SQUARE = 0.25, 40.0
LEAST_SHIFT, MOST_SHIFT = 0.5, 16.5
VECTOR, POTENTIAL = 0, 1
RELAY_RING, RELAYED = 4, 5
CHUNK = 3


def times(coeff, columns):
    total = {}
    for k, c in coeff.items():
        for q, value in columns[k].items():
            term = c * value
            total[q] = total[q] + term if q in total else term
    return total


def dot(left, right):
    total = None
    for q, value in left.items():
        if q in right:
            term = value * right[q]
            total = term if total is None else total + term
    return 0.0 if total is None else total


def advance(steps, inner, shifts, taus, removed, betas):
    vectors = [{0: 1.0}]
    image_of = []
    for i in range(steps):
        column = {i + 1: 1.0, i: shifts[i]}
        if taus[i] is not None:
            column[i - 1] = taus[i]
        image_of.append(column)
    gram, lowered = {}, []
    for n in range(steps):
        for k in range(len(lowered), n + 1):
            lowered.append({
                q: dot(vectors[k], {b: inner[q, b] for b in vectors[k]})
                for q in range(n + 1)})
            for l in range(k + 1):
                gram[k, l] = gram[l, k] = dot(vectors[l], lowered[k])
        known = {n: shifts[n]}
        if n > 0:
            known[n - 1] = betas[n - 1]
            rest = times(vectors[n], image_of)
            for k, y in known.items():
                for q, value in vectors[k].items():
                    rest[q] = rest[q] - y * value if q in rest else -y * value
        else:
            rest = {n + 1: 1.0}
        rest_lowered = {
            q: dot(rest, {b: inner[q, b] for b in rest}) for q in range(n + 2)}
        along = {k: dot(vectors[k], rest_lowered) for k in range(n + 1)}
        first = {
            k: along[k] + dot(known, {l: gram[k, l] for l in known}) for k in range(n + 1)}
        excess = {k: first[k] - known[k] if k in known else first[k] for k in range(n + 1)}
        coeffs = {
            k: along[k] - dot(excess, {
                l: gram[k, l] - 1.0 if k == l else gram[k, l] for l in range(n + 1)})
            for k in range(n + 1)}
        square = dot(rest, rest_lowered)
        for k in range(n + 1):
            back = dot(coeffs, {l: gram[k, l] for l in range(n + 1)})
            square = square + coeffs[k] * (back - 2.0 * along[k])
        beta = jnp.sqrt(jnp.maximum(square, 0.0) + EPSILON)
        inverse = 1.0 / beta
        image = dict(rest)
        for k in range(n + 1):
            for q, value in vectors[k].items():
                term = coeffs[k] * value
                image[q] = image[q] - term if q in image else -term
        vectors.append({q: value * inverse for q, value in image.items()})
        removed.append({k: coeffs[k] + known[k] if k in known else coeffs[k] for k in coeffs})
        betas.append(beta)
    return vectors[1:]


def kernel(sizes, per_cell, x_hbm, pot_hbm, out_ref, coeff_ref, tri_ref, cells, ext, swapped, relayed, slots,
           group_send, plane_recv, corner_recv, relay_recv, relay_send, pass_send, side_sems, pair_sems, stat_sems, load_sem):
    Z, Y, X = x_hbm.shape
    S, A, B = sizes
    n = S * A * B
    H = Z // 2
    D = ITERS
    T = SUBLANES
    ZE, YE = H + 2 * D, Y + 2 * T
    slab, py, pz = (lax.axis_index(name) for name in AXES)
    me = (slab * A + py) * B + pz
    partner = (1 - slab, py, pz)
    first_plane = D - slab * H
    inside = pl.ds(T, Y)

    def to_others(act):
        if n <= UNROLLED:
            slabs = [lax.rem(slab + i, S) for i in range(S)]
            pys = [lax.rem(py + i, A) for i in range(A)]
            pzs = [lax.rem(pz + i, B) for i in range(B)]
            far = sorted(
                ((i, j, k) for i in range(S) for j in range(A) for k in range(B)),
                key=lambda t: -(min(t[1], A - t[1]) + min(t[2], B - t[2])),
            )
            for i, j, k in far:
                if i or j or k:
                    act((slabs[i], pys[j], pzs[k]))
        else:
            def step(d, carry):
                t = lax.rem(me + d, n)
                act((t // (A * B), lax.rem(t // B, A), lax.rem(t, B)))
                return carry
            lax.fori_loop(1, n, step, 0)

    def source(array):
        return cells.at[0] if array == VECTOR else ext

    def remote(src, dst, sent, received, target):
        return pltpu.make_async_remote_copy(
            src_ref=src, dst_ref=dst, send_sem=sent, recv_sem=received,
            device_id=target, device_id_type=MESH)

    def reach(array):
        return D if array == VECTOR else D - 1

    def within(step, position, size):
        if step == 0:
            return None
        return position + step >= 0 if step < 0 else position + step < size

    def guarded(conditions, act):
        conditions = [c for c in conditions if c is not None]
        if not conditions:
            act()
        else:
            pl.when(functools.reduce(jnp.logical_and, conditions))(act)

    def plane_of(t, side, d):
        return block_of(t, side, d, Z)

    def lands(side, d):
        return D - d if side == 0 else D + H - 1 + d

    def rows(step, count, sending):
        if step == 0:
            return inside
        if step < 0:
            return pl.ds(T + Y - count, count) if sending else pl.ds(T - count, count)
        return pl.ds(T, count) if sending else pl.ds(T + Y, count)

    def arrival(array, t, side, d, step):
        w = d if array == VECTOR else d + 1
        if side != t:
            w = w + H - Z + (D if step == 0 else D - 1)
        return (plane_recv if step == 0 else corner_recv).at[w - 1]

    def plane_copy(array, t, side, d, step, sent):
        q, z = plane_of(t, side, d)
        count = reach(array) - d
        ref = source(array)
        return remote(
            ref.at[slab, z + first_plane, rows(step, count, True)],
            ref.at[slab, lands(side, d), rows(step, count, False)],
            sent, arrival(array, t, side, d, step), (t, py - step, pz - q))

    def wait_for(span, sem):
        pltpu.make_async_copy(span, span, sem).wait()

    def lines(count):
        if count % Y:
            return cells.at[0, 0, 0, pl.ds(0, count)]
        a, b, c = next((a, b, count // Y // (a * b)) for a in range(1, D + 2) for b in (1, 2)
                       if count // Y % (a * b) == 0 and count // Y // (a * b) <= ZE)
        return cells.at[pl.ds(0, a), pl.ds(0, b), pl.ds(0, c), pl.ds(0, Y)]

    below, above = py > 0, py < A - 1
    beside_both, beside_one = jnp.logical_and(below, above), below != above

    order = [(a, d) for w in range(1, D + 1) for a, d in ((VECTOR, w), (POTENTIAL, w - 1)) if d]
    relays = order[-RELAYED:] if relaying(Z, B) else []

    def relay_copy(k, t):
        array, d = relays[k]
        z = plane_of(t, t, d)[1]
        return remote(source(array).at[slab, z + first_plane, inside], relayed.at[k],
                      relay_send.at[0], relay_recv.at[k], (slab, py, B - 1 if t == 0 else 0))

    def onward_copy(k, t):
        array, d = relays[k]
        return remote(relayed.at[k], source(array).at[slab, lands(t, d), inside], relay_send.at[0],
                      arrival(array, t, t, d, 0), (t, py, B - 2 if t == 0 else 1))

    def each_relay(at, act):
        for t in range(2):
            if relays:
                @pl.when(pz == at[t])
                def _(t=t):
                    for k in range(len(relays)):
                        act(k, t)

    def batches(w, sending):
        found = []
        for t in range(2):
            for side in range(2):
                wanted = [(array, d) for array, d in ((VECTOR, w), (POTENTIAL, w - 1))
                          if 1 <= d <= reach(array) and plane_of(t, side, d)[0] != 0]
                if passing(Z) and side != t:
                    continue
                for q in sorted({plane_of(t, side, d)[0] for _, d in wanted}, key=abs):
                    mine = [(a, d) for a, d in wanted if plane_of(t, side, d)[0] == q]
                    sign = -1 if sending else 1
                    there = [None if sending else slab == t, within(sign * q, pz, B)]
                    for turned in (False, True):
                        keys = [(a, t, side, d, 0) for a, d in mine
                                if (sending and t == side and (a, d) in relays) == turned]
                        found.append(((q, 0, turned), there + [pz != 1 + t if turned else None], keys))
                    low, high = ([(a, t, side, d, step) for a, d in mine if reach(a) > d] for step in (-1, 1))
                    if sending:
                        found.append(((q, -1, False), there + [above], low))
                        found.append(((q, 1, False), there + [below], high))
                    else:
                        found.append(((q, 1, False), there + [beside_both], low + high))
                        found.append(((q, 1, False), there + [beside_one], low))
        return [batch for batch in found if batch[2]]

    def volume(keys):
        return sum(Y if step == 0 else reach(array) - d for array, _, _, d, step in keys)

    totals = {}
    for w in range(1, D + 1):
        for tag, conditions, keys in batches(w, True):
            totals[tag] = (conditions, totals.get(tag, (0, 0))[1] + volume(keys))
    slot_of = {tag: i for i, tag in enumerate(dict.fromkeys((q, step and 1, turned) for q, step, turned in totals))}
    assert len(slot_of) == group_count(Z, B)

    def group(tag):
        q, step, turned = tag
        return group_send.at[slot_of[q, step and 1, turned]]

    def send_planes(w):
        for tag, conditions, keys in batches(w, True):
            def start(tag=tag, keys=keys):
                for key in keys:
                    plane_copy(*key, group(tag)).start()
            guarded(conditions, start)

    def finish_planes():
        for tag, (conditions, size) in totals.items():
            q, step, _ = tag
            if step == 0:
                guarded(conditions, lambda tag=tag, size=size: wait_for(lines(size), group(tag)))
            elif step > 0:
                for times_, beside in ((2, beside_both), (1, beside_one)):
                    guarded([within(-q, pz, B), beside], lambda tag=tag, rows_=times_ * size: wait_for(
                        lines(rows_), group(tag)))

    def take_planes(w):
        for tag, conditions, keys in batches(w, False):
            array, t, side, d, step = keys[0]
            guarded(conditions, lambda keys=keys, sem=arrival(array, t, side, d, step): wait_for(
                lines(2 * volume(keys)), sem))

    def pass_copy(t):
        return remote(
            cells.at[0, pl.ds(0, 2), lands(t, 1), inside], cells.at[0, pl.ds(0, 2), lands(t, D), inside],
            pass_send.at[0], plane_recv.at[D], partner)

    def each_pass(receiving, act):
        for t in range(2):
            if passing(Z):
                guarded([slab == (1 - t if receiving else t), within(-1 if t == 0 else 1, pz, B)],
                        lambda t=t: act(t))

    def side_copy(array, t, step):
        ref = source(array)
        count = reach(array)
        return remote(
            ref.at[slab, pl.ds(first_plane, Z), rows(step, count, True)],
            ref.at[slab, pl.ds(D - t * H, Z), rows(step, count, False)],
            side_sems.at[0], side_sems.at[1], (t, py - step, pz))

    def send_sides():
        for step in (-1, 1):
            def both(step=step):
                for array in (VECTOR, POTENTIAL):
                    for other in range(2):
                        side_copy(array, other, step).start()
            guarded([within(-step, py, A)], both)

    def wait_sides(sem):
        count = 2 * (reach(VECTOR) + reach(POTENTIAL))
        for times_, beside in ((2, beside_both), (1, beside_one)):
            guarded([beside], lambda times_=times_: wait_for(
                cells.at[0, 0, pl.ds(0, Z), pl.ds(0, times_ * count)], sem))

    def near_copy(array):
        ref = source(array)
        return remote(
            ref.at[slab, pl.ds(first_plane, Z), inside],
            ref.at[slab, pl.ds(D - (1 - slab) * H, Z), inside],
            pair_sems.at[0], pair_sems.at[1], partner)

    def swap_copy(level):
        return remote(
            cells.at[level, 1 - slab, pl.ds(D, H), inside], swapped.at[level - 1],
            pair_sems.at[0], pair_sems.at[2], partner)

    def stat_copy(p, target):
        return remote(slots.at[p, me], slots.at[p, me], stat_sems.at[2], stat_sems.at[p], target)

    def fold(value):
        return jnp.sum(value.reshape(value.shape[0] // T, T, X), axis=0)

    def share(p, sums):
        lines = [jnp.sum(v, axis=0, keepdims=True) for v in sums]
        height = -(-len(lines) // T) * T
        lines = lines + [jnp.zeros((1, X), jnp.float32)] * (height - len(lines))
        totals = jnp.sum(jnp.concatenate(lines, axis=0), axis=1, keepdims=True)
        at = lax.broadcasted_iota(jnp.int32, (height, X), 0)
        lanes = lax.broadcasted_iota(jnp.int32, (height, X), 1)
        slots[p, me] = jnp.sum(jnp.where(at == lanes, totals, 0.0), axis=0, keepdims=True)

    def gathered(p, count):
        wait_for(slots.at[p, pl.ds(0, n - 1)], stat_sems.at[p])
        total = jnp.sum(slots[p], axis=0) * per_cell
        return [jnp.broadcast_to(total[:, s:s + 1], (1, X)) for s in range(count)]

    barrier = pltpu.get_barrier_semaphore()
    to_others(lambda t: pl.semaphore_signal(barrier, inc=1, device_id=t, device_id_type=MESH))
    loads = [pltpu.make_async_copy(
        hbm, source(array).at[slab, pl.ds(first_plane, Z), inside], load_sem.at[0])
        for array, hbm in ((VECTOR, x_hbm), (POTENTIAL, pot_hbm))]
    for load in loads:
        load.start()

    plane = pz * Z + slab * H - D
    present = [jnp.logical_and(plane + e >= 0, plane + e < B * Z) for e in range(ZE)]
    for e in range(ZE):
        if D <= e < D + H:
            continue
        @pl.when(jnp.logical_not(present[e]))
        def _(e=e):
            for ref in (cells.at[0], ext):
                for core in range(2):
                    ref[core, e] = jnp.zeros((YE, X), jnp.float32)
    for missing, at in ((py == 0, 0), (py == A - 1, T + Y)):
        @pl.when(missing)
        def _(at=at):
            for ref in (cells.at[0], ext):
                for core in range(2):
                    for e in range(ZE):
                        ref[core, e, at:at + T] = jnp.zeros((T, X), jnp.float32)
    wait_for(lines(2 * Z * Y), load_sem.at[0])

    def rough():
        lane = lax.broadcasted_iota(jnp.int32, (Y, X), 1)
        row = lax.broadcasted_iota(jnp.int32, (Y, X), 0)

        def apply(own, z):
            here = own(z)
            total = (jnp.where(row == 0, 0.0, pltpu.roll(here, 1, 0))
                     + jnp.where(row == Y - 1, 0.0, pltpu.roll(here, Y - 1, 0))
                     + jnp.where(lane == 0, 0.0, pltpu.roll(here, 1, 1))
                     + jnp.where(lane == X - 1, 0.0, pltpu.roll(here, X - 1, 1)))
            for beside in (z - 1, z + 1):
                if 0 <= beside < Z:
                    total = total + own(beside)
            return ext[slab, first_plane + z, inside] * here - total

        start = lambda z: cells[0, slab, first_plane + z, inside]
        once = lambda z: out_ref[0, z]
        sums = [jnp.zeros((T, X), jnp.float32)] * 5
        for z in range(Z):
            out_ref[0, z] = apply(start, z)
        for z in range(Z):
            zero, one, two = start(z), once(z), apply(once, z)
            for i, (u, v) in enumerate(((zero, zero), (zero, one), (one, one), (one, two), (two, two))):
                sums[i] = sums[i] + fold(u * v)
        return sums

    share(0, rough())
    pl.semaphore_wait(barrier, n - 1)

    each_relay((1, 2), lambda k, t: relay_copy(k, t).start())
    send_planes(1)
    to_others(lambda target: stat_copy(0, target).start())
    for array in (VECTOR, POTENTIAL):
        near_copy(array).start()
    send_sides()
    for w in range(2, D + 1):
        send_planes(w)

    def forward(k, t):
        relay_copy(k, t).wait_recv()
        onward_copy(k, t).start()

    each_relay((B - 1, 0), forward)

    first_lane = lax.broadcasted_iota(jnp.int32, (T, X), 1) == 0
    last_lane = lax.broadcasted_iota(jnp.int32, (T, X), 1) == X - 1
    line = lax.broadcasted_iota(jnp.int32, (T, X), 0)
    low_rows = jnp.where(jnp.logical_and(line < D - 1, py == 0), 0.0, 1.0)
    high_rows = jnp.where(jnp.logical_and(line > T - D, py == A - 1), 0.0, 1.0)

    def windows(l):
        reach = D - 1 if l < D else 0
        count = (Y + 2 * reach) // T
        starts = [T - reach + T * i for i in range(count)]
        return [(starts[i], min(CHUNK, count - i), i) for i in range(0, count, CHUNK)], count

    def depth(e):
        return max(D - e, e - (D + H - 1))

    def outer(e):
        return [b for b in (e - 1, e + 1) if depth(b) > depth(e)]

    def tiled(mask, tiles):
        return jnp.concatenate([mask] * tiles, axis=0) if tiles > 1 else mask

    def prepare(l, e):
        for start, tiles, _ in windows(l)[0]:
            at = lambda shift=0: pl.ds(start + shift, tiles * T)
            left, right = cells[l - 1, 0, e, at()], cells[l - 1, 1, e, at()]
            up = [pltpu.roll(v, 1, 1) for v in (left, right)]
            down = [pltpu.roll(v, X - 1, 1) for v in (left, right)]
            head, tail = tiled(first_lane, tiles), tiled(last_lane, tiles)
            along = (jnp.where(head, 0.0, up[0]) + jnp.where(tail, down[1], down[0]),
                     jnp.where(head, up[0], up[1]) + jnp.where(tail, 0.0, down[1]))
            for core, here in enumerate((left, right)):
                around = (cells[l - 1, core, e, at(-1)] + cells[l - 1, core, e, at(1)]) + along[core]
                for b in (e - 1, e + 1):
                    if b not in outer(e):
                        around = around + cells[l - 1, core, b, at()]
                if l == 1:
                    image = -around
                else:
                    image = ((DIAGONAL - shifts[l - 1]) + ext[core, e, at()]) * here - around
                    image = image - taus[l - 1] * cells[l - 2, core, e, at()]
                cells[l, core, e, at()] = image

    def finish(l, e):
        chunks, count = windows(l)
        for core in range(2):
            for start, tiles, first in chunks:
                at = pl.ds(start, tiles * T)
                image = cells[l, core, e, at]
                for b in outer(e):
                    image = image - cells[l - 1, core, b, at]
                if l == 1:
                    image = ((DIAGONAL - shifts[0]) + ext[core, e, at]) * cells[0, core, e, at] + image
                if not D <= e < D + H:
                    image = image * present[e].astype(jnp.float32)
                for i in range(tiles):
                    part = image[i * T:(i + 1) * T]
                    if l < D and first + i == 0:
                        part = part * low_rows
                    if l < D and first + i == count - 1:
                        part = part * high_rows
                    cells[l, core, e, pl.ds(start + i * T, T)] = part

    def wave(w):
        return [(l, e) for l in range(1, D + 1) for e in range(l, ZE - l) if max(l + depth(e), 0) == w]

    def measure(pairs, at, sums=None):
        sums = sums or [jnp.zeros((T, X), jnp.float32)] * len(pairs)
        for core in range(2):
            for e in at:
                held = {k: cells[k, core, e, inside] for k in sorted({k for pair in pairs for k in pair})}
                for i, (k, l) in enumerate(pairs):
                    sums[i] = sums[i] + fold(held[k] * held[l])
        return sums

    wait_for(lines(2 * Z * Y), pair_sems.at[1])
    wait_sides(side_sems.at[1])
    ready = []
    for reached in range(2):
        if reached:
            take_planes(reached)
            each_pass(False, lambda t: pass_copy(t).start())
        for e in range(1, ZE - 1):
            if depth(e) <= reached and e not in ready:
                prepare(1, e)
                ready.append(e)

    m0, m1, m2, m3, m4 = gathered(0, 5)
    some = m0 > 1e-30
    over = 1.0 / jnp.where(some, m0, 1.0)
    m1, m2, m3, m4 = m1 * over, m2 * over, m3 * over, m4 * over
    c2 = m2 - m1 * m1
    c3 = m3 - 3.0 * m1 * m2 + 2.0 * m1 * m1 * m1
    c4 = m4 - 4.0 * m1 * m3 + 6.0 * m1 * m1 * m2 - 3.0 * m1 * m1 * m1 * m1
    down = 1.0 / jnp.maximum(c2, 1e-3)
    slope = c3 * down
    bound = lambda value, low, high: jnp.minimum(jnp.maximum(value, low), high)
    alpha = [bound(jnp.where(some, DIAGONAL + a, CENTER), LEAST_SHIFT, MOST_SHIFT) for a in (m1, m1 + slope)]
    square = [bound(b, LEAST_SQUARE, MOST_SQUARE) for b in (c2, c4 * down - c2 - slope * slope)]
    shifts = [alpha[0]] + [alpha[1]] * (D - 1)
    taus = [None, square[0]] + [square[1]] * (D - 2)

    early = [(k, l) for l in range(D) for k in range(l + 1)]
    late = [(k, D) for k in range(D + 1)]
    held = range(D, D + H)
    done = [e for e in held if depth(e) < 0]
    def prepare_all(entries):
        for l, e in entries:
            if l > 1 or e not in ready:
                prepare(l, e)

    for entry in wave(0):
        prepare_all([entry])
        finish(*entry)
    prepare_all(wave(1))
    for w in range(1, D + 1):
        if w > 1:
            take_planes(w)
        if w == D:
            each_pass(True, lambda t: pass_copy(t).wait_recv())
        for l, e in wave(w):
            finish(l, e)
        swap_copy(w).start()
        if w == D - 1:
            sums = measure(early, held)
            last = measure(late, done)
        if w < D:
            prepare_all(wave(w + 1))
    sums = sums + measure(late, [e for e in held if e not in done], last)
    share(1, sums)
    to_others(lambda target: stat_copy(1, target).start())
    wait_for(lines((2 * Z + D * H) * Y), pair_sems.at[0])
    wait_sides(side_sems.at[0])
    if relays:
        wait_for(relayed, relay_send.at[0])
    finish_planes()
    each_pass(False, lambda t: pass_copy(t).wait_send())
    wait_for(swapped, pair_sems.at[2])
    for i in range(H):
        mine, other = slab * H + i, (1 - slab) * H + i
        out_ref[0, mine] = cells[0, slab, D + i, inside]
        out_ref[0, other] = cells[0, slab, first_plane + other, inside]
        for q in range(1, D + 1):
            out_ref[q, mine] = cells[q, slab, D + i, inside]
            out_ref[q, other] = swapped[q - 1, i]
    stats = gathered(1, len(sums))
    scale = 1.0 / jnp.sqrt(stats[0] + EPSILON)
    inner = {}
    for (k, l), value in zip(early + late, stats):
        inner[k, l] = inner[l, k] = value * scale * scale
    removed, betas = [], []
    found = advance(D, inner, shifts, taus, removed, betas)
    for v in range(D):
        tri_ref[0:1, v:v + 1] = removed[v][v][:, 0:1]
        tri_ref[1:2, v:v + 1] = betas[v][:, 0:1]
    found = [{q: t * scale for q, t in coords.items()} for coords in found]

    for r, value in enumerate([scale] + [coords[q] for coords in found for q in range(len(coords))]):
        coeff_ref[r:r + 1] = value

    wait_for(slots.at[pl.ds(0, 2), pl.ds(0, n - 1)], stat_sems.at[2])


def block_of(t, side, d, Z):
    z = t * (Z // 2) - d if side == 0 else (t + 1) * (Z // 2) - 1 + d
    return z // Z, z % Z


def relaying(Z, B):
    return B == RELAY_RING and block_of(0, 0, ITERS, Z)[0] == -1


def passing(Z):
    return Z - Z // 2 + 1 == ITERS


def group_count(Z, B):
    blocks = [[block_of(t, side, d, Z)[0] for d in range(1, ITERS + 1)] for t in range(2) for side in range(2)
              if side == t or not passing(Z)]
    straight = {q for row in blocks for q in row} - {0}
    beside = {q for row in blocks for q in row[:-1]} - {0}
    return len(straight) + len(beside) + (2 if relaying(Z, B) else 0)


def write_out(columns, coeff_ref, tri_ref, basis_out, tri_out, basis, sems):
    count, Z = columns.shape[:2]
    small = pltpu.make_async_copy(tri_ref, tri_out, sems.at[1])
    small.start()
    for z in range(Z):
        held = [columns[q, z] for q in range(count)]
        for k in range(count):
            total = None
            for q in reversed(range(k + 1)):
                r = 0 if k == 0 else k * (k + 1) // 2 + q
                term = coeff_ref[r:r + 1] * held[q]
                total = term if total is None else total + term
            basis[k, z] = total
        pltpu.make_async_copy(basis.at[:, z], basis_out.at[:, z], sems.at[0]).start()
    pltpu.make_async_copy(basis, basis_out, sems.at[0]).wait()
    small.wait()


def shards(sizes, start_vector, potential):
    Z, Y, X = start_vector.shape
    n = sizes[0] * sizes[1] * sizes[2]
    f32 = jnp.float32
    H, D, T = Z // 2, ITERS, SUBLANES
    assert sizes[0] == 2 and Z % 2 == 0 and H <= D and Y >= D and Y % T == 0
    vmem = pl.BlockSpec(memory_space=pltpu.VMEM)
    hbm = pl.BlockSpec(memory_space=pl.ANY)
    dma = pltpu.SemaphoreType.DMA
    extended = (2, H + 2 * D, Y + 2 * T, X)
    coeffs = -(-((D + 1) * (D + 2) // 2) // T) * T
    held = pl.pallas_call(
        functools.partial(kernel, sizes, 1.0 / (start_vector.size * n)),
        out_shape=(pltpu.VMEM((D + 1, Z, Y, X), f32), pltpu.VMEM((coeffs, X), f32), pltpu.VMEM((2, D), f32)),
        in_specs=[hbm, hbm],
        out_specs=(vmem,) * 3,
        scratch_shapes=[
            pltpu.VMEM((D + 1,) + extended, f32),
            pltpu.VMEM(extended, f32),
            pltpu.VMEM((D, H, Y, X), f32),
            pltpu.VMEM((RELAYED, Y, X), f32),
            pltpu.VMEM((2, n, 1, X), f32),
            dma((group_count(Z, sizes[2]),)),
            dma((D + max(0, D - Z + H),)),
            dma((D - 1 + max(0, D - 1 - Z + H),)),
            dma((RELAYED,)),
            dma((1,)),
            dma((1,)),
            dma((2,)),
            dma((3,)),
            dma((3,)),
            dma((1,)),
        ],
        compiler_params=pltpu.CompilerParams(collective_id=0, has_side_effects=True),
    )(start_vector, potential)
    return tuple(pl.pallas_call(
        write_out,
        out_shape=(jax.ShapeDtypeStruct((D + 1, Z, Y, X), f32), jax.ShapeDtypeStruct((2, D), f32)),
        in_specs=[vmem] * 3,
        out_specs=(hbm, hbm),
        scratch_shapes=[pltpu.VMEM((D + 1, Z, Y, X), f32), dma((2,))],
    )(*(pltpu.with_memory_space_constraint(ref, pltpu.VMEM) for ref in held)))


def solution(mesh):
    sizes = tuple(mesh.shape[name] for name in AXES)
    in_specs = (P("pz", "py", "slab"), P("pz", "py", "slab"))
    out_specs = (P(None, "pz", "py", "slab"), P())
    return jax.shard_map(functools.partial(shards, sizes), mesh=mesh, in_specs=in_specs,
                         out_specs=out_specs, check_vma=False)
```

```python
import functools

import jax
import jax.numpy as jnp
from jax import lax
from jax.experimental import pallas as pl
from jax.experimental.pallas import tpu as pltpu
from jax.sharding import PartitionSpec as P

ITERS = 5
EPSILON = 1e-06
DIAGONAL = 6.0
SUBLANES = 8
MESH = pl.DeviceIdType.MESH
AXES = ("slab", "py", "pz")
UNROLLED = 64
CENTER = 8.25
LEAST_SQUARE, MOST_SQUARE = 0.25, 40.0
LEAST_SHIFT, MOST_SHIFT = 0.5, 16.5
VECTOR, POTENTIAL = 0, 1
RELAY_RING, RELAYED = 4, 5
CHUNK = 3


def times(coeff, columns):
    total = {}
    for k, c in coeff.items():
        for q, value in columns[k].items():
            term = c * value
            total[q] = total[q] + term if q in total else term
    return total


def dot(left, right):
    total = None
    for q, value in left.items():
        if q in right:
            term = value * right[q]
            total = term if total is None else total + term
    return 0.0 if total is None else total


def advance(steps, inner, shifts, taus, removed, betas):
    vectors = [{0: 1.0}]
    image_of = []
    for i in range(steps):
        column = {i + 1: 1.0, i: shifts[i]}
        if taus[i] is not None:
            column[i - 1] = taus[i]
        image_of.append(column)
    gram, lowered = {}, []
    for n in range(steps):
        for k in range(len(lowered), n + 1):
            lowered.append({
                q: dot(vectors[k], {b: inner[q, b] for b in vectors[k]})
                for q in range(n + 1)})
            for l in range(k + 1):
                gram[k, l] = gram[l, k] = dot(vectors[l], lowered[k])
        known = {n: shifts[n]}
        if n > 0:
            known[n - 1] = betas[n - 1]
            rest = times(vectors[n], image_of)
            for k, y in known.items():
                for q, value in vectors[k].items():
                    rest[q] = rest[q] - y * value if q in rest else -y * value
        else:
            rest = {n + 1: 1.0}
        rest_lowered = {
            q: dot(rest, {b: inner[q, b] for b in rest}) for q in range(n + 2)}
        along = {k: dot(vectors[k], rest_lowered) for k in range(n + 1)}
        first = {
            k: along[k] + dot(known, {l: gram[k, l] for l in known}) for k in range(n + 1)}
        excess = {k: first[k] - known[k] if k in known else first[k] for k in range(n + 1)}
        coeffs = {
            k: along[k] - dot(excess, {
                l: gram[k, l] - 1.0 if k == l else gram[k, l] for l in range(n + 1)})
            for k in range(n + 1)}
        square = dot(rest, rest_lowered)
        for k in range(n + 1):
            back = dot(coeffs, {l: gram[k, l] for l in range(n + 1)})
            square = square + coeffs[k] * (back - 2.0 * along[k])
        beta = jnp.sqrt(jnp.maximum(square, 0.0) + EPSILON)
        inverse = 1.0 / beta
        image = dict(rest)
        for k in range(n + 1):
            for q, value in vectors[k].items():
                term = coeffs[k] * value
                image[q] = image[q] - term if q in image else -term
        vectors.append({q: value * inverse for q, value in image.items()})
        removed.append({k: coeffs[k] + known[k] if k in known else coeffs[k] for k in coeffs})
        betas.append(beta)
    return vectors[1:]


def kernel(sizes, per_cell, x_hbm, pot_hbm, out_ref, coeff_ref, tri_ref, cells, ext, swapped, relayed, slots,
           group_send, plane_recv, corner_recv, relay_recv, relay_send, pass_send, side_sems, pair_sems, stat_sems):
    Z, Y, X = x_hbm.shape
    S, A, B = sizes
    n = S * A * B
    H = Z // 2
    D = ITERS
    T = SUBLANES
    ZE, YE = H + 2 * D, Y + 2 * T
    slab, py, pz = (lax.axis_index(name) for name in AXES)
    me = (slab * A + py) * B + pz
    partner = (1 - slab, py, pz)
    first_plane = D - slab * H
    inside = pl.ds(T, Y)

    def to_others(act):
        if n <= UNROLLED:
            slabs = [lax.rem(slab + i, S) for i in range(S)]
            pys = [lax.rem(py + i, A) for i in range(A)]
            pzs = [lax.rem(pz + i, B) for i in range(B)]
            far = sorted(
                ((i, j, k) for i in range(S) for j in range(A) for k in range(B)),
                key=lambda t: -(min(t[1], A - t[1]) + min(t[2], B - t[2])),
            )
            for i, j, k in far:
                if i or j or k:
                    act((slabs[i], pys[j], pzs[k]))
        else:
            def step(d, carry):
                t = lax.rem(me + d, n)
                act((t // (A * B), lax.rem(t // B, A), lax.rem(t, B)))
                return carry
            lax.fori_loop(1, n, step, 0)

    def source(array):
        return cells.at[0] if array == VECTOR else ext

    def remote(src, dst, sent, received, target):
        return pltpu.make_async_remote_copy(
            src_ref=src, dst_ref=dst, send_sem=sent, recv_sem=received,
            device_id=target, device_id_type=MESH)

    def reach(array):
        return D if array == VECTOR else D - 1

    def within(step, position, size):
        if step == 0:
            return None
        return position + step >= 0 if step < 0 else position + step < size

    def guarded(conditions, act):
        conditions = [c for c in conditions if c is not None]
        if not conditions:
            act()
        else:
            pl.when(functools.reduce(jnp.logical_and, conditions))(act)

    def plane_of(t, side, d):
        return block_of(t, side, d, Z)

    def lands(side, d):
        return D - d if side == 0 else D + H - 1 + d

    def rows(step, count, sending):
        if step == 0:
            return inside
        if step < 0:
            return pl.ds(T + Y - count, count) if sending else pl.ds(T - count, count)
        return pl.ds(T, count) if sending else pl.ds(T + Y, count)

    def arrival(array, t, side, d, step):
        w = d if array == VECTOR else d + 1
        if side != t:
            w = w + H - Z + (D if step == 0 else D - 1)
        return (plane_recv if step == 0 else corner_recv).at[w - 1]

    def plane_copy(array, t, side, d, step, sent):
        q, z = plane_of(t, side, d)
        count = reach(array) - d
        ref = source(array)
        return remote(
            ref.at[slab, z + first_plane, rows(step, count, True)],
            ref.at[slab, lands(side, d), rows(step, count, False)],
            sent, arrival(array, t, side, d, step), (t, py - step, pz - q))

    def wait_for(span, sem):
        pltpu.make_async_copy(span, span, sem).wait()

    def lines(count):
        if count % Y:
            return cells.at[0, 0, 0, pl.ds(0, count)]
        a, b, c = next((a, b, count // Y // (a * b)) for a in range(1, D + 2) for b in (1, 2)
                       if count // Y % (a * b) == 0 and count // Y // (a * b) <= ZE)
        return cells.at[pl.ds(0, a), pl.ds(0, b), pl.ds(0, c), pl.ds(0, Y)]

    below, above = py > 0, py < A - 1
    beside_both, beside_one = jnp.logical_and(below, above), below != above

    order = [(a, d) for w in range(1, D + 1) for a, d in ((VECTOR, w), (POTENTIAL, w - 1)) if d]
    relays = order[-RELAYED:] if relaying(Z, B) else []

    def relay_copy(k, t):
        array, d = relays[k]
        z = plane_of(t, t, d)[1]
        return remote(source(array).at[slab, z + first_plane, inside], relayed.at[k],
                      relay_send.at[0], relay_recv.at[2 * k // RELAYED], (slab, py, B - 1 if t == 0 else 0))

    def onward_copy(k, t):
        array, d = relays[k]
        return remote(relayed.at[k], source(array).at[slab, lands(t, d), inside], relay_send.at[0],
                      arrival(array, t, t, d, 0), (t, py, B - 2 if t == 0 else 1))

    def each_relay(at, act):
        for t in range(2):
            if relays:
                @pl.when(pz == at[t])
                def _(t=t):
                    for k in range(len(relays)):
                        act(k, t)

    def batches(w, sending):
        found = []
        for t in range(2):
            for side in range(2):
                wanted = [(array, d) for array, d in ((VECTOR, w), (POTENTIAL, w - 1))
                          if 1 <= d <= reach(array) and plane_of(t, side, d)[0] != 0]
                if passing(Z) and side != t:
                    continue
                for q in sorted({plane_of(t, side, d)[0] for _, d in wanted}, key=abs):
                    mine = [(a, d) for a, d in wanted if plane_of(t, side, d)[0] == q]
                    sign = -1 if sending else 1
                    there = [None if sending else slab == t, within(sign * q, pz, B)]
                    for turned in (False, True):
                        keys = [(a, t, side, d, 0) for a, d in mine
                                if (sending and t == side and (a, d) in relays) == turned]
                        found.append(((q, 0, turned), there + [pz != 1 + t if turned else None], keys))
                    low, high = ([(a, t, side, d, step) for a, d in mine if reach(a) > d] for step in (-1, 1))
                    if sending:
                        found.append(((q, -1, False), there + [above], low))
                        found.append(((q, 1, False), there + [below], high))
                    else:
                        found.append(((q, 1, False), there + [beside_both], low + high))
                        found.append(((q, 1, False), there + [beside_one], low))
        return [batch for batch in found if batch[2]]

    def volume(keys):
        return sum(Y if step == 0 else reach(array) - d for array, _, _, d, step in keys)

    totals = {}
    for w in range(1, D + 1):
        for tag, conditions, keys in batches(w, True):
            totals[tag] = (conditions, totals.get(tag, (0, 0))[1] + volume(keys))
    slot_of = {tag: i for i, tag in enumerate(dict.fromkeys((q, step and 1, turned) for q, step, turned in totals))}
    assert len(slot_of) == group_count(Z, B)

    def group(tag):
        q, step, turned = tag
        return group_send.at[slot_of[q, step and 1, turned]]

    def send_planes(w):
        for tag, conditions, keys in batches(w, True):
            def start(tag=tag, keys=keys):
                for key in keys:
                    plane_copy(*key, group(tag)).start()
            guarded(conditions, start)

    def finish_planes():
        for tag, (conditions, size) in totals.items():
            q, step, _ = tag
            if step == 0:
                guarded(conditions, lambda tag=tag, size=size: wait_for(lines(size), group(tag)))
            elif step > 0:
                for times_, beside in ((2, beside_both), (1, beside_one)):
                    guarded([within(-q, pz, B), beside], lambda tag=tag, rows_=times_ * size: wait_for(
                        lines(rows_), group(tag)))

    def take_planes(w):
        for tag, conditions, keys in batches(w, False):
            array, t, side, d, step = keys[0]
            guarded(conditions, lambda keys=keys, sem=arrival(array, t, side, d, step): wait_for(
                lines(2 * volume(keys)), sem))

    def pass_copy(t):
        return remote(
            cells.at[0, pl.ds(0, 2), lands(t, 1), inside], cells.at[0, pl.ds(0, 2), lands(t, D), inside],
            pass_send.at[0], plane_recv.at[D], partner)

    def each_pass(receiving, act):
        for t in range(2):
            if passing(Z):
                guarded([slab == (1 - t if receiving else t), within(-1 if t == 0 else 1, pz, B)],
                        lambda t=t: act(t))

    def side_copy(array, t, step):
        ref = source(array)
        count = reach(array)
        return remote(
            ref.at[slab, pl.ds(first_plane, Z), rows(step, count, True)],
            ref.at[slab, pl.ds(D - t * H, Z), rows(step, count, False)],
            side_sems.at[0], side_sems.at[1], (t, py - step, pz))

    def send_sides():
        for step in (-1, 1):
            def both(step=step):
                for array in (VECTOR, POTENTIAL):
                    for other in range(2):
                        side_copy(array, other, step).start()
            guarded([within(-step, py, A)], both)

    def wait_sides(sem):
        count = 2 * (reach(VECTOR) + reach(POTENTIAL))
        for times_, beside in ((2, beside_both), (1, beside_one)):
            guarded([beside], lambda times_=times_: wait_for(
                cells.at[0, 0, pl.ds(0, Z), pl.ds(0, times_ * count)], sem))

    def near_copy(array):
        ref = source(array)
        return remote(
            ref.at[slab, pl.ds(first_plane, Z), inside],
            ref.at[slab, pl.ds(D - (1 - slab) * H, Z), inside],
            pair_sems.at[0], pair_sems.at[1], partner)

    def swap_copy(level):
        return remote(
            cells.at[level, 1 - slab, pl.ds(D, H), inside], swapped.at[level - 1],
            pair_sems.at[0], pair_sems.at[2], partner)

    def stat_copy(p, target):
        return remote(slots.at[p, me], slots.at[p, me], stat_sems.at[2], stat_sems.at[p], target)

    def fold(value):
        return jnp.sum(value.reshape(value.shape[0] // T, T, X), axis=0)

    def packed(sums, first=0):
        lines_ = [jnp.sum(v, axis=0, keepdims=True) for v in sums]
        height = -(-len(lines_) // T) * T
        lines_ = lines_ + [jnp.zeros((1, X), jnp.float32)] * (height - len(lines_))
        totals = jnp.sum(jnp.concatenate(lines_, axis=0), axis=1, keepdims=True)
        at = lax.broadcasted_iota(jnp.int32, (height, X), 0) + first
        lanes = lax.broadcasted_iota(jnp.int32, (height, X), 1)
        return jnp.sum(jnp.where(at == lanes, totals, 0.0), axis=0, keepdims=True)

    def gathered(p, count):
        wait_for(slots.at[p, pl.ds(0, n - 1)], stat_sems.at[p])
        total = jnp.sum(slots[p], axis=0) * per_cell
        return [jnp.broadcast_to(total[:, s:s + 1], (1, X)) for s in range(count)]

    barrier = pltpu.get_barrier_semaphore()
    to_others(lambda t: pl.semaphore_signal(barrier, inc=1, device_id=t, device_id_type=MESH))
    loads = [pltpu.make_async_copy(
        hbm, source(array).at[slab, pl.ds(first_plane, Z), inside], pair_sems.at[0])
        for array, hbm in ((VECTOR, x_hbm), (POTENTIAL, pot_hbm))]
    for load in loads:
        load.start()

    plane = pz * Z + slab * H - D
    present = [jnp.logical_and(plane + e >= 0, plane + e < B * Z) for e in range(ZE)]
    for e in range(ZE):
        if D <= e < D + H:
            continue
        @pl.when(jnp.logical_not(present[e]))
        def _(e=e):
            for ref in (cells.at[0], ext):
                for core in range(2):
                    ref[core, e] = jnp.zeros((YE, X), jnp.float32)
    for missing, at in ((py == 0, 0), (py == A - 1, T + Y)):
        @pl.when(missing)
        def _(at=at):
            for ref in (cells.at[0], ext):
                for core in range(2):
                    for e in range(ZE):
                        ref[core, e, at:at + T] = jnp.zeros((T, X), jnp.float32)
    wait_for(lines(2 * Z * Y), pair_sems.at[0])

    def rough():
        lane = lax.broadcasted_iota(jnp.int32, (Y, X), 1)
        row = lax.broadcasted_iota(jnp.int32, (Y, X), 0)

        def apply(own, z):
            here = own(z)
            total = (jnp.where(row == 0, 0.0, pltpu.roll(here, 1, 0))
                     + jnp.where(row == Y - 1, 0.0, pltpu.roll(here, Y - 1, 0))
                     + jnp.where(lane == 0, 0.0, pltpu.roll(here, 1, 1))
                     + jnp.where(lane == X - 1, 0.0, pltpu.roll(here, X - 1, 1)))
            for beside in (z - 1, z + 1):
                if 0 <= beside < Z:
                    total = total + own(beside)
            return ext[slab, first_plane + z, inside] * here - total

        start = lambda z: cells[0, slab, first_plane + z, inside]
        once = lambda z: out_ref[0, z]
        sums = [jnp.zeros((T, X), jnp.float32)] * 5
        for z in range(Z):
            out_ref[0, z] = apply(start, z)
        for z in range(Z):
            zero, one, two = start(z), once(z), apply(once, z)
            for i, (u, v) in enumerate(((zero, zero), (zero, one), (one, one), (one, two), (two, two))):
                sums[i] = sums[i] + fold(u * v)
        return sums

    slots[0, me] = packed(rough())
    pl.semaphore_wait(barrier, n - 1)

    each_relay((1, 2), lambda k, t: relay_copy(k, t).start())
    send_planes(1)
    to_others(lambda target: stat_copy(0, target).start())
    for array in (VECTOR, POTENTIAL):
        near_copy(array).start()
    send_sides()
    for w in range(2, D + 1):
        send_planes(w)

    def forward(k, t):
        part = [i for i in range(RELAYED) if 2 * i // RELAYED == 2 * k // RELAYED]
        if k == part[0]:
            wait_for(relayed.at[pl.ds(k, len(part))], relay_recv.at[2 * k // RELAYED])
        onward_copy(k, t).start()

    each_relay((B - 1, 0), forward)

    first_lane = lax.broadcasted_iota(jnp.int32, (T, X), 1) == 0
    last_lane = lax.broadcasted_iota(jnp.int32, (T, X), 1) == X - 1
    line = lax.broadcasted_iota(jnp.int32, (T, X), 0)
    low_rows = jnp.where(jnp.logical_and(line < D - 1, py == 0), 0.0, 1.0)
    high_rows = jnp.where(jnp.logical_and(line > T - D, py == A - 1), 0.0, 1.0)

    def windows(l):
        reach = D - 1 if l < D else 0
        count = (Y + 2 * reach) // T
        starts = [T - reach + T * i for i in range(count)]
        return [(starts[i], min(CHUNK, count - i), i) for i in range(0, count, CHUNK)], count

    def depth(e):
        return max(D - e, e - (D + H - 1))

    def outer(e):
        return [b for b in (e - 1, e + 1) if depth(b) > depth(e)]

    def tiled(mask, tiles):
        return jnp.concatenate([mask] * tiles, axis=0) if tiles > 1 else mask

    def prepare(l, e):
        for start, tiles, _ in windows(l)[0]:
            at = lambda shift=0: pl.ds(start + shift, tiles * T)
            left, right = cells[l - 1, 0, e, at()], cells[l - 1, 1, e, at()]
            up = [pltpu.roll(v, 1, 1) for v in (left, right)]
            down = [pltpu.roll(v, X - 1, 1) for v in (left, right)]
            head, tail = tiled(first_lane, tiles), tiled(last_lane, tiles)
            along = (jnp.where(head, 0.0, up[0]) + jnp.where(tail, down[1], down[0]),
                     jnp.where(head, up[0], up[1]) + jnp.where(tail, 0.0, down[1]))
            for core, here in enumerate((left, right)):
                around = (cells[l - 1, core, e, at(-1)] + cells[l - 1, core, e, at(1)]) + along[core]
                for b in (e - 1, e + 1):
                    if b not in outer(e):
                        around = around + cells[l - 1, core, b, at()]
                if l == 1:
                    image = -around
                else:
                    image = ((DIAGONAL - shifts[l - 1]) + ext[core, e, at()]) * here - around
                    image = image - taus[l - 1] * cells[l - 2, core, e, at()]
                cells[l, core, e, at()] = image

    def finish(l, e):
        chunks, count = windows(l)
        for core in range(2):
            for start, tiles, first in chunks:
                at = pl.ds(start, tiles * T)
                image = cells[l, core, e, at]
                for b in outer(e):
                    image = image - cells[l - 1, core, b, at]
                if l == 1:
                    image = ((DIAGONAL - shifts[0]) + ext[core, e, at]) * cells[0, core, e, at] + image
                if not D <= e < D + H:
                    image = image * present[e].astype(jnp.float32)
                for i in range(tiles):
                    part = image[i * T:(i + 1) * T]
                    if l < D and first + i == 0:
                        part = part * low_rows
                    if l < D and first + i == count - 1:
                        part = part * high_rows
                    cells[l, core, e, pl.ds(start + i * T, T)] = part

    def wave(w):
        return [(l, e) for l in range(1, D + 1) for e in range(l, ZE - l) if max(l + depth(e), 0) == w]

    def measure(pairs, at, sums=None):
        sums = sums or [jnp.zeros((T, X), jnp.float32)] * len(pairs)
        for core in range(2):
            for e in at:
                held = {k: cells[k, core, e, inside] for k in sorted({k for pair in pairs for k in pair})}
                for i, (k, l) in enumerate(pairs):
                    sums[i] = sums[i] + fold(held[k] * held[l])
        return sums

    wait_for(lines(2 * Z * Y), pair_sems.at[1])
    wait_sides(side_sems.at[1])
    ready = []
    for reached in range(2):
        if reached:
            take_planes(reached)
            each_pass(False, lambda t: pass_copy(t).start())
        for e in range(1, ZE - 1):
            if depth(e) <= reached and e not in ready:
                prepare(1, e)
                ready.append(e)

    m0, m1, m2, m3, m4 = gathered(0, 5)
    some = m0 > 1e-30
    over = 1.0 / jnp.where(some, m0, 1.0)
    m1, m2, m3, m4 = m1 * over, m2 * over, m3 * over, m4 * over
    c2 = m2 - m1 * m1
    c3 = m3 - 3.0 * m1 * m2 + 2.0 * m1 * m1 * m1
    c4 = m4 - 4.0 * m1 * m3 + 6.0 * m1 * m1 * m2 - 3.0 * m1 * m1 * m1 * m1
    down = 1.0 / jnp.maximum(c2, 1e-3)
    slope = c3 * down
    bound = lambda value, low, high: jnp.minimum(jnp.maximum(value, low), high)
    alpha = [bound(jnp.where(some, DIAGONAL + a, CENTER), LEAST_SHIFT, MOST_SHIFT) for a in (m1, m1 + slope)]
    square = [bound(b, LEAST_SQUARE, MOST_SQUARE) for b in (c2, c4 * down - c2 - slope * slope)]
    shifts = [alpha[0]] + [alpha[1]] * (D - 1)
    taus = [None, square[0]] + [square[1]] * (D - 2)

    early = [(k, l) for l in range(D) for k in range(l + 1)]
    late = [(k, D) for k in range(D + 1)]
    held = range(D, D + H)
    done = [e for e in held if depth(e) < 0]
    def prepare_all(entries):
        for l, e in entries:
            if l > 1 or e not in ready:
                prepare(l, e)

    for entry in wave(0):
        prepare_all([entry])
        finish(*entry)
    prepare_all(wave(1))
    for w in range(1, D + 1):
        if w > 1:
            take_planes(w)
        if w == D:
            each_pass(True, lambda t: pass_copy(t).wait_recv())
        for l, e in wave(w):
            finish(l, e)
        swap_copy(w).start()
        if w == D - 1:
            slots[1, me] = packed(measure(early, held))
            last = measure(late, done)
        if w < D:
            prepare_all(wave(w + 1))
    slots[1, me] = slots[1, me] + packed(measure(late, [e for e in held if e not in done], last), len(early))
    to_others(lambda target: stat_copy(1, target).start())
    wait_for(lines((2 * Z + D * H) * Y), pair_sems.at[0])
    wait_sides(side_sems.at[0])
    if relays:
        wait_for(relayed, relay_send.at[0])
    finish_planes()
    each_pass(False, lambda t: pass_copy(t).wait_send())
    wait_for(swapped, pair_sems.at[2])
    for i in range(H):
        mine, other = slab * H + i, (1 - slab) * H + i
        out_ref[0, mine] = cells[0, slab, D + i, inside]
        out_ref[0, other] = cells[0, slab, first_plane + other, inside]
        for q in range(1, D + 1):
            out_ref[q, mine] = cells[q, slab, D + i, inside]
            out_ref[q, other] = swapped[q - 1, i]
    stats = gathered(1, len(early) + len(late))
    scale = 1.0 / jnp.sqrt(stats[0] + EPSILON)
    inner = {}
    for (k, l), value in zip(early + late, stats):
        inner[k, l] = inner[l, k] = value * scale * scale
    removed, betas = [], []
    found = advance(D, inner, shifts, taus, removed, betas)
    for v in range(D):
        tri_ref[0:1, v:v + 1] = removed[v][v][:, 0:1]
        tri_ref[1:2, v:v + 1] = betas[v][:, 0:1]
    found = [{q: t * scale for q, t in coords.items()} for coords in found]

    for r, value in enumerate([scale] + [coords[q] for coords in found for q in range(len(coords))]):
        coeff_ref[r:r + 1] = value

    wait_for(slots.at[pl.ds(0, 2), pl.ds(0, n - 1)], stat_sems.at[2])


def block_of(t, side, d, Z):
    z = t * (Z // 2) - d if side == 0 else (t + 1) * (Z // 2) - 1 + d
    return z // Z, z % Z


def relaying(Z, B):
    return B == RELAY_RING and block_of(0, 0, ITERS, Z)[0] == -1


def passing(Z):
    return Z - Z // 2 + 1 == ITERS


def group_count(Z, B):
    blocks = [[block_of(t, side, d, Z)[0] for d in range(1, ITERS + 1)] for t in range(2) for side in range(2)
              if side == t or not passing(Z)]
    straight = {q for row in blocks for q in row} - {0}
    beside = {q for row in blocks for q in row[:-1]} - {0}
    return len(straight) + len(beside) + (2 if relaying(Z, B) else 0)


def write_out(columns, coeff_ref, tri_ref, basis_out, tri_out, basis, sems):
    count, Z = columns.shape[:2]
    small = pltpu.make_async_copy(tri_ref, tri_out, sems.at[1])
    small.start()
    for z in range(Z):
        held = [columns[q, z] for q in range(count)]
        for k in range(count):
            total = None
            for q in reversed(range(k + 1)):
                r = 0 if k == 0 else k * (k + 1) // 2 + q
                term = coeff_ref[r:r + 1] * held[q]
                total = term if total is None else total + term
            basis[k, z] = total
        pltpu.make_async_copy(basis.at[:, z], basis_out.at[:, z], sems.at[0]).start()
    pltpu.make_async_copy(basis, basis_out, sems.at[0]).wait()
    small.wait()


def shards(sizes, start_vector, potential):
    Z, Y, X = start_vector.shape
    n = sizes[0] * sizes[1] * sizes[2]
    f32 = jnp.float32
    H, D, T = Z // 2, ITERS, SUBLANES
    assert sizes[0] == 2 and Z % 2 == 0 and H <= D and Y >= D and Y % T == 0
    vmem = pl.BlockSpec(memory_space=pltpu.VMEM)
    hbm = pl.BlockSpec(memory_space=pl.ANY)
    dma = pltpu.SemaphoreType.DMA
    extended = (2, H + 2 * D, Y + 2 * T, X)
    coeffs = -(-((D + 1) * (D + 2) // 2) // T) * T
    held = pl.pallas_call(
        functools.partial(kernel, sizes, 1.0 / (start_vector.size * n)),
        out_shape=(pltpu.VMEM((D + 1, Z, Y, X), f32), pltpu.VMEM((coeffs, X), f32), pltpu.VMEM((2, D), f32)),
        in_specs=[hbm, hbm],
        out_specs=(vmem,) * 3,
        scratch_shapes=[
            pltpu.VMEM((D + 1,) + extended, f32),
            pltpu.VMEM(extended, f32),
            pltpu.VMEM((D, H, Y, X), f32),
            pltpu.VMEM((RELAYED, Y, X), f32),
            pltpu.VMEM((2, n, 1, X), f32),
            dma((group_count(Z, sizes[2]),)),
            dma((D + max(0, D - Z + H),)),
            dma((D - 1 + max(0, D - 1 - Z + H),)),
            dma((2,)),
            dma((1,)),
            dma((1,)),
            dma((2,)),
            dma((3,)),
            dma((3,)),
        ],
        compiler_params=pltpu.CompilerParams(collective_id=0, has_side_effects=True),
    )(start_vector, potential)
    return tuple(pl.pallas_call(
        write_out,
        out_shape=(jax.ShapeDtypeStruct((D + 1, Z, Y, X), f32), jax.ShapeDtypeStruct((2, D), f32)),
        in_specs=[vmem] * 3,
        out_specs=(hbm, hbm),
        scratch_shapes=[pltpu.VMEM((D + 1, Z, Y, X), f32), dma((2,))],
    )(*(pltpu.with_memory_space_constraint(ref, pltpu.VMEM) for ref in held)))


def solution(mesh):
    sizes = tuple(mesh.shape[name] for name in AXES)
    in_specs = (P("pz", "py", "slab"), P("pz", "py", "slab"))
    out_specs = (P(None, "pz", "py", "slab"), P())
    return jax.shard_map(functools.partial(shards, sizes), mesh=mesh, in_specs=in_specs,
                         out_specs=out_specs, check_vma=False)
```

```python
import functools

import jax
import jax.numpy as jnp
from jax import lax
from jax.experimental import pallas as pl
from jax.experimental.pallas import tpu as pltpu
from jax.sharding import PartitionSpec as P

ITERS = 5
EPSILON = 1e-06
DIAGONAL = 6.0
SUBLANES = 8
MESH = pl.DeviceIdType.MESH
AXES = ("slab", "py", "pz")
UNROLLED = 64
CENTER = 8.25
LEAST_SQUARE, MOST_SQUARE = 0.25, 40.0
LEAST_SHIFT, MOST_SHIFT = 0.5, 16.5
VECTOR, POTENTIAL = 0, 1
RELAY_RING, RELAYED = 4, 5
CHUNK = 2


def times(coeff, columns):
    total = {}
    for k, c in coeff.items():
        for q, value in columns[k].items():
            term = c * value
            total[q] = total[q] + term if q in total else term
    return total


def dot(left, right):
    total = None
    for q, value in left.items():
        if q in right:
            term = value * right[q]
            total = term if total is None else total + term
    return 0.0 if total is None else total


def advance(steps, inner, shifts, taus, removed, betas):
    vectors = [{0: 1.0}]
    image_of = []
    for i in range(steps):
        column = {i + 1: 1.0, i: shifts[i]}
        if taus[i] is not None:
            column[i - 1] = taus[i]
        image_of.append(column)
    gram, lowered = {}, []
    for n in range(steps):
        for k in range(len(lowered), n + 1):
            lowered.append({
                q: dot(vectors[k], {b: inner[q, b] for b in vectors[k]})
                for q in range(n + 1)})
            for l in range(k + 1):
                gram[k, l] = gram[l, k] = dot(vectors[l], lowered[k])
        known = {n: shifts[n]}
        if n > 0:
            known[n - 1] = betas[n - 1]
            rest = times(vectors[n], image_of)
            for k, y in known.items():
                for q, value in vectors[k].items():
                    rest[q] = rest[q] - y * value if q in rest else -y * value
        else:
            rest = {n + 1: 1.0}
        rest_lowered = {
            q: dot(rest, {b: inner[q, b] for b in rest}) for q in range(n + 2)}
        along = {k: dot(vectors[k], rest_lowered) for k in range(n + 1)}
        first = {
            k: along[k] + dot(known, {l: gram[k, l] for l in known}) for k in range(n + 1)}
        excess = {k: first[k] - known[k] if k in known else first[k] for k in range(n + 1)}
        coeffs = {
            k: along[k] - dot(excess, {
                l: gram[k, l] - 1.0 if k == l else gram[k, l] for l in range(n + 1)})
            for k in range(n + 1)}
        square = dot(rest, rest_lowered)
        for k in range(n + 1):
            back = dot(coeffs, {l: gram[k, l] for l in range(n + 1)})
            square = square + coeffs[k] * (back - 2.0 * along[k])
        beta = jnp.sqrt(jnp.maximum(square, 0.0) + EPSILON)
        inverse = 1.0 / beta
        image = dict(rest)
        for k in range(n + 1):
            for q, value in vectors[k].items():
                term = coeffs[k] * value
                image[q] = image[q] - term if q in image else -term
        vectors.append({q: value * inverse for q, value in image.items()})
        removed.append({k: coeffs[k] + known[k] if k in known else coeffs[k] for k in coeffs})
        betas.append(beta)
    return vectors[1:]


def kernel(sizes, per_cell, x_hbm, pot_hbm, out_ref, coeff_ref, tri_ref, cells, ext, swapped, relayed, slots,
           group_send, plane_recv, corner_recv, relay_recv, relay_send, pass_send, side_sems, pair_sems, stat_sems):
    Z, Y, X = x_hbm.shape
    S, A, B = sizes
    n = S * A * B
    H = Z // 2
    D = ITERS
    T = SUBLANES
    ZE, YE = H + 2 * D, Y + 2 * T
    slab, py, pz = (lax.axis_index(name) for name in AXES)
    me = (slab * A + py) * B + pz
    partner = (1 - slab, py, pz)
    first_plane = D - slab * H
    inside = pl.ds(T, Y)

    def to_others(act):
        if n <= UNROLLED:
            slabs = [lax.rem(slab + i, S) for i in range(S)]
            pys = [lax.rem(py + i, A) for i in range(A)]
            pzs = [lax.rem(pz + i, B) for i in range(B)]
            far = sorted(
                ((i, j, k) for i in range(S) for j in range(A) for k in range(B)),
                key=lambda t: -(min(t[1], A - t[1]) + min(t[2], B - t[2])),
            )
            for i, j, k in far:
                if i or j or k:
                    act((slabs[i], pys[j], pzs[k]))
        else:
            def step(d, carry):
                t = lax.rem(me + d, n)
                act((t // (A * B), lax.rem(t // B, A), lax.rem(t, B)))
                return carry
            lax.fori_loop(1, n, step, 0)

    def source(array):
        return cells.at[0] if array == VECTOR else ext

    def remote(src, dst, sent, received, target):
        return pltpu.make_async_remote_copy(
            src_ref=src, dst_ref=dst, send_sem=sent, recv_sem=received,
            device_id=target, device_id_type=MESH)

    def reach(array):
        return D if array == VECTOR else D - 1

    def within(step, position, size):
        if step == 0:
            return None
        return position + step >= 0 if step < 0 else position + step < size

    def guarded(conditions, act):
        conditions = [c for c in conditions if c is not None]
        if not conditions:
            act()
        else:
            pl.when(functools.reduce(jnp.logical_and, conditions))(act)

    def plane_of(t, side, d):
        return block_of(t, side, d, Z)

    def lands(side, d):
        return D - d if side == 0 else D + H - 1 + d

    def rows(step, count, sending):
        if step == 0:
            return inside
        if step < 0:
            return pl.ds(T + Y - count, count) if sending else pl.ds(T - count, count)
        return pl.ds(T, count) if sending else pl.ds(T + Y, count)

    def arrival(array, t, side, d, step):
        w = d if array == VECTOR else d + 1
        if side != t:
            w = w + H - Z + (D if step == 0 else D - 1)
        return (plane_recv if step == 0 else corner_recv).at[w - 1]

    def plane_copy(array, t, side, d, step, sent):
        q, z = plane_of(t, side, d)
        count = reach(array) - d
        ref = source(array)
        return remote(
            ref.at[slab, z + first_plane, rows(step, count, True)],
            ref.at[slab, lands(side, d), rows(step, count, False)],
            sent, arrival(array, t, side, d, step), (t, py - step, pz - q))

    def wait_for(span, sem):
        pltpu.make_async_copy(span, span, sem).wait()

    def lines(count):
        if count % Y:
            return cells.at[0, 0, 0, pl.ds(0, count)]
        a, b, c = next((a, b, count // Y // (a * b)) for a in range(1, D + 2) for b in (1, 2)
                       if count // Y % (a * b) == 0 and count // Y // (a * b) <= ZE)
        return cells.at[pl.ds(0, a), pl.ds(0, b), pl.ds(0, c), pl.ds(0, Y)]

    below, above = py > 0, py < A - 1
    beside_both, beside_one = jnp.logical_and(below, above), below != above

    order = [(a, d) for w in range(1, D + 1) for a, d in ((VECTOR, w), (POTENTIAL, w - 1)) if d]
    relays = order[-RELAYED:] if relaying(Z, B) else []

    def relay_copy(k, t):
        array, d = relays[k]
        z = plane_of(t, t, d)[1]
        return remote(source(array).at[slab, z + first_plane, inside], relayed.at[k],
                      relay_send.at[0], relay_recv.at[2 * k // RELAYED], (slab, py, B - 1 if t == 0 else 0))

    def onward_copy(k, t):
        array, d = relays[k]
        return remote(relayed.at[k], source(array).at[slab, lands(t, d), inside], relay_send.at[0],
                      arrival(array, t, t, d, 0), (t, py, B - 2 if t == 0 else 1))

    def each_relay(at, act):
        for t in range(2):
            if relays:
                @pl.when(pz == at[t])
                def _(t=t):
                    for k in range(len(relays)):
                        act(k, t)

    def batches(w, sending):
        found = []
        for t in range(2):
            for side in range(2):
                wanted = [(array, d) for array, d in ((VECTOR, w), (POTENTIAL, w - 1))
                          if 1 <= d <= reach(array) and plane_of(t, side, d)[0] != 0]
                if passing(Z) and side != t:
                    continue
                for q in sorted({plane_of(t, side, d)[0] for _, d in wanted}, key=abs):
                    mine = [(a, d) for a, d in wanted if plane_of(t, side, d)[0] == q]
                    sign = -1 if sending else 1
                    there = [None if sending else slab == t, within(sign * q, pz, B)]
                    for turned in (False, True):
                        keys = [(a, t, side, d, 0) for a, d in mine
                                if (sending and t == side and (a, d) in relays) == turned]
                        found.append(((q, 0, turned), there + [pz != 1 + t if turned else None], keys))
                    low, high = ([(a, t, side, d, step) for a, d in mine if reach(a) > d] for step in (-1, 1))
                    if sending:
                        found.append(((q, -1, False), there + [above], low))
                        found.append(((q, 1, False), there + [below], high))
                    else:
                        found.append(((q, 1, False), there + [beside_both], low + high))
                        found.append(((q, 1, False), there + [beside_one], low))
        return [batch for batch in found if batch[2]]

    def volume(keys):
        return sum(Y if step == 0 else reach(array) - d for array, _, _, d, step in keys)

    totals = {}
    for w in range(1, D + 1):
        for tag, conditions, keys in batches(w, True):
            totals[tag] = (conditions, totals.get(tag, (0, 0))[1] + volume(keys))
    slot_of = {tag: i for i, tag in enumerate(dict.fromkeys((q, step and 1, turned) for q, step, turned in totals))}
    assert len(slot_of) == group_count(Z, B)

    def group(tag):
        q, step, turned = tag
        return group_send.at[slot_of[q, step and 1, turned]]

    def send_planes(w):
        for tag, conditions, keys in batches(w, True):
            def start(tag=tag, keys=keys):
                for key in keys:
                    plane_copy(*key, group(tag)).start()
            guarded(conditions, start)

    def finish_planes():
        for tag, (conditions, size) in totals.items():
            q, step, _ = tag
            if step == 0:
                guarded(conditions, lambda tag=tag, size=size: wait_for(lines(size), group(tag)))
            elif step > 0:
                for times_, beside in ((2, beside_both), (1, beside_one)):
                    guarded([within(-q, pz, B), beside], lambda tag=tag, rows_=times_ * size: wait_for(
                        lines(rows_), group(tag)))

    def take_planes(w):
        for tag, conditions, keys in batches(w, False):
            array, t, side, d, step = keys[0]
            guarded(conditions, lambda keys=keys, sem=arrival(array, t, side, d, step): wait_for(
                lines(2 * volume(keys)), sem))

    def pass_copy(t):
        return remote(
            cells.at[0, pl.ds(0, 2), lands(t, 1), inside], cells.at[0, pl.ds(0, 2), lands(t, D), inside],
            pass_send.at[0], plane_recv.at[D], partner)

    def each_pass(receiving, act):
        for t in range(2):
            if passing(Z):
                guarded([slab == (1 - t if receiving else t), within(-1 if t == 0 else 1, pz, B)],
                        lambda t=t: act(t))

    def side_copy(array, t, step):
        ref = source(array)
        count = reach(array)
        return remote(
            ref.at[slab, pl.ds(first_plane, Z), rows(step, count, True)],
            ref.at[slab, pl.ds(D - t * H, Z), rows(step, count, False)],
            side_sems.at[0], side_sems.at[1], (t, py - step, pz))

    def send_sides():
        for step in (-1, 1):
            def both(step=step):
                for array in (VECTOR, POTENTIAL):
                    for other in range(2):
                        side_copy(array, other, step).start()
            guarded([within(-step, py, A)], both)

    def wait_sides(sem):
        count = 2 * (reach(VECTOR) + reach(POTENTIAL))
        for times_, beside in ((2, beside_both), (1, beside_one)):
            guarded([beside], lambda times_=times_: wait_for(
                cells.at[0, 0, pl.ds(0, Z), pl.ds(0, times_ * count)], sem))

    def near_copy(array):
        ref = source(array)
        return remote(
            ref.at[slab, pl.ds(first_plane, Z), inside],
            ref.at[slab, pl.ds(D - (1 - slab) * H, Z), inside],
            pair_sems.at[0], pair_sems.at[1], partner)

    def swap_copy(level):
        return remote(
            cells.at[level, 1 - slab, pl.ds(D, H), inside], swapped.at[level - 1],
            pair_sems.at[0], pair_sems.at[2], partner)

    def stat_copy(p, target):
        return remote(slots.at[p, me], slots.at[p, me], stat_sems.at[2], stat_sems.at[p], target)

    def fold(value):
        return jnp.sum(value.reshape(value.shape[0] // T, T, X), axis=0)

    def packed(sums, first=0):
        lines_ = [jnp.sum(v, axis=0, keepdims=True) for v in sums]
        height = -(-len(lines_) // T) * T
        lines_ = lines_ + [jnp.zeros((1, X), jnp.float32)] * (height - len(lines_))
        totals = jnp.sum(jnp.concatenate(lines_, axis=0), axis=1, keepdims=True)
        at = lax.broadcasted_iota(jnp.int32, (height, X), 0) + first
        lanes = lax.broadcasted_iota(jnp.int32, (height, X), 1)
        return jnp.sum(jnp.where(at == lanes, totals, 0.0), axis=0, keepdims=True)

    def gathered(p, count):
        wait_for(slots.at[p, pl.ds(0, n - 1)], stat_sems.at[p])
        total = jnp.sum(slots[p], axis=0) * per_cell
        return [jnp.broadcast_to(total[:, s:s + 1], (1, X)) for s in range(count)]

    barrier = pltpu.get_barrier_semaphore()
    to_others(lambda t: pl.semaphore_signal(barrier, inc=1, device_id=t, device_id_type=MESH))
    loads = [pltpu.make_async_copy(
        hbm, source(array).at[slab, pl.ds(first_plane, Z), inside], pair_sems.at[0])
        for array, hbm in ((VECTOR, x_hbm), (POTENTIAL, pot_hbm))]
    for load in loads:
        load.start()

    plane = pz * Z + slab * H - D
    present = [jnp.logical_and(plane + e >= 0, plane + e < B * Z) for e in range(ZE)]
    for e in range(ZE):
        if D <= e < D + H:
            continue
        @pl.when(jnp.logical_not(present[e]))
        def _(e=e):
            for ref in (cells.at[0], ext):
                for core in range(2):
                    ref[core, e] = jnp.zeros((YE, X), jnp.float32)
    for missing, at in ((py == 0, 0), (py == A - 1, T + Y)):
        @pl.when(missing)
        def _(at=at):
            for ref in (cells.at[0], ext):
                for core in range(2):
                    for e in range(ZE):
                        ref[core, e, at:at + T] = jnp.zeros((T, X), jnp.float32)
    wait_for(lines(2 * Z * Y), pair_sems.at[0])

    def rough():
        lane = lax.broadcasted_iota(jnp.int32, (Y, X), 1)
        row = lax.broadcasted_iota(jnp.int32, (Y, X), 0)

        def apply(own, z):
            here = own(z)
            total = (jnp.where(row == 0, 0.0, pltpu.roll(here, 1, 0))
                     + jnp.where(row == Y - 1, 0.0, pltpu.roll(here, Y - 1, 0))
                     + jnp.where(lane == 0, 0.0, pltpu.roll(here, 1, 1))
                     + jnp.where(lane == X - 1, 0.0, pltpu.roll(here, X - 1, 1)))
            for beside in (z - 1, z + 1):
                if 0 <= beside < Z:
                    total = total + own(beside)
            return ext[slab, first_plane + z, inside] * here - total

        start = lambda z: cells[0, slab, first_plane + z, inside]
        once = lambda z: out_ref[0, z]
        sums = [jnp.zeros((T, X), jnp.float32)] * 5
        for z in range(Z):
            out_ref[0, z] = apply(start, z)
        for z in range(Z):
            zero, one, two = start(z), once(z), apply(once, z)
            for i, (u, v) in enumerate(((zero, zero), (zero, one), (one, one), (one, two), (two, two))):
                sums[i] = sums[i] + fold(u * v)
        return sums

    slots[0, me] = packed(rough())
    pl.semaphore_wait(barrier, n - 1)

    to_others(lambda target: stat_copy(0, target).start())
    each_relay((1, 2), lambda k, t: relay_copy(k, t).start())
    send_planes(1)
    for array in (VECTOR, POTENTIAL):
        near_copy(array).start()
    send_sides()
    for w in range(2, D + 1):
        send_planes(w)

    def forward(k, t):
        part = [i for i in range(RELAYED) if 2 * i // RELAYED == 2 * k // RELAYED]
        if k == part[0]:
            wait_for(relayed.at[pl.ds(k, len(part))], relay_recv.at[2 * k // RELAYED])
        onward_copy(k, t).start()

    each_relay((B - 1, 0), forward)

    first_lane = lax.broadcasted_iota(jnp.int32, (T, X), 1) == 0
    last_lane = lax.broadcasted_iota(jnp.int32, (T, X), 1) == X - 1
    line = lax.broadcasted_iota(jnp.int32, (T, X), 0)
    low_rows = jnp.where(jnp.logical_and(line < D - 1, py == 0), 0.0, 1.0)
    high_rows = jnp.where(jnp.logical_and(line > T - D, py == A - 1), 0.0, 1.0)

    def windows(l):
        reach = D - 1 if l < D else 0
        count = (Y + 2 * reach) // T
        starts = [T - reach + T * i for i in range(count)]
        return [(starts[i], min(CHUNK, count - i), i) for i in range(0, count, CHUNK)], count

    def depth(e):
        return max(D - e, e - (D + H - 1))

    def outer(e):
        return [b for b in (e - 1, e + 1) if depth(b) > depth(e)]

    def tiled(mask, tiles):
        return jnp.concatenate([mask] * tiles, axis=0) if tiles > 1 else mask

    def prepare(l, e):
        for start, tiles, _ in windows(l)[0]:
            at = lambda shift=0: pl.ds(start + shift, tiles * T)
            left, right = cells[l - 1, 0, e, at()], cells[l - 1, 1, e, at()]
            up = [pltpu.roll(v, 1, 1) for v in (left, right)]
            down = [pltpu.roll(v, X - 1, 1) for v in (left, right)]
            head, tail = tiled(first_lane, tiles), tiled(last_lane, tiles)
            along = (jnp.where(head, 0.0, up[0]) + jnp.where(tail, down[1], down[0]),
                     jnp.where(head, up[0], up[1]) + jnp.where(tail, 0.0, down[1]))
            for core, here in enumerate((left, right)):
                around = (cells[l - 1, core, e, at(-1)] + cells[l - 1, core, e, at(1)]) + along[core]
                for b in (e - 1, e + 1):
                    if b not in outer(e):
                        around = around + cells[l - 1, core, b, at()]
                if l == 1:
                    image = -around
                else:
                    image = ((DIAGONAL - shifts[l - 1]) + ext[core, e, at()]) * here - around
                    image = image - taus[l - 1] * cells[l - 2, core, e, at()]
                cells[l, core, e, at()] = image

    def finish(l, e):
        chunks, count = windows(l)
        for core in range(2):
            for start, tiles, first in chunks:
                at = pl.ds(start, tiles * T)
                image = cells[l, core, e, at]
                for b in outer(e):
                    image = image - cells[l - 1, core, b, at]
                if l == 1:
                    image = ((DIAGONAL - shifts[0]) + ext[core, e, at]) * cells[0, core, e, at] + image
                if not D <= e < D + H:
                    image = image * present[e].astype(jnp.float32)
                for i in range(tiles):
                    part = image[i * T:(i + 1) * T]
                    if l < D and first + i == 0:
                        part = part * low_rows
                    if l < D and first + i == count - 1:
                        part = part * high_rows
                    cells[l, core, e, pl.ds(start + i * T, T)] = part

    def wave(w):
        return [(l, e) for l in range(1, D + 1) for e in range(l, ZE - l) if max(l + depth(e), 0) == w]

    def measure(pairs, at, sums=None):
        sums = sums or [jnp.zeros((T, X), jnp.float32)] * len(pairs)
        for core in range(2):
            for e in at:
                held = {k: cells[k, core, e, inside] for k in sorted({k for pair in pairs for k in pair})}
                for i, (k, l) in enumerate(pairs):
                    sums[i] = sums[i] + fold(held[k] * held[l])
        return sums

    wait_for(lines(2 * Z * Y), pair_sems.at[1])
    wait_sides(side_sems.at[1])
    ready = []
    for reached in range(2):
        if reached:
            take_planes(reached)
            each_pass(False, lambda t: pass_copy(t).start())
        for e in range(1, ZE - 1):
            if depth(e) <= reached and e not in ready:
                prepare(1, e)
                ready.append(e)

    m0, m1, m2, m3, m4 = gathered(0, 5)
    some = m0 > 1e-30
    over = 1.0 / jnp.where(some, m0, 1.0)
    m1, m2, m3, m4 = m1 * over, m2 * over, m3 * over, m4 * over
    c2 = m2 - m1 * m1
    c3 = m3 - 3.0 * m1 * m2 + 2.0 * m1 * m1 * m1
    c4 = m4 - 4.0 * m1 * m3 + 6.0 * m1 * m1 * m2 - 3.0 * m1 * m1 * m1 * m1
    down = 1.0 / jnp.maximum(c2, 1e-3)
    slope = c3 * down
    bound = lambda value, low, high: jnp.minimum(jnp.maximum(value, low), high)
    alpha = [bound(jnp.where(some, DIAGONAL + a, CENTER), LEAST_SHIFT, MOST_SHIFT) for a in (m1, m1 + slope)]
    square = [bound(b, LEAST_SQUARE, MOST_SQUARE) for b in (c2, c4 * down - c2 - slope * slope)]
    shifts = [alpha[0]] + [alpha[1]] * (D - 1)
    taus = [None, square[0]] + [square[1]] * (D - 2)

    early = [(k, l) for l in range(D) for k in range(l + 1)]
    late = [(k, D) for k in range(D + 1)]
    held = range(D, D + H)
    done = [e for e in held if depth(e) < 0]
    def prepare_all(entries):
        for l, e in entries:
            if l > 1 or e not in ready:
                prepare(l, e)

    for entry in wave(0):
        prepare_all([entry])
        finish(*entry)
    prepare_all(wave(1))
    for w in range(1, D + 1):
        if w > 1:
            take_planes(w)
        if w == D:
            each_pass(True, lambda t: pass_copy(t).wait_recv())
        for l, e in wave(w):
            finish(l, e)
        swap_copy(w).start()
        if w == D - 1:
            slots[1, me] = packed(measure(early, held))
            last = measure(late, done)
        if w < D:
            prepare_all(wave(w + 1))
    slots[1, me] = slots[1, me] + packed(measure(late, [e for e in held if e not in done], last), len(early))
    to_others(lambda target: stat_copy(1, target).start())
    wait_for(lines((2 * Z + D * H) * Y), pair_sems.at[0])
    wait_sides(side_sems.at[0])
    if relays:
        wait_for(relayed, relay_send.at[0])
    finish_planes()
    each_pass(False, lambda t: pass_copy(t).wait_send())
    wait_for(swapped, pair_sems.at[2])
    for i in range(H):
        mine, other = slab * H + i, (1 - slab) * H + i
        out_ref[0, mine] = cells[0, slab, D + i, inside]
        out_ref[0, other] = cells[0, slab, first_plane + other, inside]
        for q in range(1, D + 1):
            out_ref[q, mine] = cells[q, slab, D + i, inside]
            out_ref[q, other] = swapped[q - 1, i]
    stats = gathered(1, len(early) + len(late))
    scale = 1.0 / jnp.sqrt(stats[0] + EPSILON)
    inner = {}
    for (k, l), value in zip(early + late, stats):
        inner[k, l] = inner[l, k] = value * scale * scale
    removed, betas = [], []
    found = advance(D, inner, shifts, taus, removed, betas)
    for v in range(D):
        tri_ref[0:1, v:v + 1] = removed[v][v][:, 0:1]
        tri_ref[1:2, v:v + 1] = betas[v][:, 0:1]
    found = [{q: t * scale for q, t in coords.items()} for coords in found]

    for r, value in enumerate([scale] + [coords[q] for coords in found for q in range(len(coords))]):
        coeff_ref[r:r + 1] = value

    wait_for(slots.at[pl.ds(0, 2), pl.ds(0, n - 1)], stat_sems.at[2])


def block_of(t, side, d, Z):
    z = t * (Z // 2) - d if side == 0 else (t + 1) * (Z // 2) - 1 + d
    return z // Z, z % Z


def relaying(Z, B):
    return B == RELAY_RING and block_of(0, 0, ITERS, Z)[0] == -1


def passing(Z):
    return Z - Z // 2 + 1 == ITERS


def group_count(Z, B):
    blocks = [[block_of(t, side, d, Z)[0] for d in range(1, ITERS + 1)] for t in range(2) for side in range(2)
              if side == t or not passing(Z)]
    straight = {q for row in blocks for q in row} - {0}
    beside = {q for row in blocks for q in row[:-1]} - {0}
    return len(straight) + len(beside) + (2 if relaying(Z, B) else 0)


def write_out(columns, coeff_ref, tri_ref, basis_out, tri_out, basis, sems):
    count, Z = columns.shape[:2]
    small = pltpu.make_async_copy(tri_ref, tri_out, sems.at[1])
    small.start()
    for z in range(Z):
        held = [columns[q, z] for q in range(count)]
        for k in range(count):
            total = None
            for q in reversed(range(k + 1)):
                r = 0 if k == 0 else k * (k + 1) // 2 + q
                term = coeff_ref[r:r + 1] * held[q]
                total = term if total is None else total + term
            basis[k, z] = total
        pltpu.make_async_copy(basis.at[:, z], basis_out.at[:, z], sems.at[0]).start()
    pltpu.make_async_copy(basis, basis_out, sems.at[0]).wait()
    small.wait()


def shards(sizes, start_vector, potential):
    Z, Y, X = start_vector.shape
    n = sizes[0] * sizes[1] * sizes[2]
    f32 = jnp.float32
    H, D, T = Z // 2, ITERS, SUBLANES
    assert sizes[0] == 2 and Z % 2 == 0 and H <= D and Y >= D and Y % T == 0
    vmem = pl.BlockSpec(memory_space=pltpu.VMEM)
    hbm = pl.BlockSpec(memory_space=pl.ANY)
    dma = pltpu.SemaphoreType.DMA
    extended = (2, H + 2 * D, Y + 2 * T, X)
    coeffs = -(-((D + 1) * (D + 2) // 2) // T) * T
    held = pl.pallas_call(
        functools.partial(kernel, sizes, 1.0 / (start_vector.size * n)),
        out_shape=(pltpu.VMEM((D + 1, Z, Y, X), f32), pltpu.VMEM((coeffs, X), f32), pltpu.VMEM((2, D), f32)),
        in_specs=[hbm, hbm],
        out_specs=(vmem,) * 3,
        scratch_shapes=[
            pltpu.VMEM((D + 1,) + extended, f32),
            pltpu.VMEM(extended, f32),
            pltpu.VMEM((D, H, Y, X), f32),
            pltpu.VMEM((RELAYED, Y, X), f32),
            pltpu.VMEM((2, n, 1, X), f32),
            dma((group_count(Z, sizes[2]),)),
            dma((D + max(0, D - Z + H),)),
            dma((D - 1 + max(0, D - 1 - Z + H),)),
            dma((2,)),
            dma((1,)),
            dma((1,)),
            dma((2,)),
            dma((3,)),
            dma((3,)),
        ],
        compiler_params=pltpu.CompilerParams(collective_id=0, has_side_effects=True),
    )(start_vector, potential)
    return tuple(pl.pallas_call(
        write_out,
        out_shape=(jax.ShapeDtypeStruct((D + 1, Z, Y, X), f32), jax.ShapeDtypeStruct((2, D), f32)),
        in_specs=[vmem] * 3,
        out_specs=(hbm, hbm),
        scratch_shapes=[pltpu.VMEM((D + 1, Z, Y, X), f32), dma((2,))],
    )(*(pltpu.with_memory_space_constraint(ref, pltpu.VMEM) for ref in held)))


def solution(mesh):
    sizes = tuple(mesh.shape[name] for name in AXES)
    in_specs = (P("pz", "py", "slab"), P("pz", "py", "slab"))
    out_specs = (P(None, "pz", "py", "slab"), P())
    return jax.shard_map(functools.partial(shards, sizes), mesh=mesh, in_specs=in_specs,
                         out_specs=out_specs, check_vma=False)
```
